128 devices in a mesh: gx: 4 (over z), gy: 4 (over y), gz: 8 (over x, core).
Axes of the slice: x: 4, y: 4, z: 4, core: 2. Of those that a mesh axis runs over, the one named last changes fastest.
Arguments:
- positions: float32 [3, 64, 64, 2048], P(None, 'gx', 'gy', 'gz'), may hold values from -6 to 6
- pair_node: int32 [4, 4, 8, 32, 256], P('gx', 'gy', 'gz'), may hold values from 0 to 255
- pair_line: int32 [4, 4, 8, 32], P('gx', 'gy', 'gz'), may hold values from 0 to 255
- pair_far: int32 [4, 4, 8, 32, 256], P('gx', 'gy', 'gz'), may hold values from 0 to 261, as said below
- far_line: int32 [4, 4, 8, 32], P('gx', 'gy', 'gz'), may hold values from 0 to 483, as said below
- pair_geom: float32 [4, 4, 8, 32, 4, 256], P('gx', 'gy', 'gz'), may hold values from -4 to 4
- live_blocks: int32 [4, 4, 8], P('gx', 'gy', 'gz'), may hold values from 8 to 32, as said below
Outputs:
- corrected: float32 [3, 64, 64, 2048], P(None, 'gx', 'gy', 'gz')
- sweep_history: float32 [2, 5], replicated
The draws below stay inside these ranges and needn't reach their ends.
Inputs may be any that keep to these rules, and one draw needn't show every extreme that they name: `pair_far`: together with far_line: at most one of the three coordinates of node b lies outside the owner block's own nodes; node b lies inside the whole grid; in slots below 16 node b is one of the owner block's own nodes. `far_line`: together with pair_far, as stated there. `live_blocks`: some owner block has all 32 slots live.
All inputs are finite; a program needn't handle non-finite values.
Results may differ from the reference program's by a relative error of at most 0.0001.
Values sent between devices are 32-bit elements; how exact they have to be, the bound alone decides.
No kernel may reach another device: no remote copies, remote signals or barrier semaphores. Data moves between devices by JAX's collectives and lax.ppermute only.
A program may use at most 64 MiB of HBM per device.

```python
import jax
import jax.numpy as jnp
from jax import lax

CX = 16
CY = 16
CZ = 256
BLOCKS = 32
PAIRS_BLK = 256
RIM = 3
SWEEPS = 5
NX = 64
NY = 64
NZ = 2048
PAIRS_ALL = 1048576
N_GX = 4
N_GY = 4
N_GZ = 8


def far_layout(key):
    grid_x = NX // CX
    grid_y = NY // CY
    grid_z = NZ // CZ
    block_shape = (grid_x, grid_y, grid_z, BLOCKS)
    full_shape = (grid_x, grid_y, grid_z, BLOCKS, PAIRS_BLK)
    subkeys = jax.random.split(jax.random.fold_in(key, 7117), 8)
    line_x = jax.random.randint(subkeys[0], block_shape, RIM, CX + RIM)
    line_y = jax.random.randint(subkeys[1], block_shape, RIM, CY + RIM)
    coord_z = jax.random.randint(subkeys[2], full_shape, RIM, CZ + RIM)
    face_axis = jax.random.randint(subkeys[3], block_shape, 0, 3)
    high_block = jax.random.randint(subkeys[4], block_shape, 0, 2)
    layer_block = jax.random.randint(subkeys[5], block_shape, 0, RIM)
    high_pair = jax.random.randint(subkeys[6], full_shape, 0, 2)
    layer_pair = jax.random.randint(subkeys[7], full_shape, 0, RIM)
    rim_slot = lax.broadcasted_iota(jnp.int32, block_shape, 3) >= BLOCKS // 2

    def rim_coord(shape, axis_dim, extent, blocks_along, high_face, rim_layer):
        block_pos = lax.broadcasted_iota(jnp.int32, shape, axis_dim)
        low_side = jnp.where(block_pos == 0, RIM + rim_layer, rim_layer)
        high_side = jnp.where(block_pos == blocks_along - 1, extent + RIM - 1 - rim_layer, extent + RIM + rim_layer)
        return jnp.where(high_face == 1, high_side, low_side)
    line_x = jnp.where(rim_slot & (face_axis == 0), rim_coord(block_shape, 0, CX, grid_x, high_block, layer_block), line_x)
    line_y = jnp.where(rim_slot & (face_axis == 1), rim_coord(block_shape, 1, CY, grid_y, high_block, layer_block), line_y)
    z_face = (rim_slot & (face_axis == 2))[:, :, :, :, None]
    coord_z = jnp.where(z_face, rim_coord(full_shape, 2, CZ, grid_z, high_pair, layer_pair), coord_z)
    return ((line_x * (CY + 2 * RIM) + line_y).astype(jnp.int32), coord_z.astype(jnp.int32))


def draw_pair_far(key, part):
    return far_layout(key)[1]


def draw_far_line(key, part):
    return far_layout(key)[0]


def draw_live_blocks(key, part):
    grid_x = NX // CX
    grid_y = NY // CY
    grid_z = NZ // CZ
    full_shape = (grid_x, grid_y, grid_z)
    subkeys = jax.random.split(key, 3)
    base_count = jax.random.randint(subkeys[0], full_shape, BLOCKS // 4, BLOCKS // 2 + 1)
    heavy_dev = jax.random.randint(subkeys[1], full_shape, 0, 8) == 0
    chosen = jax.random.randint(subkeys[2], (), 0, grid_x * grid_y * grid_z)
    linear = (lax.broadcasted_iota(jnp.int32, full_shape, 0) * grid_y + lax.broadcasted_iota(jnp.int32, full_shape, 1)) * grid_z + lax.broadcasted_iota(jnp.int32, full_shape, 2)
    return jnp.where(heavy_dev | (linear == chosen), BLOCKS, base_count).astype(jnp.int32)


def set_ends(drawn, own_key, low, top_value):
    longest = drawn.shape.index(max(drawn.shape))
    spots = []
    for shift in (0, 1):
        where = [jax.random.randint(jax.random.fold_in(own_key, axis), (), 0, length) for axis, length in enumerate(drawn.shape)]
        where[longest] = (where[longest] + shift) % drawn.shape[longest]
        spots.append(tuple(where))
    return drawn.at[spots[0]].set(low).at[spots[1]].set(top_value)


def shard_levels(stream_key, dims, cuts, least, top_value):
    level = 1.0
    for dim, shards_of in cuts:
        steps = jax.random.uniform(jax.random.fold_in(jax.random.fold_in(stream_key, 6), dim), (shards_of,), jnp.float32, least / len(cuts), top_value / len(cuts))
        level = level * jnp.repeat(jnp.exp(steps), dims[dim] // shards_of).reshape((-1,) + (1,) * (len(dims) - 1 - dim))
    return level


def centred(own_key, shape, width, most, cuts=(), kind=jnp.bfloat16):
    gain = shard_levels(own_key, shape, cuts, -0.22, 0.18) if cuts else 1.0
    drawn = jax.random.normal(own_key, shape, jnp.float32) * width * gain
    return jnp.minimum(jnp.maximum(drawn, -most), most).astype(kind)


def setup_inputs(seed: int = 0) -> dict:
    seeds = jax.random.split(jax.random.key(seed), 8)
    return {
        "positions": centred(seeds[0], (3, NX, NY, NZ), 1.0, 6.0, ((1, 4), (2, 4), (3, 8)), jnp.float32),
        "pair_node": set_ends(jax.random.randint(seeds[1], (N_GX, N_GY, N_GZ, BLOCKS, PAIRS_BLK), 0, CZ), jax.random.fold_in(seeds[1], 1), 0, CZ - 1).astype(jnp.int32),
        "pair_line": set_ends(jax.random.randint(seeds[2], (N_GX, N_GY, N_GZ, BLOCKS), 0, CX * CY), jax.random.fold_in(seeds[2], 1), 0, (CX * CY) - 1).astype(jnp.int32),
        "pair_far": draw_pair_far(jax.random.fold_in(seeds[7], 71), 0),
        "far_line": draw_far_line(jax.random.fold_in(seeds[7], 71), 0),
        "pair_geom": centred(seeds[5], (N_GX, N_GY, N_GZ, BLOCKS, 4, PAIRS_BLK), 0.6, 4.0, ((0, 4), (1, 4), (2, 8)), jnp.float32),
        "live_blocks": draw_live_blocks(jax.random.fold_in(seeds[7], 71), 0),
    }


relax_factor = 0.9

def reference(positions, pair_node, pair_line, pair_far, far_line, pair_geom, live_blocks):
    full_shape = pair_node.shape
    block_x = lax.broadcasted_iota(jnp.int32, full_shape, 0)
    block_y = lax.broadcasted_iota(jnp.int32, full_shape, 1)
    block_z = lax.broadcasted_iota(jnp.int32, full_shape, 2)
    slot_index = lax.broadcasted_iota(jnp.int32, full_shape, 3)
    line_full = jnp.broadcast_to(pair_line[:, :, :, :, None], full_shape)
    node_x = block_x * CX + line_full // CY
    node_y = block_y * CY + line_full % CY
    node_z = block_z * CZ + pair_node
    own_flat = ((node_x * NY + node_y) * NZ + node_z).reshape(-1).astype(jnp.int32)
    ext_y = CY + 2 * RIM
    far_full = jnp.broadcast_to(far_line[:, :, :, :, None], full_shape)
    far_x = far_full // ext_y
    far_y = far_full % ext_y
    far_z = pair_far
    pad_y = NY + 2 * RIM
    pad_z = NZ + 2 * RIM
    far_flat = (((block_x * CX + far_x) * pad_y + block_y * CY + far_y) * pad_z + block_z * CZ + far_z).reshape(-1).astype(jnp.int32)
    live_mask = (slot_index < live_blocks[:, :, :, None, None]).reshape(-1)
    geometry = jnp.moveaxis(pair_geom, 4, 0).reshape(4, -1)
    node_count = NX * NY * NZ
    live_ones = jnp.where(live_mask, 1.0, 0.0).astype(jnp.float32)
    counts = jnp.zeros((node_count,), jnp.float32).at[own_flat].add(live_ones)
    current = positions.reshape(3, -1)
    energies = []
    residuals = []
    for sweep_idx in range(SWEEPS):
        padded = jnp.pad(current.reshape(3, NX, NY, NZ), ((0, 0), (RIM, RIM), (RIM, RIM), (RIM, RIM))).reshape(3, -1)
        differ = current[:, own_flat] - padded[:, far_flat]
        gap_value = lax.optimization_barrier(jnp.sum(geometry[0:3] * differ, axis=0)) - geometry[3]
        depth_value = jnp.where(live_mask, jnp.maximum(-gap_value, 0.0), 0.0)
        energy = jnp.sum(depth_value * depth_value)
        node_total = jnp.zeros((3, node_count), jnp.float32).at[:, own_flat].add(depth_value[None, :] * geometry[0:3])
        scale_factor = 1.0 / (1.0 + energy / PAIRS_ALL)
        correction = relax_factor * scale_factor * node_total / (1.0 + counts)
        current = current + correction
        residuals.append(jnp.sum(correction * correction))
        energies.append(energy)
    history = jnp.stack([jnp.sqrt(1.0 + jnp.stack(energies) / (PAIRS_BLK * BLOCKS)), jnp.sqrt(1.0 + jnp.stack(residuals) / (CX * CY * CZ))])
    return (current.reshape(3, NX, NY, NZ), history)
```

```python
import functools

import jax
import jax.numpy as jnp
from jax import lax
from jax.experimental import pallas as pl
from jax.experimental.pallas import tpu as pltpu
from jax.sharding import Mesh
from jax.sharding import PartitionSpec as P

SWEEPS = 5
RELAX = 0.9
XY = ("gx", "gy")
GZ = ("gz_0", "gz_1")
ALL = ("gx", "gy", "gz_0", "gz_1")
F32 = jnp.float32
BF16 = jnp.bfloat16
I32 = jnp.int32
SLOTS = 32
OUTER = 16
N_PAIRS = 1048576
NODES_BLK = 65536
PAIRS_SLOTS = 8192


def iota(shape, dim):
    return lax.broadcasted_iota(I32, shape, dim)


def split3(x):
    hi = x.astype(BF16)
    rest = x - hi.astype(F32)
    mid = rest.astype(BF16)
    low = (rest - mid.astype(F32)).astype(BF16)
    return hi, mid, low


def pick(sel, x):
    hi, mid, low = split3(x)
    dot = functools.partial(jnp.dot, preferred_element_type=F32)
    return (dot(sel, low) + dot(sel, mid)) + dot(sel, hi)


def hot(a, b):
    return jnp.where(a == b, 1.0, 0.0).astype(BF16)


def column(row, first, count):
    shape = (count, row.shape[1])
    chosen = iota(shape, 0) + first == iota(shape, 1)
    return jnp.sum(jnp.where(chosen, jnp.broadcast_to(row, shape), 0.0), axis=1, keepdims=True)


def take128(x, index):
    return jnp.take_along_axis(x, index, axis=1, mode="promise_in_bounds")


def take_lanes(x, index):
    low = index & 127
    high = index >= 128
    parts = []
    for t in (0, 1):
        cut = slice(t * 128, (t + 1) * 128)
        a = take128(x[:, :128], low[:, cut])
        b = take128(x[:, 128:], low[:, cut])
        parts.append(jnp.where(high[:, cut], b, a))
    return jnp.concatenate(parts, axis=1)


def decode(far_line):
    x = (far_line * 2979) >> 16
    y = far_line - 22 * x - 3
    x = x - 3
    return x, y, (x & 15) * 16 + (y & 15)


def edge_lanes(parts, low_first, high_first):
    lane = iota((parts[0].shape[0], 128), 1)
    out = jnp.zeros((parts[0].shape[0], 128), F32)
    for c in range(3):
        for first, half, at in ((low_first, 0, 0), (high_first, 1, 125)):
            if first is None:
                continue
            to = first + 3 * c
            moved = parts[c][:, half * 128 : half * 128 + 128]
            if (to - at) % 128:
                moved = pltpu.roll(moved, (to - at) % 128, axis=1)
            out = jnp.where((lane >= to) & (lane < to + 3), moved, out)
    return out


def pack_kernel(pos, far, geom, fline, pline, xdn, xup, ydn, yup, zdn, zup, geom_out):
    for c in range(4):
        geom_out[c] = geom[:, c, :]
    fcol = column(fline[...].astype(F32), OUTER, OUTER).astype(I32)
    x, y, line = decode(fcol)
    tag = (line + 1).astype(F32)
    far_z = jnp.clip(far[OUTER:, :] - 3, 0, 255).astype(F32)
    for buf, mask in ((xdn, x < 0), (xup, x > 15), (ydn, y < 0), (yup, y > 15)):
        for c in range(3):
            buf[144 + 16 * c : 160 + 16 * c, :] = geom_out[c, OUTER:, :]
        buf[192:208, :] = far_z
        buf[208:224, :] = jnp.broadcast_to(jnp.where(mask, tag, 0.0), (OUTER, 256))
    for c in range(3):
        xdn[48 * c : 48 * c + 48, :] = pos[c, 0:48, :]
        xup[48 * c : 48 * c + 48, :] = pos[c, 208:256, :]
        for i in range(16):
            to = 48 * c + 3 * i
            ydn[to : to + 3, :] = pos[c, 16 * i : 16 * i + 3, :]
            yup[to : to + 3, :] = pos[c, 16 * i + 13 : 16 * i + 16, :]
    parts = [pos[c] for c in range(3)]
    zdn[0:256, :] = edge_lanes(parts, 0, None)
    zup[0:256, :] = edge_lanes(parts, None, 9)
    lines = jnp.broadcast_to(pline[...].astype(F32) + 1.0, (8, SLOTS))
    for buf in (zdn, zup):
        buf[256:264, :] = jnp.zeros((8, 128), F32)
        buf[256:264, 0:SLOTS] = lines


def z_index(far_outer):
    z = far_outer - 3
    below = z < 0
    above = z > 255
    index = jnp.where(below, z + 12, jnp.where(above, z - 256, 0))
    return index, below | above


def z_values(edges, far_outer):
    index, outside = z_index(far_outer)
    out = []
    for c in range(3):
        parts = [
            take128(edges, index[:, t * 128 : (t + 1) * 128] + 3 * c) for t in (0, 1)
        ]
        out.append(jnp.where(outside, jnp.concatenate(parts, axis=1), 0.0))
    return out


def scatter(rows, node, xs, ys):
    for r, value in enumerate(rows):
        for t in (0, 1):
            xs[t, pl.ds(r, SLOTS, stride=8), :] = value[:, t * 128 : (t + 1) * 128]
    for t in (0, 1):
        xs[t, pl.ds(4, SLOTS, stride=8), :] = node[:, t * 128 : (t + 1) * 128].astype(F32)
        for r in [r for r in range(len(rows), 8) if r != 4]:
            xs[t, pl.ds(r, SLOTS, stride=8), :] = jnp.zeros((SLOTS, 128), F32)
    places = iota((256, 256), 0).astype(F32).astype(BF16)
    one = jnp.ones((), BF16)
    zero = jnp.zeros((), BF16)

    def group(g, carry):
        for i in range(8):
            at = pl.multiple_of(g * 64 + i * 8, 8)
            x = jnp.concatenate([xs[0, pl.ds(at, 8), :], xs[1, pl.ds(at, 8), :]], axis=1)
            index = jnp.broadcast_to(x[4:5, :].astype(BF16), (256, 256))
            onehot = jnp.where(places == index, one, zero)
            hi = x.astype(BF16).astype(F32)
            rest = x - hi
            mid = rest.astype(BF16).astype(F32)
            lhs = jnp.concatenate([hi, mid, rest - mid, jnp.zeros_like(x)], axis=0).astype(BF16)
            got = lax.dot_general(
                lhs, onehot, (((1,), (1,)), ((), ())), preferred_element_type=F32
            )
            total = (got[16:24] + got[8:16]) + got[0:8]
            ys[0, pl.ds(at, 8), :] = total[:, :128]
            ys[1, pl.ds(at, 8), :] = total[:, 128:]
        return carry

    lax.fori_loop(0, SLOTS // 8, group, 0)
    return [
        jnp.concatenate([ys[t, pl.ds(r, SLOTS, stride=8), :] for t in (0, 1)], axis=1)
        for r in range(len(rows))
    ]


def pair_tile(first, second):
    lane = iota((8, 128), 1)
    return jnp.where(lane == 0, first, jnp.where(lane == 1, second, 0.0))


def depth_of(gap, live):
    return jnp.where(iota((SLOTS, 256), 0) < live, jnp.maximum(-gap, 0.0), 0.0)


def total2(x):
    return jnp.sum(jnp.sum(x, axis=0, keepdims=True), axis=1, keepdims=True)


def residual_of(near, pline):
    shape = (SLOTS, SLOTS)
    row = jnp.broadcast_to(pline.astype(F32), shape)
    col = column(pline.astype(F32), 0, SLOTS)
    again = jnp.where((row == col) & (iota(shape, 1) < iota(shape, 0)), 1.0, 0.0)
    first = jnp.sum(again, axis=1, keepdims=True) == 0.0
    square = near[0] * near[0] + near[1] * near[1] + near[2] * near[2]
    return total2(jnp.where(first, square, 0.0))


def respond(normal, energy, node, far, geom, pline, sel, requests, place, out, edge, change):
    lines = [pick(sel[...], normal[c]) for c in range(3)]
    residual = residual_of([v[0:SLOTS] for v in lines], pline)
    tile = pair_tile(energy, residual)
    tile = jnp.concatenate([tile, tile], axis=1)
    for j in range(16):
        out[j, 0:OUTER, :] = jnp.zeros((OUTER, 256), F32)
        out[j, OUTER:24, :] = tile
    x, y = place[0], place[1]
    me = x * 4 + y
    for d, (buf, to, there) in enumerate(
        (
            (requests[0], me - 4, x > 0),
            (requests[1], me + 4, x < 3),
            (requests[2], me - 1, y > 0),
            (requests[3], me + 1, y < 3),
        )
    ):
        at = 2 * SLOTS + OUTER * d
        index = buf[192:208, :].astype(I32)
        answer = jnp.zeros((OUTER, 256), F32)
        for c in range(3):
            value = take_lanes(lines[c][at : at + OUTER], index)
            answer = answer + buf[144 + 16 * c : 160 + 16 * c, :] * value

        @pl.when(there)
        def _():
            out[jnp.where(there, to, 0), 0:OUTER, :] = answer

    z = far[...] - 3
    inside = (z >= 0) & (z < 256)
    index = jnp.clip(z, 0, 255)
    moved = jnp.zeros((SLOTS, 256), F32)
    for c in range(3):
        near = take_lanes(lines[c][0:SLOTS], node[...])
        other = jnp.where(inside, take_lanes(lines[c][SLOTS : 2 * SLOTS], index), 0.0)
        moved = moved + geom[c] * (near - other)
    change[...] = moved
    edge[...] = edge_lanes(normal, 0, 9)


def first_kernel(
    place,
    pos,
    node,
    far,
    geom,
    pline,
    fline,
    live,
    xlo,
    xhi,
    ylo,
    yhi,
    zlo,
    zhi,
    out,
    edge,
    change,
    gap_out,
    normal_out,
    sel_out,
    selz_out,
    inverse_out,
    xs,
    ys,
):
    own = pline[...].astype(F32)
    near_col = column(own, 0, SLOTS)
    far_col = column(fline[...].astype(F32), 0, SLOTS)
    x, y, line = decode(far_col.astype(I32))
    inside = (x >= 0) & (x < 16) & (y >= 0) & (y < 16)
    local = jnp.where(inside, line, -2).astype(F32)
    xo, yo = x[OUTER:], y[OUTER:]
    face = jnp.where(xo < 0, (xo + 3) * 16 + yo, -1)
    face = jnp.where(xo > 15, 48 + (xo - 16) * 16 + yo, face)
    face = jnp.where(yo < 0, 96 + xo * 3 + yo + 3, face)
    face = jnp.where(yo > 15, 144 + xo * 3 + yo - 16, face)
    requests = (xlo, xhi, ylo, yhi)
    wanted = jnp.concatenate(
        [near_col, local] + [buf[208:224, 0:1] - 1.0 for buf in requests], axis=0
    )
    sel = hot(jnp.broadcast_to(own, (128, SLOTS)), wanted)
    sel_out[...] = sel
    selz = jnp.concatenate([zhi[256:257, 0:SLOTS], zlo[256:257, 0:SLOTS]], axis=1) - 1.0
    selz_out[...] = hot(jnp.broadcast_to(selz, (OUTER, 2 * SLOTS)), local[OUTER:])
    lines_f = iota((2 * SLOTS, 256), 1).astype(F32)
    sel_pos = hot(lines_f, jnp.concatenate([near_col, local], axis=0))
    sel_face = hot(iota((OUTER, 192), 1), face)
    lane = iota((256, 128), 1)
    edges = jnp.where(lane < 9, zhi[0:256, :], zlo[0:256, :])
    edges = pick(sel_pos[SLOTS + OUTER :], edges)
    ends = z_values(edges, far[OUTER:, :])
    z = far[...] - 3
    within = (z >= 0) & (z < 256)
    index = jnp.clip(z, 0, 255)
    gap = -geom[3]
    terms = jnp.zeros((SLOTS, 256), F32)
    for c in range(3):
        got = pick(sel_pos, pos[c])
        faces = jnp.concatenate([buf[48 * c : 48 * c + 48, :] for buf in requests], axis=0)
        outer = got[SLOTS + OUTER :] + pick(sel_face, faces)
        near = take_lanes(got[0:SLOTS], node[...])
        other = jnp.concatenate([got[SLOTS : SLOTS + OUTER], outer], axis=0)
        other = jnp.where(within, take_lanes(other, index), 0.0)
        other = other + jnp.concatenate([jnp.zeros((OUTER, 256), F32), ends[c]], axis=0)
        terms = terms + geom[c] * (near - other)
    gap = terms + gap
    gap_out[...] = gap
    depth = depth_of(gap, live[...])
    ones = jnp.where(iota((SLOTS, 256), 0) < live[...], 1.0, 0.0)
    got = scatter([depth * geom[c] for c in range(3)] + [ones], node[...], xs, ys)
    inverse = 1.0 / (1.0 + pick(sel[0:SLOTS], got[3]))
    inverse_out[...] = inverse
    normal = [got[c] * inverse for c in range(3)]
    for c in range(3):
        normal_out[c] = normal[c]
    respond(
        normal, total2(depth * depth), node, far, geom, pline[...], sel_out, requests, place,
        out, edge, change,
    )


def forward_kernel(got, edge, out):
    sums = jnp.sum(got[...], axis=0)[:, :128]
    for j in range(8):
        out[j, 0:SLOTS, :] = edge[...]
        out[j, SLOTS:40, :] = sums


def update(place, gap, change, far, geom, got, gotz, selz):
    sums = jnp.sum(gotz[:, SLOTS:40, :], axis=0)
    energy = sums[0:1, 0:1]
    scale = RELAX * (1.0 / (1.0 + energy / N_PAIRS))
    x, y, k = place[0], place[1], place[2]
    me = x * 4 + y
    outer = jnp.zeros((OUTER, 256), F32)
    for to, there in ((me - 4, x > 0), (me + 4, x < 3), (me - 1, y > 0), (me + 1, y < 3)):
        reply = got[jnp.where(there, to, me), 0:OUTER, :]
        outer = outer + jnp.where(there, reply, 0.0)
    lane = iota((SLOTS, 128), 1)
    above = jnp.where((lane < 9) & (k < 7), gotz[jnp.minimum(k + 1, 7), 0:SLOTS, :], 0.0)
    below = jnp.where((lane >= 9) & (k > 0), gotz[jnp.maximum(k - 1, 0), 0:SLOTS, :], 0.0)
    ends = z_values(
        pick(selz[...], jnp.concatenate([above, below], axis=0)), far[OUTER:, :]
    )
    for c in range(3):
        outer = outer + geom[c, OUTER:, :] * ends[c]
    full = change[...] - jnp.concatenate([jnp.zeros((OUTER, 256), F32), outer], axis=0)
    return sums, scale, gap[...] + scale * full


def sweep_kernel(
    last, place, gap, change, normal, moved, inverse, node, far, geom, pline, live, sel, selz,
    got, gotz, *rest,
):
    if last:
        out, sums_out, normal_out, moved_out, xs, ys = rest
    else:
        xlo, xhi, ylo, yhi = rest[:4]
        out, edge, change_out, gap_out, sums_out, normal_out, moved_out, xs, ys = rest[4:]
    sums, scale, fresh = update(place, gap, change, far, geom, got, gotz, selz)
    sums_out[...] = sums
    for c in range(3):
        moved_out[c] = moved[c] + scale * normal[c]
    depth = depth_of(fresh, live[...])
    energy = total2(depth * depth)
    found = scatter([depth * geom[c] for c in range(3)], node[...], xs, ys)
    fresh_normal = [found[c] * inverse[...] for c in range(3)]
    for c in range(3):
        normal_out[c] = fresh_normal[c]
    if last:
        lines = [pick(sel[0:SLOTS, :], fresh_normal[c]) for c in range(3)]
        tile = pair_tile(energy, residual_of(lines, pline[...]))
        out[...] = jnp.broadcast_to(tile[0:1, :], (128, 128))
    else:
        gap_out[...] = fresh
        respond(
            fresh_normal, energy, node, far, geom, pline[...], sel, (xlo, xhi, ylo, yhi), place,
            out, edge, change_out,
        )


def last_kernel(pos, normal, moved, pline, got, s0, s1, s2, s3, out, history):
    sums = jnp.sum(got[...], axis=0, keepdims=True)
    every = [s[0:1, :] for s in (s0, s1, s2, s3)] + [sums]
    scales = [RELAX * (1.0 / (1.0 + s[:, 0:1] / N_PAIRS)) for s in every]
    sel = hot(iota((256, SLOTS), 0), jnp.broadcast_to(pline[...], (256, SLOTS)))
    for c in range(3):
        out[c] = pos[c] + pick(sel, moved[c] + scales[-1] * normal[c])
    for t in range(SWEEPS):
        residual = scales[t] * scales[t] * every[t][:, 1:2]
        history[0:1, t : t + 1] = jnp.sqrt(1.0 + every[t][:, 0:1] / PAIRS_SLOTS)
        history[1:2, t : t + 1] = jnp.sqrt(1.0 + residual / NODES_BLK)


def call(kernel, outs, args, scratch=(), smem=False, specs=None):
    vmem = pl.BlockSpec(memory_space=pltpu.VMEM)
    in_specs = specs or [vmem] * len(args)
    if smem:
        in_specs = [pl.BlockSpec(memory_space=pltpu.SMEM)] + in_specs[1:]
    return pl.pallas_call(
        kernel,
        out_shape=outs,
        in_specs=in_specs,
        out_specs=jax.tree.map(lambda _: vmem, outs),
        scratch_shapes=list(scratch),
    )(*args)


def shape(*dims, dtype=F32):
    return jax.ShapeDtypeStruct(dims, dtype)


def shift(x, axis, up):
    count = lax.axis_size(axis)
    pairs = [(i, i + 1) for i in range(count - 1)]
    return lax.ppermute(x, axis, pairs if up else [(b, a) for a, b in pairs])


def local(positions, pair_node, pair_line, pair_far, far_line, pair_geom, live_blocks):
    pos = positions.reshape(3, 256, 256)
    node = pair_node.reshape(SLOTS, 256)
    far = pair_far.reshape(SLOTS, 256)
    geom = pair_geom.reshape(SLOTS, 4, 256)
    pline = pair_line.reshape(1, SLOTS)
    fline = far_line.reshape(1, SLOTS)
    live = live_blocks.reshape(1, 1)
    place = jnp.stack([lax.axis_index("gx"), lax.axis_index("gy"), lax.axis_index(GZ)])
    place = place.astype(I32)
    work = [pltpu.VMEM((2, 256, 128), F32)] * 2

    face, ends = shape(224, 256), shape(264, 128)
    xdn, xup, ydn, yup, zdn, zup, geom = call(
        pack_kernel,
        [face] * 4 + [ends] * 2 + [shape(4, SLOTS, 256)],
        [pos, far, geom, fline, pline],
    )
    requests = [
        shift(xup, "gx", True),
        shift(xdn, "gx", False),
        shift(yup, "gy", True),
        shift(ydn, "gy", False),
    ]
    zlo = shift(zup, GZ, True)
    zhi = shift(zdn, GZ, False)
    triple, flat = shape(3, SLOTS, 256), shape(SLOTS, 256)
    outbound, edges = shape(16, 24, 256), shape(SLOTS, 128)
    out, edge, change, gap, normal, sel, selz, inverse = call(
        first_kernel,
        [
            outbound,
            edges,
            flat,
            flat,
            triple,
            shape(128, SLOTS, dtype=BF16),
            shape(OUTER, 2 * SLOTS, dtype=BF16),
            flat,
        ],
        [place, pos, node, far, geom, pline, fline, live, *requests, zlo, zhi],
        work,
        smem=True,
    )
    moved = jnp.zeros((3, SLOTS, 256), F32)
    totals = []
    vmem = pl.BlockSpec(memory_space=pltpu.VMEM)
    for t in range(1, SWEEPS):
        got = lax.all_to_all(out, XY, 0, 0, tiled=True)
        out = pl.pallas_call(
            forward_kernel,
            out_shape=shape(8, 40, 128),
            grid=(1,),
            in_specs=[
                pl.BlockSpec((16, 8, 256), lambda i: (0, 2, 0)),
                pl.BlockSpec((SLOTS, 128), lambda i: (0, 0)),
            ],
            out_specs=pl.BlockSpec((8, 40, 128), lambda i: (0, 0, 0)),
        )(got, edge)
        gotz = lax.all_to_all(out, GZ, 0, 0, tiled=True)
        last = t + 1 == SWEEPS
        args = [
            place, gap, change, normal, moved, inverse, node, far, geom, pline, live, sel, selz,
            got, gotz,
        ]
        sums_shape = shape(8, 128)
        if last:
            out, sums, normal, moved = call(
                functools.partial(sweep_kernel, True),
                [shape(128, 128), sums_shape, triple, triple],
                args,
                work,
                smem=True,
            )
        else:
            out, edge, change, gap, sums, normal, moved = call(
                functools.partial(sweep_kernel, False),
                [outbound, edges, flat, flat, sums_shape, triple, triple],
                args + requests,
                work,
                smem=True,
            )
        totals.append(sums)
    got = lax.all_to_all(out, ALL, 0, 0, tiled=True)
    corrected, history = call(
        last_kernel,
        [shape(3, 256, 256), shape(2, SWEEPS)],
        [pos, normal, moved, pline, got, *totals],
    )
    return corrected.reshape(positions.shape), history


def solution(mesh):
    finer = Mesh(
        mesh.devices.reshape(mesh.shape["gx"], mesh.shape["gy"], 4, 2), ("gx", "gy", "gz_0", "gz_1")
    )
    placed = (
        P(None, "gx", "gy", GZ),
        P("gx", "gy", GZ, None, None),
        P("gx", "gy", GZ, None),
        P("gx", "gy", GZ, None, None),
        P("gx", "gy", GZ, None),
        P("gx", "gy", GZ, None, None, None),
        P("gx", "gy", GZ),
    )
    return jax.shard_map(
        local,
        mesh=finer,
        in_specs=placed,
        out_specs=(P(None, "gx", "gy", GZ), P()),
        check_vma=False,
    )
```

```python
import functools

import jax
import jax.numpy as jnp
from jax import lax
from jax.experimental import pallas as pl
from jax.experimental.pallas import tpu as pltpu
from jax.sharding import Mesh
from jax.sharding import PartitionSpec as P

SWEEPS = 5
RELAX = 0.9
XY = ("gx", "gy")
GZ = ("gz_0", "gz_1")
ALL = ("gx", "gy", "gz_0", "gz_1")
F32 = jnp.float32
BF16 = jnp.bfloat16
I32 = jnp.int32
SLOTS = 32
OUTER = 16
N_PAIRS = 1048576
NODES_BLK = 65536
PAIRS_SLOTS = 8192


def iota(shape, dim):
    return lax.broadcasted_iota(I32, shape, dim)


def split3(x):
    hi = x.astype(BF16)
    rest = x - hi.astype(F32)
    mid = rest.astype(BF16)
    low = (rest - mid.astype(F32)).astype(BF16)
    return hi, mid, low


def pick(sel, x):
    hi, mid, low = split3(x)
    dot = functools.partial(jnp.dot, preferred_element_type=F32)
    return (dot(sel, low) + dot(sel, mid)) + dot(sel, hi)


def hot(a, b):
    return jnp.where(a == b, 1.0, 0.0).astype(BF16)


def column(row, first, count):
    shape = (count, row.shape[1])
    chosen = iota(shape, 0) + first == iota(shape, 1)
    return jnp.sum(jnp.where(chosen, jnp.broadcast_to(row, shape), 0.0), axis=1, keepdims=True)


def take128(x, index):
    return jnp.take_along_axis(x, index, axis=1, mode="promise_in_bounds")


def take_lanes(x, index):
    low = index & 127
    high = index >= 128
    parts = []
    for t in (0, 1):
        cut = slice(t * 128, (t + 1) * 128)
        a = take128(x[:, :128], low[:, cut])
        b = take128(x[:, 128:], low[:, cut])
        parts.append(jnp.where(high[:, cut], b, a))
    return jnp.concatenate(parts, axis=1)


def decode(far_line):
    x = (far_line * 2979) >> 16
    y = far_line - 22 * x - 3
    x = x - 3
    return x, y, (x & 15) * 16 + (y & 15)


def edge_lanes(parts, low_first, high_first):
    lane = iota((parts[0].shape[0], 128), 1)
    out = jnp.zeros((parts[0].shape[0], 128), F32)
    for c in range(3):
        for first, half, at in ((low_first, 0, 0), (high_first, 1, 125)):
            if first is None:
                continue
            to = first + 3 * c
            moved = parts[c][:, half * 128 : half * 128 + 128]
            if (to - at) % 128:
                moved = pltpu.roll(moved, (to - at) % 128, axis=1)
            out = jnp.where((lane >= to) & (lane < to + 3), moved, out)
    return out


def pack_kernel(
    pos, node, far, geom, pline, fline, live, xdn, xup, ydn, yup, zdn, zup, geom_out, *copies
):
    for source, copy in zip((pos, node, far, pline, fline, live), copies, strict=True):
        copy[...] = source[...]
    for c in range(4):
        geom_out[c] = geom[:, c, :]
    fcol = column(fline[...].astype(F32), OUTER, OUTER).astype(I32)
    x, y, line = decode(fcol)
    tag = (line + 1).astype(F32)
    far_z = jnp.clip(far[OUTER:, :] - 3, 0, 255).astype(F32)
    for buf, mask in ((xdn, x < 0), (xup, x > 15), (ydn, y < 0), (yup, y > 15)):
        for c in range(3):
            buf[144 + 16 * c : 160 + 16 * c, :] = geom_out[c, OUTER:, :]
        buf[192:208, :] = far_z
        buf[208:224, :] = jnp.broadcast_to(jnp.where(mask, tag, 0.0), (OUTER, 256))
    for c in range(3):
        xdn[48 * c : 48 * c + 48, :] = pos[c, 0:48, :]
        xup[48 * c : 48 * c + 48, :] = pos[c, 208:256, :]
        for i in range(16):
            to = 48 * c + 3 * i
            ydn[to : to + 3, :] = pos[c, 16 * i : 16 * i + 3, :]
            yup[to : to + 3, :] = pos[c, 16 * i + 13 : 16 * i + 16, :]
    parts = [pos[c] for c in range(3)]
    zdn[0:256, :] = edge_lanes(parts, 0, None)
    zup[0:256, :] = edge_lanes(parts, None, 9)
    lines = jnp.broadcast_to(pline[...].astype(F32) + 1.0, (8, SLOTS))
    for buf in (zdn, zup):
        buf[256:264, :] = jnp.zeros((8, 128), F32)
        buf[256:264, 0:SLOTS] = lines


def z_index(far_outer):
    z = far_outer - 3
    below = z < 0
    above = z > 255
    index = jnp.where(below, z + 12, jnp.where(above, z - 256, 0))
    return index, below | above


def z_values(edges, far_outer):
    index, outside = z_index(far_outer)
    out = []
    for c in range(3):
        parts = [
            take128(edges, index[:, t * 128 : (t + 1) * 128] + 3 * c) for t in (0, 1)
        ]
        out.append(jnp.where(outside, jnp.concatenate(parts, axis=1), 0.0))
    return out


def scatter(rows, node, xs, ys):
    for r, value in enumerate(rows):
        for t in (0, 1):
            xs[t, pl.ds(r, SLOTS, stride=8), :] = value[:, t * 128 : (t + 1) * 128]
    for t in (0, 1):
        xs[t, pl.ds(4, SLOTS, stride=8), :] = node[:, t * 128 : (t + 1) * 128].astype(F32)
        for r in [r for r in range(len(rows), 8) if r != 4]:
            xs[t, pl.ds(r, SLOTS, stride=8), :] = jnp.zeros((SLOTS, 128), F32)
    places = iota((256, 256), 0).astype(F32).astype(BF16)
    one = jnp.ones((), BF16)
    zero = jnp.zeros((), BF16)

    def group(g, carry):
        for i in range(8):
            at = pl.multiple_of(g * 64 + i * 8, 8)
            x = jnp.concatenate([xs[0, pl.ds(at, 8), :], xs[1, pl.ds(at, 8), :]], axis=1)
            index = jnp.broadcast_to(x[4:5, :].astype(BF16), (256, 256))
            onehot = jnp.where(places == index, one, zero)
            hi = x.astype(BF16).astype(F32)
            rest = x - hi
            mid = rest.astype(BF16).astype(F32)
            lhs = jnp.concatenate([hi, mid, rest - mid, jnp.zeros_like(x)], axis=0).astype(BF16)
            got = lax.dot_general(
                lhs, onehot, (((1,), (1,)), ((), ())), preferred_element_type=F32
            )
            total = (got[16:24] + got[8:16]) + got[0:8]
            ys[0, pl.ds(at, 8), :] = total[:, :128]
            ys[1, pl.ds(at, 8), :] = total[:, 128:]
        return carry

    lax.fori_loop(0, SLOTS // 8, group, 0)
    return [
        jnp.concatenate([ys[t, pl.ds(r, SLOTS, stride=8), :] for t in (0, 1)], axis=1)
        for r in range(len(rows))
    ]


def pair_tile(first, second):
    lane = iota((8, 128), 1)
    return jnp.where(lane == 0, first, jnp.where(lane == 1, second, 0.0))


def depth_of(gap, live):
    return jnp.where(iota((SLOTS, 256), 0) < live, jnp.maximum(-gap, 0.0), 0.0)


def total2(x):
    return jnp.sum(jnp.sum(x, axis=0, keepdims=True), axis=1, keepdims=True)


def residual_of(near, pline):
    shape = (SLOTS, SLOTS)
    row = jnp.broadcast_to(pline.astype(F32), shape)
    col = column(pline.astype(F32), 0, SLOTS)
    again = jnp.where((row == col) & (iota(shape, 1) < iota(shape, 0)), 1.0, 0.0)
    first = jnp.sum(again, axis=1, keepdims=True) == 0.0
    square = near[0] * near[0] + near[1] * near[1] + near[2] * near[2]
    return total2(jnp.where(first, square, 0.0))


def respond(normal, energy, node, far, geom, pline, sel, requests, out, edge, change):
    lines = [pick(sel[...], normal[c]) for c in range(3)]
    residual = residual_of([v[0:SLOTS] for v in lines], pline)
    tile = pair_tile(energy, residual)
    tile = jnp.concatenate([tile, tile], axis=1)
    for j in range(16):
        out[j, 0:OUTER, :] = jnp.zeros((OUTER, 256), F32)
        out[j, OUTER:24, :] = tile
    x, y, _ = position()
    me = x * 4 + y
    for d, (buf, to, there) in enumerate(
        (
            (requests[0], me - 4, x > 0),
            (requests[1], me + 4, x < 3),
            (requests[2], me - 1, y > 0),
            (requests[3], me + 1, y < 3),
        )
    ):
        at = 2 * SLOTS + OUTER * d
        index = buf[192:208, :].astype(I32)
        answer = jnp.zeros((OUTER, 256), F32)
        for c in range(3):
            value = take_lanes(lines[c][at : at + OUTER], index)
            answer = answer + buf[144 + 16 * c : 160 + 16 * c, :] * value

        @pl.when(there)
        def _():
            out[jnp.where(there, to, 0), 0:OUTER, :] = answer

    z = far[...] - 3
    inside = (z >= 0) & (z < 256)
    index = jnp.clip(z, 0, 255)
    moved = jnp.zeros((SLOTS, 256), F32)
    for c in range(3):
        near = take_lanes(lines[c][0:SLOTS], node[...])
        other = jnp.where(inside, take_lanes(lines[c][SLOTS : 2 * SLOTS], index), 0.0)
        moved = moved + geom[c] * (near - other)
    change[...] = moved
    edge[...] = edge_lanes(normal, 0, 9)


def first_kernel(
    pos,
    node,
    far,
    geom,
    pline,
    fline,
    live,
    xlo,
    xhi,
    ylo,
    yhi,
    zlo,
    zhi,
    out,
    edge,
    change,
    gap_out,
    normal_out,
    moved_out,
    sel_out,
    selz_out,
    inverse_out,
    xs,
    ys,
):
    own = pline[...].astype(F32)
    near_col = column(own, 0, SLOTS)
    far_col = column(fline[...].astype(F32), 0, SLOTS)
    x, y, line = decode(far_col.astype(I32))
    inside = (x >= 0) & (x < 16) & (y >= 0) & (y < 16)
    local = jnp.where(inside, line, -2).astype(F32)
    xo, yo = x[OUTER:], y[OUTER:]
    face = jnp.where(xo < 0, (xo + 3) * 16 + yo, -1)
    face = jnp.where(xo > 15, 48 + (xo - 16) * 16 + yo, face)
    face = jnp.where(yo < 0, 96 + xo * 3 + yo + 3, face)
    face = jnp.where(yo > 15, 144 + xo * 3 + yo - 16, face)
    requests = (xlo, xhi, ylo, yhi)
    wanted = jnp.concatenate(
        [near_col, local] + [buf[208:224, 0:1] - 1.0 for buf in requests], axis=0
    )
    sel = hot(jnp.broadcast_to(own, (128, SLOTS)), wanted)
    sel_out[...] = sel
    selz = jnp.concatenate([zhi[256:257, 0:SLOTS], zlo[256:257, 0:SLOTS]], axis=1) - 1.0
    selz_out[...] = hot(jnp.broadcast_to(selz, (OUTER, 2 * SLOTS)), local[OUTER:])
    lines_f = iota((2 * SLOTS, 256), 1).astype(F32)
    sel_pos = hot(lines_f, jnp.concatenate([near_col, local], axis=0))
    sel_face = hot(iota((OUTER, 192), 1), face)
    lane = iota((256, 128), 1)
    edges = jnp.where(lane < 9, zhi[0:256, :], zlo[0:256, :])
    edges = pick(sel_pos[SLOTS + OUTER :], edges)
    ends = z_values(edges, far[OUTER:, :])
    z = far[...] - 3
    within = (z >= 0) & (z < 256)
    index = jnp.clip(z, 0, 255)
    gap = -geom[3]
    terms = jnp.zeros((SLOTS, 256), F32)
    for c in range(3):
        got = pick(sel_pos, pos[c])
        faces = jnp.concatenate([buf[48 * c : 48 * c + 48, :] for buf in requests], axis=0)
        outer = got[SLOTS + OUTER :] + pick(sel_face, faces)
        near = take_lanes(got[0:SLOTS], node[...])
        other = jnp.concatenate([got[SLOTS : SLOTS + OUTER], outer], axis=0)
        other = jnp.where(within, take_lanes(other, index), 0.0)
        other = other + jnp.concatenate([jnp.zeros((OUTER, 256), F32), ends[c]], axis=0)
        terms = terms + geom[c] * (near - other)
    gap = terms + gap
    gap_out[...] = gap
    depth = depth_of(gap, live[...])
    ones = jnp.where(iota((SLOTS, 256), 0) < live[...], 1.0, 0.0)
    got = scatter([depth * geom[c] for c in range(3)] + [ones], node[...], xs, ys)
    inverse = 1.0 / (1.0 + pick(sel[0:SLOTS], got[3]))
    inverse_out[...] = inverse
    normal = [got[c] * inverse for c in range(3)]
    for c in range(3):
        normal_out[c] = normal[c]
        moved_out[c] = jnp.zeros((SLOTS, 256), F32)
    respond(
        normal, total2(depth * depth), node, far, geom, pline[...], sel_out, requests, out, edge,
        change,
    )


def forward_kernel(got, edge, out):
    sums = jnp.sum(got[:, OUTER:24, 0:128], axis=0)
    for j in range(8):
        out[j, 0:SLOTS, :] = edge[...]
        out[j, SLOTS:40, :] = sums


def update(gap, change, far, geom, got, gotz, selz):
    sums = jnp.sum(gotz[:, SLOTS:40, :], axis=0)
    energy = sums[0:1, 0:1]
    scale = RELAX * (1.0 / (1.0 + energy / N_PAIRS))
    x, y, k = position()
    me = x * 4 + y
    outer = jnp.zeros((OUTER, 256), F32)
    for to, there in ((me - 4, x > 0), (me + 4, x < 3), (me - 1, y > 0), (me + 1, y < 3)):
        reply = got[jnp.where(there, to, me), 0:OUTER, :]
        outer = outer + jnp.where(there, reply, 0.0)
    lane = iota((SLOTS, 128), 1)
    above = jnp.where((lane < 9) & (k < 7), gotz[jnp.minimum(k + 1, 7), 0:SLOTS, :], 0.0)
    below = jnp.where((lane >= 9) & (k > 0), gotz[jnp.maximum(k - 1, 0), 0:SLOTS, :], 0.0)
    ends = z_values(
        pick(selz[...], jnp.concatenate([above, below], axis=0)), far[OUTER:, :]
    )
    for c in range(3):
        outer = outer + geom[c, OUTER:, :] * ends[c]
    full = change[...] - jnp.concatenate([jnp.zeros((OUTER, 256), F32), outer], axis=0)
    return sums, scale, gap[...] + scale * full


def sweep_kernel(
    last, gap, change, normal, moved, inverse, node, far, geom, pline, live, sel, selz,
    got, gotz, *rest,
):
    if last:
        out, sums_out, normal_out, moved_out, xs, ys = rest
    else:
        xlo, xhi, ylo, yhi = rest[:4]
        out, edge, change_out, gap_out, sums_out, normal_out, moved_out, xs, ys = rest[4:]
    sums, scale, fresh = update(gap, change, far, geom, got, gotz, selz)
    sums_out[...] = sums
    for c in range(3):
        moved_out[c] = moved[c] + scale * normal[c]
    depth = depth_of(fresh, live[...])
    energy = total2(depth * depth)
    found = scatter([depth * geom[c] for c in range(3)], node[...], xs, ys)
    fresh_normal = [found[c] * inverse[...] for c in range(3)]
    for c in range(3):
        normal_out[c] = fresh_normal[c]
    if last:
        lines = [pick(sel[0:SLOTS, :], fresh_normal[c]) for c in range(3)]
        tile = pair_tile(energy, residual_of(lines, pline[...]))
        out[...] = jnp.broadcast_to(tile[0:1, :], (128, 128))
    else:
        gap_out[...] = fresh
        respond(
            fresh_normal, energy, node, far, geom, pline[...], sel, (xlo, xhi, ylo, yhi), out, edge,
            change_out,
        )


def last_kernel(pos, normal, moved, pline, got, s0, s1, s2, s3, out, history):
    sums = jnp.sum(got[...], axis=0, keepdims=True)
    every = [s[0:1, :] for s in (s0, s1, s2, s3)] + [sums]
    scales = [RELAX * (1.0 / (1.0 + s[:, 0:1] / N_PAIRS)) for s in every]
    sel = hot(iota((256, SLOTS), 0), jnp.broadcast_to(pline[...], (256, SLOTS)))
    for c in range(3):
        out[c] = pos[c] + pick(sel, moved[c] + scales[-1] * normal[c])
    for t in range(SWEEPS):
        residual = scales[t] * scales[t] * every[t][:, 1:2]
        history[0:1, t : t + 1] = jnp.sqrt(1.0 + every[t][:, 0:1] / PAIRS_SLOTS)
        history[1:2, t : t + 1] = jnp.sqrt(1.0 + residual / NODES_BLK)


def position():
    return lax.axis_index("gx"), lax.axis_index("gy"), lax.axis_index(GZ)


def call(kernel, outs, args, scratch=(), inputs=False):
    vmem = pl.BlockSpec(memory_space=pltpu.VMEM)
    return pl.pallas_call(
        kernel,
        out_shape=outs,
        in_specs=[vmem] * len(args),
        out_specs=[vmem] * len(outs) if isinstance(outs, list) else vmem,
        scratch_shapes=list(scratch),
        compiler_params=pltpu.CompilerParams(vmem_limit_bytes=12 * 2**20),
    )(*(args if inputs else [in_vmem(x) for x in args]))


def shape(*dims, dtype=F32):
    return pltpu.VMEM(dims, dtype)


def in_vmem(x):
    return pltpu.with_memory_space_constraint(x, pltpu.VMEM)


def shift(x, axis, up):
    count = lax.axis_size(axis)
    pairs = [(i, i + 1) for i in range(count - 1)]
    return lax.ppermute(x, axis, pairs if up else [(b, a) for a, b in pairs])


def local(positions, pair_node, pair_line, pair_far, far_line, pair_geom, live_blocks):
    pos = positions.reshape(3, 256, 256)
    node = pair_node.reshape(SLOTS, 256)
    far = pair_far.reshape(SLOTS, 256)
    geom = pair_geom.reshape(SLOTS, 4, 256)
    pline = pair_line.reshape(1, SLOTS)
    fline = far_line.reshape(1, SLOTS)
    live = live_blocks.reshape(1, 1)
    work = [pltpu.VMEM((2, 256, 128), F32)] * 2

    face, ends = shape(224, 256), shape(264, 128)
    flat = shape(SLOTS, 256)
    flat_i = shape(SLOTS, 256, dtype=I32)
    few = shape(1, SLOTS, dtype=I32)
    packed = call(
        pack_kernel,
        [face] * 4
        + [ends] * 2
        + [shape(4, SLOTS, 256), shape(3, 256, 256), flat_i, flat_i, few, few]
        + [shape(1, 1, dtype=I32)],
        [pos, node, far, geom, pline, fline, live],
        inputs=True,
    )
    xdn, xup, ydn, yup, zdn, zup, geom, pos, node, far, pline, fline, live = packed
    requests = [
        shift(xup, "gx", True),
        shift(xdn, "gx", False),
        shift(yup, "gy", True),
        shift(ydn, "gy", False),
    ]
    zlo = shift(zup, GZ, True)
    zhi = shift(zdn, GZ, False)
    triple = shape(3, SLOTS, 256)
    outbound, edges = shape(16, 24, 256), shape(SLOTS, 128)
    out, edge, change, gap, normal, moved, sel, selz, inverse = call(
        first_kernel,
        [
            outbound,
            edges,
            flat,
            flat,
            triple,
            triple,
            shape(128, SLOTS, dtype=BF16),
            shape(OUTER, 2 * SLOTS, dtype=BF16),
            flat,
        ],
        [pos, node, far, geom, pline, fline, live, *requests, zlo, zhi],
        work,
    )
    totals = []
    for t in range(1, SWEEPS):
        got = lax.all_to_all(out, XY, 0, 0, tiled=True)
        out = call(forward_kernel, shape(8, 40, 128), [got, edge])
        gotz = lax.all_to_all(out, GZ, 0, 0, tiled=True)
        last = t + 1 == SWEEPS
        args = [
            gap, change, normal, moved, inverse, node, far, geom, pline, live, sel, selz,
            got, gotz,
        ]
        sums_shape = shape(8, 128)
        if last:
            out, sums, normal, moved = call(
                functools.partial(sweep_kernel, True),
                [shape(128, 128), sums_shape, triple, triple],
                args,
                work,
            )
        else:
            out, edge, change, gap, sums, normal, moved = call(
                functools.partial(sweep_kernel, False),
                [outbound, edges, flat, flat, sums_shape, triple, triple],
                args + requests,
                work,
            )
        totals.append(sums)
    got = lax.all_to_all(out, ALL, 0, 0, tiled=True)
    corrected, history = call(
        last_kernel,
        [jax.ShapeDtypeStruct((3, 256, 256), F32), jax.ShapeDtypeStruct((2, SWEEPS), F32)],
        [pos, normal, moved, pline, got, *totals],
    )
    return corrected.reshape(positions.shape), history


def solution(mesh):
    finer = Mesh(
        mesh.devices.reshape(mesh.shape["gx"], mesh.shape["gy"], 4, 2), ("gx", "gy", "gz_0", "gz_1")
    )
    placed = (
        P(None, "gx", "gy", GZ),
        P("gx", "gy", GZ, None, None),
        P("gx", "gy", GZ, None),
        P("gx", "gy", GZ, None, None),
        P("gx", "gy", GZ, None),
        P("gx", "gy", GZ, None, None, None),
        P("gx", "gy", GZ),
    )
    return jax.shard_map(
        local,
        mesh=finer,
        in_specs=placed,
        out_specs=(P(None, "gx", "gy", GZ), P()),
        check_vma=False,
    )
```

```python
import functools

import jax
import jax.numpy as jnp
from jax import lax
from jax.experimental import pallas as pl
from jax.experimental.pallas import tpu as pltpu
from jax.sharding import Mesh
from jax.sharding import PartitionSpec as P

SWEEPS = 5
RELAX = 0.9
XY = ("gx", "gy")
GZ = ("gz_0", "gz_1")
ALL = ("gx", "gy", "gz_0", "gz_1")
F32 = jnp.float32
BF16 = jnp.bfloat16
I32 = jnp.int32
SLOTS = 32
OUTER = 16
N_PAIRS = 1048576
NODES_BLK = 65536
PAIRS_SLOTS = 8192


def iota(shape, dim):
    return lax.broadcasted_iota(I32, shape, dim)


def pick(sel, x):
    hi = x.astype(BF16)
    mid = (x - hi.astype(F32)).astype(BF16)
    dot = functools.partial(jnp.dot, preferred_element_type=F32)
    return dot(sel, mid) + dot(sel, hi)


def hot(a, b):
    return jnp.where(a == b, 1.0, 0.0).astype(BF16)


def column(row, first, count):
    shape = (count, row.shape[1])
    chosen = iota(shape, 0) + first == iota(shape, 1)
    return jnp.sum(jnp.where(chosen, jnp.broadcast_to(row, shape), 0.0), axis=1, keepdims=True)


def take128(x, index):
    return jnp.take_along_axis(x, index, axis=1, mode="promise_in_bounds")


def take_lanes(xs, index):
    columns = [[] for _ in xs]
    for t in (0, 1):
        cut = index[:, t * 128 : (t + 1) * 128]
        low = cut & 127
        high = cut > 127
        rows = [[] for _ in xs]
        for g in range(0, index.shape[0], 8):
            at = slice(g, g + 8)
            for x, row in zip(xs, rows, strict=True):
                a = take128(x[at, :128], low[at])
                b = take128(x[at, 128:], low[at])
                row.append(jnp.where(high[at], b, a))
        for column_parts, row in zip(columns, rows, strict=True):
            column_parts.append(jnp.concatenate(row, axis=0))
    return [jnp.concatenate(parts, axis=1) for parts in columns]


def decode(far_line):
    x = (far_line * 2979) >> 16
    y = far_line - 22 * x - 3
    x = x - 3
    return x, y, (x & 15) * 16 + (y & 15)


def edge_lanes(parts, low_first, high_first):
    lane = iota((parts[0].shape[0], 128), 1)
    out = jnp.zeros((parts[0].shape[0], 128), F32)
    for c in range(3):
        for first, half, at in ((low_first, 0, 0), (high_first, 1, 125)):
            if first is None:
                continue
            to = first + 3 * c
            moved = parts[c][:, half * 128 : half * 128 + 128]
            if (to - at) % 128:
                moved = pltpu.roll(moved, (to - at) % 128, axis=1)
            out = jnp.where((lane >= to) & (lane < to + 3), moved, out)
    return out


def pack_kernel(
    pos, node, far, geom, pline, fline, live, xdn, xup, ydn, yup, zdn, zup, geom_out, *copies
):
    for source, copy in zip((pos, node, far, pline, fline, live), copies, strict=True):
        copy[...] = source[...]
    for c in range(4):
        geom_out[c] = geom[:, c, :]
    fcol = column(fline[...].astype(F32), OUTER, OUTER).astype(I32)
    x, y, line = decode(fcol)
    tag = (line + 1).astype(F32)
    far_z = jnp.clip(far[OUTER:, :] - 3, 0, 255).astype(F32)
    for buf, mask in ((xdn, x < 0), (xup, x > 15), (ydn, y < 0), (yup, y > 15)):
        for c in range(3):
            buf[144 + 16 * c : 160 + 16 * c, :] = geom_out[c, OUTER:, :]
        buf[192:208, :] = far_z
        buf[208:224, :] = jnp.broadcast_to(jnp.where(mask, tag, 0.0), (OUTER, 256))
    for c in range(3):
        xdn[48 * c : 48 * c + 48, :] = pos[c, 0:48, :]
        xup[48 * c : 48 * c + 48, :] = pos[c, 208:256, :]
        for i in range(16):
            to = 48 * c + 3 * i
            ydn[to : to + 3, :] = pos[c, 16 * i : 16 * i + 3, :]
            yup[to : to + 3, :] = pos[c, 16 * i + 13 : 16 * i + 16, :]
    parts = [pos[c] for c in range(3)]
    zdn[0:256, :] = edge_lanes(parts, 0, None)
    zup[0:256, :] = edge_lanes(parts, None, 9)
    lines = jnp.broadcast_to(pline[...].astype(F32) + 1.0, (8, SLOTS))
    for buf in (zdn, zup):
        buf[256:264, :] = jnp.zeros((8, 128), F32)
        buf[256:264, 0:SLOTS] = lines


def z_index(far_outer):
    z = far_outer - 3
    below = z < 0
    above = z > 255
    index = jnp.where(below, z + 12, jnp.where(above, z - 256, 0))
    return index, below | above


def z_values(edges, far_outer):
    index, outside = z_index(far_outer)
    out = []
    for c in range(3):
        parts = [
            take128(edges, index[:, t * 128 : (t + 1) * 128] + 3 * c) for t in (0, 1)
        ]
        out.append(jnp.where(outside, jnp.concatenate(parts, axis=1), 0.0))
    return out


def onehots(node, hots, work):
    for t in (0, 1):
        work[t, 0:SLOTS, :] = node[:, t * 128 : (t + 1) * 128].astype(F32)
    places = iota((256, 256), 0).astype(F32).astype(BF16)
    one, zero = jnp.ones((), BF16), jnp.zeros((), BF16)
    for s in range(SLOTS):
        row = jnp.concatenate([work[t, s : s + 1, :] for t in (0, 1)], axis=1)
        index = jnp.broadcast_to(row.astype(BF16), (256, 256))
        hots[s] = jnp.where(places == index, one, zero)


def scatter(rows, hots, xs, ys):
    for r, value in enumerate(rows):
        for t in (0, 1):
            xs[t, pl.ds(r, SLOTS, stride=8), :] = value[:, t * 128 : (t + 1) * 128]
    for s in range(SLOTS):
        at = slice(8 * s, 8 * s + 8)
        x = jnp.concatenate([xs[0, at, :], xs[1, at, :]], axis=1)
        hi = x.astype(BF16).astype(F32)
        got = lax.dot_general(
            jnp.concatenate([hi, x - hi], axis=0).astype(BF16),
            hots[s],
            (((1,), (1,)), ((), ())),
            preferred_element_type=F32,
        )
        total = got[8:16] + got[0:8]
        ys[0, at, :] = total[:, :128]
        ys[1, at, :] = total[:, 128:]
    return [
        jnp.concatenate([ys[t, pl.ds(r, SLOTS, stride=8), :] for t in (0, 1)], axis=1)
        for r in range(len(rows))
    ]


def pair_tile(first, second):
    lane = iota((8, 128), 1)
    return jnp.where(lane == 18, first, jnp.where(lane == 19, second, 0.0))


def pack_edges(edges):
    lane = iota((8, 128), 1)
    out = jnp.zeros((8, 128), F32)
    for g in range(4):
        part = edges[8 * g : 8 * g + 8]
        part = pltpu.roll(part, 32 * g, axis=1) if g else part
        out = jnp.where((lane >= 32 * g) & (lane < 32 * g + 18), part, out)
    return out


def unpack_edges(tile):
    return jnp.concatenate(
        [tile] + [pltpu.roll(tile, 128 - 32 * g, axis=1) for g in range(1, 4)], axis=0
    )


def depth_of(gap, live):
    return jnp.where(iota((SLOTS, 256), 0) < live, jnp.maximum(-gap, 0.0), 0.0)


def total2(x):
    return jnp.sum(jnp.sum(x, axis=0, keepdims=True), axis=1, keepdims=True)


def first_mask(pline):
    shape = (SLOTS, SLOTS)
    row = jnp.broadcast_to(pline.astype(F32), shape)
    col = column(pline.astype(F32), 0, SLOTS)
    again = jnp.where((row == col) & (iota(shape, 1) < iota(shape, 0)), 1.0, 0.0)
    first = jnp.sum(again, axis=1, keepdims=True) == 0.0
    return jnp.broadcast_to(jnp.where(first, 1.0, 0.0), (SLOTS, 256))


def residual_of(near, first):
    square = near[0] * near[0] + near[1] * near[1] + near[2] * near[2]
    return total2(first[...] * square)


def own_index(far):
    z = far[...] - 3
    return jnp.clip(z, 0, 255), (z >= 0) & (z < 256)


def respond(normal, energy, node, far, geom, first, sel, requests, out, edge, change):
    edge[...] = pack_edges(edge_lanes(normal, 0, 9))
    lines = [pick(sel[...], normal[c]) for c in range(3)]
    residual = residual_of([v[0:SLOTS] for v in lines], first)
    tile = pair_tile(energy, residual)
    tile = jnp.concatenate([tile, tile], axis=1)
    for j in range(16):
        out[j, 0:OUTER, :] = jnp.zeros((OUTER, 256), F32)
        out[j, OUTER:24, :] = tile
    x, y, _ = position()
    me = x * 4 + y
    answers = []
    for d, buf in enumerate(requests):
        at = 2 * SLOTS + OUTER * d
        values = take_lanes([v[at : at + OUTER] for v in lines], buf[192:208, :].astype(I32))
        answer = jnp.zeros((OUTER, 256), F32)
        for c in range(3):
            answer = answer + buf[144 + 16 * c : 160 + 16 * c, :] * values[c]
        answers.append(answer)
    index, inside = own_index(far)
    near = take_lanes([v[0:SLOTS] for v in lines], node[...])
    other = take_lanes([v[SLOTS : 2 * SLOTS] for v in lines], index)
    moved = jnp.zeros((SLOTS, 256), F32)
    for c in range(3):
        moved = moved + geom[c] * (near[c] - jnp.where(inside, other[c], 0.0))
    change[...] = moved
    sides = ((me - 4, x > 0), (me + 4, x < 3), (me - 1, y > 0), (me + 1, y < 3))
    for answer, (to, there) in zip(answers, sides, strict=True):
        out[jnp.where(there, to, me), 0:OUTER, :] = answer


def first_kernel(
    pos,
    node,
    far,
    geom,
    pline,
    fline,
    live,
    xlo,
    xhi,
    ylo,
    yhi,
    zlo,
    zhi,
    out,
    edge,
    change,
    gap_out,
    normal_out,
    moved_out,
    sel_out,
    selz_out,
    inverse_out,
    hots,
    first,
    xs,
    ys,
):
    own = pline[...].astype(F32)
    near_col = column(own, 0, SLOTS)
    far_col = column(fline[...].astype(F32), 0, SLOTS)
    x, y, line = decode(far_col.astype(I32))
    inside = (x >= 0) & (x < 16) & (y >= 0) & (y < 16)
    local = jnp.where(inside, line, -2).astype(F32)
    xo, yo = x[OUTER:], y[OUTER:]
    face = jnp.where(xo < 0, (xo + 3) * 16 + yo, -1)
    face = jnp.where(xo > 15, 48 + (xo - 16) * 16 + yo, face)
    face = jnp.where(yo < 0, 96 + xo * 3 + yo + 3, face)
    face = jnp.where(yo > 15, 144 + xo * 3 + yo - 16, face)
    requests = (xlo, xhi, ylo, yhi)
    wanted = jnp.concatenate(
        [near_col, local] + [buf[208:224, 0:1] - 1.0 for buf in requests], axis=0
    )
    sel = hot(jnp.broadcast_to(own, (128, SLOTS)), wanted)
    sel_out[...] = sel
    selz = jnp.concatenate([zhi[256:257, 0:SLOTS], zlo[256:257, 0:SLOTS]], axis=1) - 1.0
    selz_out[...] = hot(jnp.broadcast_to(selz, (OUTER, 2 * SLOTS)), local[OUTER:])
    lines_f = iota((2 * SLOTS, 256), 1).astype(F32)
    sel_pos = hot(lines_f, jnp.concatenate([near_col, local], axis=0))
    sel_face = hot(iota((OUTER, 192), 1), face)
    lane = iota((256, 128), 1)
    edges = jnp.where(lane < 9, zhi[0:256, :], zlo[0:256, :])
    edges = pick(sel_pos[SLOTS + OUTER :], edges)
    ends = z_values(edges, far[OUTER:, :])
    index, within = own_index(far)
    gap = -geom[3]
    terms = jnp.zeros((SLOTS, 256), F32)
    for c in range(3):
        got = pick(sel_pos, pos[c])
        faces = jnp.concatenate([buf[48 * c : 48 * c + 48, :] for buf in requests], axis=0)
        outer = got[SLOTS + OUTER :] + pick(sel_face, faces)
        (near,) = take_lanes([got[0:SLOTS]], node[...])
        other = jnp.concatenate([got[SLOTS : SLOTS + OUTER], outer], axis=0)
        other = jnp.where(within, take_lanes([other], index)[0], 0.0)
        other = other + jnp.concatenate([jnp.zeros((OUTER, 256), F32), ends[c]], axis=0)
        terms = terms + geom[c] * (near - other)
    gap = terms + gap
    gap_out[...] = gap
    onehots(node, hots, xs)
    first[...] = first_mask(pline[...])
    depth = depth_of(gap, live[...])
    ones = jnp.where(iota((SLOTS, 256), 0) < live[...], 1.0, 0.0)
    got = scatter([depth * geom[c] for c in range(3)] + [ones], hots, xs, ys)
    inverse = 1.0 / (1.0 + pick(sel[0:SLOTS], got[3]))
    inverse_out[...] = inverse
    normal = [got[c] * inverse for c in range(3)]
    for c in range(3):
        normal_out[c] = normal[c]
        moved_out[c] = jnp.zeros((SLOTS, 256), F32)
    respond(
        normal, total2(depth * depth), node, far, geom, first, sel_out, requests, out, edge,
        change,
    )


def forward_kernel(got, edge, out):
    sums = jnp.sum(got[:, OUTER:24, 0:128], axis=0)
    lane = iota((8, 128), 1)
    sums = jnp.where((iota((8, 128), 0) == 0) & (lane > 17) & (lane < 20), sums, edge[...])
    for j in range(8):
        out[j] = sums


def update(gap, change, far, geom, got, gotz, selz):
    sums = jnp.sum(gotz[...], axis=0)
    energy = sums[0:1, 18:19]
    scale = RELAX * (1.0 / (1.0 + energy / N_PAIRS))
    x, y, k = position()
    me = x * 4 + y
    outer = jnp.zeros((OUTER, 256), F32)
    for to, there in ((me - 4, x > 0), (me + 4, x < 3), (me - 1, y > 0), (me + 1, y < 3)):
        reply = got[jnp.where(there, to, me), 0:OUTER, :]
        outer = outer + jnp.where(there, reply, 0.0)
    lane = iota((SLOTS, 128), 1)
    above = unpack_edges(gotz[jnp.minimum(k + 1, 7)])
    above = jnp.where((lane < 9) & (k < 7), above, 0.0)
    below = unpack_edges(gotz[jnp.maximum(k - 1, 0)])
    below = jnp.where((lane > 8) & (lane < 18) & (k > 0), below, 0.0)
    ends = z_values(
        pick(selz[...], jnp.concatenate([above, below], axis=0)), far[OUTER:, :]
    )
    for c in range(3):
        outer = outer + geom[c, OUTER:, :] * ends[c]
    full = change[...] - jnp.concatenate([jnp.zeros((OUTER, 256), F32), outer], axis=0)
    return sums, scale, gap[...] + scale * full


def sweep_kernel(
    last, gap, change, normal, moved, inverse, node, far, geom, first, live, sel, selz, hots,
    got, gotz, *rest,
):
    if last:
        out, sums_out, normal_out, moved_out, xs, ys = rest
    else:
        xlo, xhi, ylo, yhi = rest[:4]
        out, edge, change_out, gap_out, sums_out, normal_out, moved_out, xs, ys = rest[4:]
    sums, scale, fresh = update(gap, change, far, geom, got, gotz, selz)
    sums_out[...] = sums
    for c in range(3):
        moved_out[c] = moved[c] + scale * normal[c]
    depth = depth_of(fresh, live[...])
    energy = total2(depth * depth)
    found = scatter([depth * geom[c] for c in range(3)], hots, xs, ys)
    fresh_normal = [found[c] * inverse[...] for c in range(3)]
    for c in range(3):
        normal_out[c] = fresh_normal[c]
    if last:
        lines = [pick(sel[0:SLOTS, :], fresh_normal[c]) for c in range(3)]
        tile = pair_tile(energy, residual_of(lines, first))
        out[...] = jnp.broadcast_to(tile[0:1, :], (128, 128))
    else:
        gap_out[...] = fresh
        respond(
            fresh_normal, energy, node, far, geom, first, sel, (xlo, xhi, ylo, yhi), out, edge,
            change_out,
        )


def last_kernel(pos, normal, moved, pline, got, s0, s1, s2, s3, out, history):
    sums = jnp.sum(got[...], axis=0, keepdims=True)
    every = [s[0:1, :] for s in (s0, s1, s2, s3)] + [sums]
    scales = [RELAX * (1.0 / (1.0 + s[:, 18:19] / N_PAIRS)) for s in every]
    sel = hot(iota((256, SLOTS), 0), jnp.broadcast_to(pline[...], (256, SLOTS)))
    for c in range(3):
        out[c] = pos[c] + pick(sel, moved[c] + scales[-1] * normal[c])
    for t in range(SWEEPS):
        residual = scales[t] * scales[t] * every[t][:, 19:20]
        history[0:1, t : t + 1] = jnp.sqrt(1.0 + every[t][:, 18:19] / PAIRS_SLOTS)
        history[1:2, t : t + 1] = jnp.sqrt(1.0 + residual / NODES_BLK)


def position():
    return lax.axis_index("gx"), lax.axis_index("gy"), lax.axis_index(GZ)


def call(kernel, outs, args, scratch=(), inputs=False):
    vmem = pl.BlockSpec(memory_space=pltpu.VMEM)
    return pl.pallas_call(
        kernel,
        out_shape=outs,
        in_specs=[vmem] * len(args),
        out_specs=[vmem] * len(outs) if isinstance(outs, list) else vmem,
        scratch_shapes=list(scratch),
        compiler_params=pltpu.CompilerParams(vmem_limit_bytes=12 * 2**20),
    )(*(args if inputs else [in_vmem(x) for x in args]))


def shape(*dims, dtype=F32):
    return pltpu.VMEM(dims, dtype)


def in_vmem(x):
    return pltpu.with_memory_space_constraint(x, pltpu.VMEM)


def shift(x, axis, up):
    count = lax.axis_size(axis)
    pairs = [(i, i + 1) for i in range(count - 1)]
    return lax.ppermute(x, axis, pairs if up else [(b, a) for a, b in pairs])


def local(positions, pair_node, pair_line, pair_far, far_line, pair_geom, live_blocks):
    pos = positions.reshape(3, 256, 256)
    node = pair_node.reshape(SLOTS, 256)
    far = pair_far.reshape(SLOTS, 256)
    geom = pair_geom.reshape(SLOTS, 4, 256)
    pline = pair_line.reshape(1, SLOTS)
    fline = far_line.reshape(1, SLOTS)
    live = live_blocks.reshape(1, 1)
    work = [pltpu.VMEM((2, 256, 128), F32)] * 2

    face, ends = shape(224, 256), shape(264, 128)
    flat = shape(SLOTS, 256)
    flat_i = shape(SLOTS, 256, dtype=I32)
    few = shape(1, SLOTS, dtype=I32)
    packed = call(
        pack_kernel,
        [face] * 4
        + [ends] * 2
        + [shape(4, SLOTS, 256), shape(3, 256, 256), flat_i, flat_i, few, few]
        + [shape(1, 1, dtype=I32)],
        [pos, node, far, geom, pline, fline, live],
        inputs=True,
    )
    xdn, xup, ydn, yup, zdn, zup, geom, pos, node, far, pline, fline, live = packed
    requests = [
        shift(xup, "gx", True),
        shift(xdn, "gx", False),
        shift(yup, "gy", True),
        shift(ydn, "gy", False),
    ]
    zlo = shift(zup, GZ, True)
    zhi = shift(zdn, GZ, False)
    triple = shape(3, SLOTS, 256)
    outbound, edges = shape(16, 24, 256), shape(8, 128)
    out, edge, change, gap, normal, moved, sel, selz, inverse, hots, first = call(
        first_kernel,
        [
            outbound,
            edges,
            flat,
            flat,
            triple,
            triple,
            shape(128, SLOTS, dtype=BF16),
            shape(OUTER, 2 * SLOTS, dtype=BF16),
            flat,
            shape(SLOTS, 256, 256, dtype=BF16),
            flat,
        ],
        [pos, node, far, geom, pline, fline, live, *requests, zlo, zhi],
        work,
    )
    totals = []
    for t in range(1, SWEEPS):
        got = lax.all_to_all(out, XY, 0, 0, tiled=True)
        out = call(forward_kernel, shape(8, 8, 128), [got, edge])
        gotz = lax.all_to_all(out, GZ, 0, 0, tiled=True)
        last = t + 1 == SWEEPS
        args = [
            gap, change, normal, moved, inverse, node, far, geom, first, live, sel, selz,
            hots, got, gotz,
        ]
        sums_shape = shape(8, 128)
        if last:
            out, sums, normal, moved = call(
                functools.partial(sweep_kernel, True),
                [shape(128, 128), sums_shape, triple, triple],
                args,
                work,
            )
        else:
            out, edge, change, gap, sums, normal, moved = call(
                functools.partial(sweep_kernel, False),
                [outbound, edges, flat, flat, sums_shape, triple, triple],
                args + requests,
                work,
            )
        totals.append(sums)
    got = lax.all_to_all(out, ALL, 0, 0, tiled=True)
    corrected, history = call(
        last_kernel,
        [jax.ShapeDtypeStruct((3, 256, 256), F32), jax.ShapeDtypeStruct((2, SWEEPS), F32)],
        [pos, normal, moved, pline, got, *totals],
    )
    return corrected.reshape(positions.shape), history


def solution(mesh):
    finer = Mesh(
        mesh.devices.reshape(mesh.shape["gx"], mesh.shape["gy"], 4, 2), ("gx", "gy", "gz_0", "gz_1")
    )
    placed = (
        P(None, "gx", "gy", GZ),
        P("gx", "gy", GZ, None, None),
        P("gx", "gy", GZ, None),
        P("gx", "gy", GZ, None, None),
        P("gx", "gy", GZ, None),
        P("gx", "gy", GZ, None, None, None),
        P("gx", "gy", GZ),
    )
    return jax.shard_map(
        local,
        mesh=finer,
        in_specs=placed,
        out_specs=(P(None, "gx", "gy", GZ), P()),
        check_vma=False,
    )
```

```python
import functools

import jax
import jax.numpy as jnp
from jax import lax
from jax.experimental import pallas as pl
from jax.experimental.pallas import tpu as pltpu
from jax.sharding import Mesh
from jax.sharding import PartitionSpec as P

SWEEPS = 5
RELAX = 0.9
XY = ("gx", "gy")
GZ = ("gz_0", "gz_1")
ALL = ("gx", "gy", "gz_0", "gz_1")
F32 = jnp.float32
BF16 = jnp.bfloat16
I32 = jnp.int32
SLOTS = 32
OUTER = 16
N_PAIRS = 1048576
NODES_BLK = 65536
PAIRS_SLOTS = 8192


def iota(shape, dim):
    return lax.broadcasted_iota(I32, shape, dim)


def pick(sel, x):
    hi = x.astype(BF16)
    mid = (x - hi.astype(F32)).astype(BF16)
    dot = functools.partial(jnp.dot, preferred_element_type=F32)
    return dot(sel, mid) + dot(sel, hi)


def hot(a, b):
    return jnp.where(a == b, 1.0, 0.0).astype(BF16)


def column(row, first, count):
    shape = (count, row.shape[1])
    chosen = iota(shape, 0) + first == iota(shape, 1)
    return jnp.sum(jnp.where(chosen, jnp.broadcast_to(row, shape), 0.0), axis=1, keepdims=True)


def take128(x, index):
    return jnp.take_along_axis(x, index, axis=1, mode="promise_in_bounds")


def take_lanes(xs, index):
    columns = [[] for _ in xs]
    for t in (0, 1):
        cut = index[:, t * 128 : (t + 1) * 128]
        low = cut & 127
        high = cut > 127
        rows = [[] for _ in xs]
        for g in range(0, index.shape[0], 8):
            at = slice(g, g + 8)
            for x, row in zip(xs, rows, strict=True):
                a = take128(x[at, :128], low[at])
                b = take128(x[at, 128:], low[at])
                row.append(jnp.where(high[at], b, a))
        for column_parts, row in zip(columns, rows, strict=True):
            column_parts.append(jnp.concatenate(row, axis=0))
    return [jnp.concatenate(parts, axis=1) for parts in columns]


def decode(far_line):
    x = (far_line * 2979) >> 16
    y = far_line - 22 * x - 3
    x = x - 3
    return x, y, (x & 15) * 16 + (y & 15)


def edge_lanes(parts, low_first, high_first):
    lane = iota((parts[0].shape[0], 128), 1)
    out = jnp.zeros((parts[0].shape[0], 128), F32)
    for c in range(3):
        for first, half, at in ((low_first, 0, 0), (high_first, 1, 125)):
            if first is None:
                continue
            to = first + 3 * c
            moved = parts[c][:, half * 128 : half * 128 + 128]
            if (to - at) % 128:
                moved = pltpu.roll(moved, (to - at) % 128, axis=1)
            out = jnp.where((lane >= to) & (lane < to + 3), moved, out)
    return out


def pack_rows(tall):
    lane = iota((SLOTS, 128), 1)
    out = jnp.zeros((SLOTS, 128), F32)
    for g in range(8):
        part = tall[32 * g : 32 * g + 32]
        part = pltpu.roll(part, 16 * g, axis=1) if g else part
        out = jnp.where((lane >= 16 * g) & (lane < 16 * g + 16), part, out)
    return out


def unpack_rows(flat):
    return jnp.concatenate(
        [flat] + [pltpu.roll(flat, 128 - 16 * g, axis=1) for g in range(1, 8)], axis=0
    )


def pack_kernel(
    pos_in, node_in, far_in, geom_in, pline_in, fline_in, live_in,
    xdn, xup, ydn, yup, zdn, zup, geom, pos, node, far, pline, fline, live,
    geom_raw, sems,
):
    copies = [
        pltpu.make_async_copy(source, target, sems.at[n])
        for n, (source, target) in enumerate(
            (
                (fline_in, fline),
                (far_in, far),
                (geom_in, geom_raw),
                (pline_in, pline),
                (pos_in, pos),
                (node_in, node),
                (live_in, live),
            )
        )
    ]
    for copy in copies:
        copy.start()
    for copy in copies[:4]:
        copy.wait()
    for c in range(4):
        geom[c] = geom_raw[:, c, :]
    fcol = column(fline[...].astype(F32), OUTER, OUTER).astype(I32)
    x, y, line = decode(fcol)
    tag = (line + 1).astype(F32)
    far_z = jnp.clip(far[OUTER:, :] - 3, 0, 255).astype(F32)
    for buf, mask in ((xdn, x < 0), (xup, x > 15), (ydn, y < 0), (yup, y > 15)):
        for c in range(3):
            buf[144 + 16 * c : 160 + 16 * c, :] = geom[c, OUTER:, :]
        buf[192:208, :] = far_z
        buf[208:224, :] = jnp.broadcast_to(jnp.where(mask, tag, 0.0), (OUTER, 256))
    lines = jnp.broadcast_to(pline[...].astype(F32) + 1.0, (8, SLOTS))
    for buf in (zdn, zup):
        buf[32:40, :] = jnp.zeros((8, 128), F32)
        buf[32:40, 0:SLOTS] = lines
    for copy in copies[4:]:
        copy.wait()
    for c in range(3):
        xdn[48 * c : 48 * c + 48, :] = pos[c, 0:48, :]
        xup[48 * c : 48 * c + 48, :] = pos[c, 208:256, :]
        for i in range(16):
            to = 48 * c + 3 * i
            ydn[to : to + 3, :] = pos[c, 16 * i : 16 * i + 3, :]
            yup[to : to + 3, :] = pos[c, 16 * i + 13 : 16 * i + 16, :]
    parts = [pos[c] for c in range(3)]
    zdn[0:32, :] = pack_rows(edge_lanes(parts, 0, None))
    zup[0:32, :] = pack_rows(edge_lanes(parts, None, 0))


def z_index(far_outer):
    z = far_outer - 3
    below = z < 0
    above = z > 255
    index = jnp.where(below, z + 12, jnp.where(above, z - 256, 0))
    return index, below | above


def z_values(edges, far_outer):
    index, outside = z_index(far_outer)
    out = []
    for c in range(3):
        parts = [
            take128(edges, index[:, t * 128 : (t + 1) * 128] + 3 * c) for t in (0, 1)
        ]
        out.append(jnp.where(outside, jnp.concatenate(parts, axis=1), 0.0))
    return out


def onehots(node, hots, work):
    for t in (0, 1):
        work[t, 0:SLOTS, :] = node[:, t * 128 : (t + 1) * 128].astype(F32)
    places = iota((256, 256), 0).astype(F32).astype(BF16)
    one, zero = jnp.ones((), BF16), jnp.zeros((), BF16)
    for s in range(SLOTS):
        row = jnp.concatenate([work[t, s : s + 1, :] for t in (0, 1)], axis=1)
        index = jnp.broadcast_to(row.astype(BF16), (256, 256))
        hots[s] = jnp.where(places == index, one, zero)


def scatter(rows, hots, xs, ys):
    for r, value in enumerate(rows):
        for t in (0, 1):
            xs[t, pl.ds(r, SLOTS, stride=8), :] = value[:, t * 128 : (t + 1) * 128]
    for s in range(SLOTS):
        at = slice(8 * s, 8 * s + 8)
        x = jnp.concatenate([xs[0, at, :], xs[1, at, :]], axis=1)
        hi = x.astype(BF16).astype(F32)
        got = lax.dot_general(
            jnp.concatenate([hi, x - hi], axis=0).astype(BF16),
            hots[s],
            (((1,), (1,)), ((), ())),
            preferred_element_type=F32,
        )
        total = got[8:16] + got[0:8]
        ys[0, at, :] = total[:, :128]
        ys[1, at, :] = total[:, 128:]
    return [
        jnp.concatenate([ys[t, pl.ds(r, SLOTS, stride=8), :] for t in (0, 1)], axis=1)
        for r in range(len(rows))
    ]


def pair_tile(first, second):
    lane = iota((8, 128), 1)
    return jnp.where(lane == 18, first, jnp.where(lane == 19, second, 0.0))


def pack_edges(edges):
    lane = iota((8, 128), 1)
    out = jnp.zeros((8, 128), F32)
    for g in range(4):
        part = edges[8 * g : 8 * g + 8]
        part = pltpu.roll(part, 32 * g, axis=1) if g else part
        out = jnp.where((lane >= 32 * g) & (lane < 32 * g + 18), part, out)
    return out


def unpack_edges(tile):
    return jnp.concatenate(
        [tile] + [pltpu.roll(tile, 128 - 32 * g, axis=1) for g in range(1, 4)], axis=0
    )


def depth_of(gap, live):
    return jnp.where(iota((SLOTS, 256), 0) < live, jnp.maximum(-gap, 0.0), 0.0)


def total2(x):
    return jnp.sum(jnp.sum(x, axis=0, keepdims=True), axis=1, keepdims=True)


def first_mask(pline):
    shape = (SLOTS, SLOTS)
    row = jnp.broadcast_to(pline.astype(F32), shape)
    col = column(pline.astype(F32), 0, SLOTS)
    again = jnp.where((row == col) & (iota(shape, 1) < iota(shape, 0)), 1.0, 0.0)
    first = jnp.sum(again, axis=1, keepdims=True) == 0.0
    return jnp.broadcast_to(jnp.where(first, 1.0, 0.0), (SLOTS, 256))


def residual_of(near, first):
    square = near[0] * near[0] + near[1] * near[1] + near[2] * near[2]
    return total2(first[...] * square)


def own_index(far):
    z = far[...] - 3
    return jnp.clip(z, 0, 255), (z >= 0) & (z < 256)


def respond(normal, energy, node, far, geom, first, sel, requests, out, edge, change):
    edge[...] = pack_edges(edge_lanes(normal, 0, 9))
    lines = [pick(sel[...], normal[c]) for c in range(3)]
    residual = residual_of([v[0:SLOTS] for v in lines], first)
    tile = pair_tile(energy, residual)
    for j in range(16):
        out[j, 0:32, :] = jnp.zeros((32, 128), F32)
        out[j, 32:40, :] = tile
    x, y, _ = position()
    me = x * 4 + y
    answers = []
    for d, buf in enumerate(requests):
        at = 2 * SLOTS + OUTER * d
        values = take_lanes([v[at : at + OUTER] for v in lines], buf[192:208, :].astype(I32))
        answer = jnp.zeros((OUTER, 256), F32)
        for c in range(3):
            answer = answer + buf[144 + 16 * c : 160 + 16 * c, :] * values[c]
        answers.append(answer)
    index, inside = own_index(far)
    near = take_lanes([v[0:SLOTS] for v in lines], node[...])
    other = take_lanes([v[SLOTS : 2 * SLOTS] for v in lines], index)
    moved = jnp.zeros((SLOTS, 256), F32)
    for c in range(3):
        moved = moved + geom[c] * (near[c] - jnp.where(inside, other[c], 0.0))
    change[...] = moved
    sides = ((me - 4, x > 0), (me + 4, x < 3), (me - 1, y > 0), (me + 1, y < 3))
    for answer, (to, there) in zip(answers, sides, strict=True):
        out[jnp.where(there, to, me), 0:OUTER, :] = answer[:, :128]
        out[jnp.where(there, to, me), OUTER:32, :] = answer[:, 128:]


def base_kernel(
    pos, node, far, geom, pline, fline, live,
    gap_out, own_out, face_out, inverse_out, hots, first, xs, ys,
):
    onehots(node, hots, xs)
    first[...] = first_mask(pline[...])
    own = pline[...].astype(F32)
    near_col = column(own, 0, SLOTS)
    far_col = column(fline[...].astype(F32), 0, SLOTS)
    x, y, line = decode(far_col.astype(I32))
    inside = (x >= 0) & (x < 16) & (y >= 0) & (y < 16)
    local = jnp.where(inside, line, -2).astype(F32)
    both = jnp.concatenate([near_col, local], axis=0)
    own_out[...] = jnp.broadcast_to(both, (2 * SLOTS, 128))
    xo, yo = x[OUTER:], y[OUTER:]
    face = jnp.where(xo < 0, (xo + 3) * 16 + yo, -1)
    face = jnp.where(xo > 15, 48 + (xo - 16) * 16 + yo, face)
    face = jnp.where(yo < 0, 96 + xo * 3 + yo + 3, face)
    face = jnp.where(yo > 15, 144 + xo * 3 + yo - 16, face)
    face_out[...] = hot(iota((OUTER, 192), 1), face)
    ones = jnp.where(iota((SLOTS, 256), 0) < live[...], 1.0, 0.0)
    (counts,) = scatter([ones], hots, xs, ys)
    same = hot(jnp.broadcast_to(own, (SLOTS, SLOTS)), near_col)
    inverse_out[...] = 1.0 / (1.0 + pick(same, counts))
    sel = hot(iota((2 * SLOTS, 256), 1).astype(F32), both)
    index, within = own_index(far)
    got = [pick(sel, pos[c]) for c in range(3)]
    near = take_lanes([v[0:SLOTS] for v in got], node[...])
    other = take_lanes([v[SLOTS:] for v in got], index)
    gap = jnp.zeros((SLOTS, 256), F32)
    for c in range(3):
        gap = gap + geom[c] * (near[c] - jnp.where(within, other[c], 0.0))
    gap_out[...] = gap - geom[3]


def first_kernel(
    gap_in, own, face, inverse, far, geom, pline, live, node, hots, first,
    xlo, xhi, ylo, yhi, zlo, zhi,
    out, edge, change, gap_out, normal_out, moved_out, sel_out, selz_out, xs, ys,
):
    requests = (xlo, xhi, ylo, yhi)
    wanted = jnp.concatenate(
        [own[:, 0:1]] + [buf[208:224, 0:1] - 1.0 for buf in requests], axis=0
    )
    sel_out[...] = hot(jnp.broadcast_to(pline[...].astype(F32), (128, SLOTS)), wanted)
    local = own[SLOTS + OUTER :, 0:1]
    selz = jnp.concatenate([zhi[32:33, 0:SLOTS], zlo[32:33, 0:SLOTS]], axis=1) - 1.0
    selz_out[...] = hot(jnp.broadcast_to(selz, (OUTER, 2 * SLOTS)), local)
    edges = jnp.where(
        iota((256, 128), 1) < 9,
        unpack_rows(zhi[0:32, :]),
        pltpu.roll(unpack_rows(zlo[0:32, :]), 9, axis=1),
    )
    sel = hot(iota((OUTER, 256), 1).astype(F32), local)
    ends = z_values(pick(sel, edges), far[OUTER:, :])
    index, within = own_index(far)
    faces = [
        pick(face[...], jnp.concatenate([buf[48 * c : 48 * c + 48, :] for buf in requests], axis=0))
        for c in range(3)
    ]
    faces = take_lanes(faces, index[OUTER:])
    outer = jnp.zeros((OUTER, 256), F32)
    for c in range(3):
        outer = outer + geom[c, OUTER:, :] * (
            jnp.where(within[OUTER:], faces[c], 0.0) + ends[c]
        )
    gap = gap_in[...] - jnp.concatenate([jnp.zeros((OUTER, 256), F32), outer], axis=0)
    gap_out[...] = gap
    depth = depth_of(gap, live[...])
    got = scatter([depth * geom[c] for c in range(3)], hots, xs, ys)
    normal = [got[c] * inverse[...] for c in range(3)]
    for c in range(3):
        normal_out[c] = normal[c]
        moved_out[c] = jnp.zeros((SLOTS, 256), F32)
    respond(
        normal, total2(depth * depth), node, far, geom, first, sel_out, requests, out, edge,
        change,
    )


def forward_kernel(got, edge, out):
    sums = jnp.sum(got[:, 32:40, :], axis=0)
    lane = iota((8, 128), 1)
    sums = jnp.where((iota((8, 128), 0) == 0) & (lane > 17) & (lane < 20), sums, edge[...])
    for j in range(8):
        out[j] = sums


def update(gap, change, far, geom, got, gotz, selz):
    sums = jnp.sum(gotz[...], axis=0)
    energy = sums[0:1, 18:19]
    scale = RELAX * (1.0 / (1.0 + energy / N_PAIRS))
    x, y, k = position()
    me = x * 4 + y
    outer = jnp.zeros((OUTER, 256), F32)
    for to, there in ((me - 4, x > 0), (me + 4, x < 3), (me - 1, y > 0), (me + 1, y < 3)):
        at = jnp.where(there, to, me)
        reply = jnp.concatenate([got[at, 0:OUTER, :], got[at, OUTER:32, :]], axis=1)
        outer = outer + jnp.where(there, reply, 0.0)
    lane = iota((SLOTS, 128), 1)
    above = unpack_edges(gotz[jnp.minimum(k + 1, 7)])
    above = jnp.where((lane < 9) & (k < 7), above, 0.0)
    below = unpack_edges(gotz[jnp.maximum(k - 1, 0)])
    below = jnp.where((lane > 8) & (lane < 18) & (k > 0), below, 0.0)
    ends = z_values(
        pick(selz[...], jnp.concatenate([above, below], axis=0)), far[OUTER:, :]
    )
    for c in range(3):
        outer = outer + geom[c, OUTER:, :] * ends[c]
    full = change[...] - jnp.concatenate([jnp.zeros((OUTER, 256), F32), outer], axis=0)
    return sums, scale, gap[...] + scale * full


def sweep_kernel(
    last, gap, change, normal, moved, inverse, node, far, geom, first, live, sel, selz, hots,
    got, gotz, *rest,
):
    if last:
        out, sums_out, normal_out, moved_out, xs, ys = rest
    else:
        xlo, xhi, ylo, yhi = rest[:4]
        out, edge, change_out, gap_out, sums_out, normal_out, moved_out, xs, ys = rest[4:]
    sums, scale, fresh = update(gap, change, far, geom, got, gotz, selz)
    sums_out[...] = sums
    for c in range(3):
        moved_out[c] = moved[c] + scale * normal[c]
    depth = depth_of(fresh, live[...])
    energy = total2(depth * depth)
    found = scatter([depth * geom[c] for c in range(3)], hots, xs, ys)
    fresh_normal = [found[c] * inverse[...] for c in range(3)]
    for c in range(3):
        normal_out[c] = fresh_normal[c]
    if last:
        lines = [pick(sel[0:SLOTS, :], fresh_normal[c]) for c in range(3)]
        tile = pair_tile(energy, residual_of(lines, first))
        out[...] = jnp.broadcast_to(tile[0:1, :], (128, 128))
    else:
        gap_out[...] = fresh
        respond(
            fresh_normal, energy, node, far, geom, first, sel, (xlo, xhi, ylo, yhi), out, edge,
            change_out,
        )


def last_kernel(pos, normal, moved, pline, got, s0, s1, s2, s3, out, history):
    sums = jnp.sum(got[...], axis=0, keepdims=True)
    every = [s[0:1, :] for s in (s0, s1, s2, s3)] + [sums]
    scales = [RELAX * (1.0 / (1.0 + s[:, 18:19] / N_PAIRS)) for s in every]
    sel = hot(iota((256, SLOTS), 0), jnp.broadcast_to(pline[...], (256, SLOTS)))
    for c in range(3):
        out[c] = pos[c] + pick(sel, moved[c] + scales[-1] * normal[c])
    for t in range(SWEEPS):
        residual = scales[t] * scales[t] * every[t][:, 19:20]
        history[0:1, t : t + 1] = jnp.sqrt(1.0 + every[t][:, 18:19] / PAIRS_SLOTS)
        history[1:2, t : t + 1] = jnp.sqrt(1.0 + residual / NODES_BLK)


def position():
    return lax.axis_index("gx"), lax.axis_index("gy"), lax.axis_index(GZ)


within = pltpu.with_memory_space_constraint


def call(kernel, outs, args, scratch=(), inputs=False):
    vmem = pl.BlockSpec(memory_space=pltpu.VMEM)
    hbm = pl.BlockSpec(memory_space=pltpu.HBM)
    return pl.pallas_call(
        kernel,
        out_shape=outs,
        in_specs=[hbm if inputs else vmem] * len(args),
        out_specs=[vmem] * len(outs) if isinstance(outs, list) else vmem,
        scratch_shapes=list(scratch),
        compiler_params=pltpu.CompilerParams(vmem_limit_bytes=12 * 2**20),
    )(*(args if inputs else [within(x, pltpu.VMEM) for x in args]))


def shape(*dims, dtype=F32):
    return pltpu.VMEM(dims, dtype)


def shift(x, axis, up):
    count = lax.axis_size(axis)
    pairs = [(i, i + 1) for i in range(count - 1)]
    return lax.ppermute(x, axis, pairs if up else [(b, a) for a, b in pairs])


def local(positions, pair_node, pair_line, pair_far, far_line, pair_geom, live_blocks):
    pos = positions.reshape(3, 256, 256)
    node = pair_node.reshape(SLOTS, 256)
    far = pair_far.reshape(SLOTS, 256)
    geom = pair_geom.reshape(SLOTS, 4, 256)
    pline = pair_line.reshape(1, SLOTS)
    fline = far_line.reshape(1, SLOTS)
    live = live_blocks.reshape(1, 1)
    work = [pltpu.VMEM((2, 256, 128), F32)] * 2

    face, ends = shape(224, 256), shape(40, 128)
    flat = shape(SLOTS, 256)
    flat_i = shape(SLOTS, 256, dtype=I32)
    few = shape(1, SLOTS, dtype=I32)
    packed = call(
        pack_kernel,
        [face] * 4
        + [ends] * 2
        + [shape(4, SLOTS, 256), shape(3, 256, 256), flat_i, flat_i, few, few]
        + [shape(1, 1, dtype=I32)],
        [within(x, pltpu.HBM) for x in (pos, node, far, geom, pline, fline)] + [live],
        [pltpu.VMEM((SLOTS, 4, 256), F32), pltpu.SemaphoreType.DMA((7,))],
        inputs=True,
    )
    xdn, xup, ydn, yup, zdn, zup, geom, pos, node, far, pline, fline, live = packed
    requests = [
        shift(xup, "gx", True),
        shift(xdn, "gx", False),
        shift(yup, "gy", True),
        shift(ydn, "gy", False),
    ]
    zlo = shift(zup, GZ, True)
    zhi = shift(zdn, GZ, False)
    triple = shape(3, SLOTS, 256)
    outbound, edges = shape(16, 40, 128), shape(8, 128)
    gap, own, face, inverse, hots, first = call(
        base_kernel,
        [
            flat,
            shape(2 * SLOTS, 128),
            shape(OUTER, 192, dtype=BF16),
            flat,
            shape(SLOTS, 256, 256, dtype=BF16),
            flat,
        ],
        [pos, node, far, geom, pline, fline, live],
        work,
    )
    out, edge, change, gap, normal, moved, sel, selz = call(
        first_kernel,
        [
            outbound,
            edges,
            flat,
            flat,
            triple,
            triple,
            shape(128, SLOTS, dtype=BF16),
            shape(OUTER, 2 * SLOTS, dtype=BF16),
        ],
        [gap, own, face, inverse, far, geom, pline, live, node, hots, first]
        + requests
        + [zlo, zhi],
        work,
    )
    totals = []
    for t in range(1, SWEEPS):
        got = lax.all_to_all(out, XY, 0, 0, tiled=True)
        out = call(forward_kernel, shape(8, 8, 128), [got, edge])
        gotz = lax.all_to_all(out, GZ, 0, 0, tiled=True)
        last = t + 1 == SWEEPS
        args = [
            gap, change, normal, moved, inverse, node, far, geom, first, live, sel, selz,
            hots, got, gotz,
        ]
        sums_shape = shape(8, 128)
        if last:
            out, sums, normal, moved = call(
                functools.partial(sweep_kernel, True),
                [shape(128, 128), sums_shape, triple, triple],
                args,
                work,
            )
        else:
            out, edge, change, gap, sums, normal, moved = call(
                functools.partial(sweep_kernel, False),
                [outbound, edges, flat, flat, sums_shape, triple, triple],
                args + requests,
                work,
            )
        totals.append(sums)
    got = lax.all_to_all(out, ALL, 0, 0, tiled=True)
    corrected, history = call(
        last_kernel,
        [jax.ShapeDtypeStruct((3, 256, 256), F32), jax.ShapeDtypeStruct((2, SWEEPS), F32)],
        [pos, normal, moved, pline, got, *totals],
    )
    return corrected.reshape(positions.shape), history


def solution(mesh):
    finer = Mesh(
        mesh.devices.reshape(mesh.shape["gx"], mesh.shape["gy"], 4, 2), ("gx", "gy", "gz_0", "gz_1")
    )
    placed = (
        P(None, "gx", "gy", GZ),
        P("gx", "gy", GZ, None, None),
        P("gx", "gy", GZ, None),
        P("gx", "gy", GZ, None, None),
        P("gx", "gy", GZ, None),
        P("gx", "gy", GZ, None, None, None),
        P("gx", "gy", GZ),
    )
    return jax.shard_map(
        local,
        mesh=finer,
        in_specs=placed,
        out_specs=(P(None, "gx", "gy", GZ), P()),
        check_vma=False,
    )
```

```python
import functools

import jax
import jax.numpy as jnp
from jax import lax
from jax.experimental import pallas as pl
from jax.experimental.pallas import tpu as pltpu
from jax.sharding import Mesh
from jax.sharding import PartitionSpec as P

SWEEPS = 5
RELAX = 0.9
XY = ("gx", "gy")
GZ = ("gz_0", "gz_1")
ALL = ("gx", "gy", "gz_0", "gz_1")
F32 = jnp.float32
BF16 = jnp.bfloat16
I32 = jnp.int32
SLOTS = 32
OUTER = 16
N_PAIRS = 1048576
NODES_BLK = 65536
PAIRS_SLOTS = 8192


def iota(shape, dim):
    return lax.broadcasted_iota(I32, shape, dim)


def pick(sel, x):
    hi = x.astype(BF16)
    mid = (x - hi.astype(F32)).astype(BF16)
    dot = functools.partial(jnp.dot, preferred_element_type=F32)
    if sel.shape[1] == 2 * x.shape[0]:
        return dot(sel, jnp.concatenate([hi, mid], axis=0))
    return dot(sel, mid) + dot(sel, hi)


def hot(a, b):
    return jnp.where(a == b, 1.0, 0.0).astype(BF16)


def twice(row):
    return jnp.concatenate([row, row], axis=1)


def column(row, first, count):
    shape = (count, row.shape[1])
    chosen = iota(shape, 0) + first == iota(shape, 1)
    return jnp.sum(jnp.where(chosen, jnp.broadcast_to(row, shape), 0.0), axis=1, keepdims=True)


def take128(x, index):
    return jnp.take_along_axis(x, index, axis=1, mode="promise_in_bounds")


def take_lanes(xs, index):
    columns = [[] for _ in xs]
    for t in (0, 1):
        cut = index[:, t * 128 : (t + 1) * 128]
        low = cut & 127
        high = cut > 127
        rows = [[] for _ in xs]
        for g in range(0, index.shape[0], 8):
            at = slice(g, g + 8)
            for x, row in zip(xs, rows, strict=True):
                a = take128(x[at, :128], low[at])
                b = take128(x[at, 128:], low[at])
                row.append(jnp.where(high[at], b, a))
        for column_parts, row in zip(columns, rows, strict=True):
            column_parts.append(jnp.concatenate(row, axis=0))
    return [jnp.concatenate(parts, axis=1) for parts in columns]


def decode(far_line):
    x = (far_line * 2979) >> 16
    y = far_line - 22 * x - 3
    x = x - 3
    return x, y, (x & 15) * 16 + (y & 15)


def edge_lanes(parts, low_first, high_first):
    lane = iota((parts[0].shape[0], 128), 1)
    out = jnp.zeros((parts[0].shape[0], 128), F32)
    for c in range(3):
        for first, half, at in ((low_first, 0, 0), (high_first, 1, 125)):
            if first is None:
                continue
            to = first + 3 * c
            moved = parts[c][:, half * 128 : half * 128 + 128]
            if (to - at) % 128:
                moved = pltpu.roll(moved, (to - at) % 128, axis=1)
            out = jnp.where((lane >= to) & (lane < to + 3), moved, out)
    return out


def pack_rows(tall):
    lane = iota((SLOTS, 128), 1)
    out = jnp.zeros((SLOTS, 128), F32)
    for g in range(8):
        part = tall[32 * g : 32 * g + 32]
        part = pltpu.roll(part, 16 * g, axis=1) if g else part
        out = jnp.where((lane >= 16 * g) & (lane < 16 * g + 16), part, out)
    return out


def unpack_rows(flat):
    return jnp.concatenate(
        [flat] + [pltpu.roll(flat, 128 - 16 * g, axis=1) for g in range(1, 8)], axis=0
    )


def position():
    k = lax.axis_index(GZ)
    return (lax.axis_index("gx") * 4 + lax.axis_index("gy")) * 8 + k, k


def evens():
    return [lax.axis_index(axis) % 2 == 0 for axis in ("gx", "gy", "gz_1")]


def pack_kernel(
    pos_in, node_in, far_in, geom_in, pline_in, fline_in, live_in,
    xa, xb, ya, yb, za, zb, geom, pos, node, far, pline, fline, live,
    geom_raw, sems,
):
    copies = [
        pltpu.make_async_copy(source, target, sems.at[n])
        for n, (source, target) in enumerate(
            (
                (fline_in, fline),
                (far_in, far),
                (geom_in, geom_raw),
                (pline_in, pline),
                (pos_in, pos),
                (node_in, node),
                (live_in, live),
            )
        )
    ]
    for copy in copies:
        copy.start()
    for copy in copies[:4]:
        copy.wait()
    for c in range(4):
        geom[c] = geom_raw[:, c, :]
    fcol = column(fline[...].astype(F32), OUTER, OUTER).astype(I32)
    x, y, line = decode(fcol)
    tag = (line + 1).astype(F32)
    far_z = jnp.clip(far[OUTER:, :] - 3, 0, 255).astype(F32)
    even_x, even_y, even_z = evens()
    low = (x < 0).astype(I32), (y < 0).astype(I32)
    high = (x > 15).astype(I32), (y > 15).astype(I32)
    for axis, even, first, second in ((0, even_x, xa, xb), (1, even_y, ya, yb)):
        for buf, mask in (
            (first, jnp.where(even, high[axis], low[axis])),
            (second, jnp.where(even, low[axis], high[axis])),
        ):
            for c in range(3):
                buf[144 + 16 * c : 160 + 16 * c, :] = geom[c, OUTER:, :]
            buf[192:208, :] = far_z
            buf[208:224, :] = jnp.broadcast_to(jnp.where(mask > 0, tag, 0.0), (OUTER, 256))
    lines = jnp.broadcast_to(pline[...].astype(F32) + 1.0, (8, SLOTS))
    for buf in (za, zb):
        buf[32:40, :] = jnp.zeros((8, 128), F32)
        buf[32:40, 0:SLOTS] = lines
    for copy in copies[4:]:
        copy.wait()
    for c in range(3):
        low, high = pos[c, 0:48, :], pos[c, 208:256, :]
        xa[48 * c : 48 * c + 48, :] = jnp.where(even_x, high, low)
        xb[48 * c : 48 * c + 48, :] = jnp.where(even_x, low, high)
        for i in range(16):
            to = 48 * c + 3 * i
            low, high = pos[c, 16 * i : 16 * i + 3, :], pos[c, 16 * i + 13 : 16 * i + 16, :]
            ya[to : to + 3, :] = jnp.where(even_y, high, low)
            yb[to : to + 3, :] = jnp.where(even_y, low, high)
    parts = [pos[c] for c in range(3)]
    low = pack_rows(edge_lanes(parts, 0, None))
    high = pack_rows(edge_lanes(parts, None, 0))
    za[0:32, :] = jnp.where(even_z, high, low)
    zb[0:32, :] = jnp.where(even_z, low, high)


def z_index(far_outer):
    z = far_outer - 3
    below = z < 0
    above = z > 255
    index = jnp.where(below, z + 12, jnp.where(above, z - 256, 0))
    return index, below | above


def z_values(edges, far_outer):
    index, outside = z_index(far_outer)
    out = []
    for c in range(3):
        parts = [
            take128(edges, index[:, t * 128 : (t + 1) * 128] + 3 * c) for t in (0, 1)
        ]
        out.append(jnp.where(outside, jnp.concatenate(parts, axis=1), 0.0))
    return out


def scatter(rows, node, xs, ys):
    for r, value in enumerate(rows):
        for t in (0, 1):
            xs[t, pl.ds(r, SLOTS, stride=8), :] = value[:, t * 128 : (t + 1) * 128]
    places = iota((256, 256), 0).astype(F32).astype(BF16)
    one, zero = jnp.ones((), BF16), jnp.zeros((), BF16)
    for s in range(SLOTS):
        at = slice(8 * s, 8 * s + 8)
        x = jnp.concatenate([xs[0, at, :], xs[1, at, :]], axis=1)
        hi = x.astype(BF16).astype(F32)
        index = node[s : s + 1, :].astype(F32).astype(BF16)
        got = lax.dot_general(
            jnp.concatenate([hi, x - hi], axis=0).astype(BF16),
            jnp.where(places == jnp.broadcast_to(index, (256, 256)), one, zero),
            (((1,), (1,)), ((), ())),
            preferred_element_type=F32,
        )
        total = got[8:16] + got[0:8]
        ys[0, at, :] = total[:, :128]
        ys[1, at, :] = total[:, 128:]
    return [
        jnp.concatenate([ys[t, pl.ds(r, SLOTS, stride=8), :] for t in (0, 1)], axis=1)
        for r in range(len(rows))
    ]


def pair_tile(first, second):
    lane = iota((4, 128), 1)
    return jnp.where(lane == 9, first, jnp.where(lane == 10, second, 0.0))


def pack_edges(edges):
    lane = iota((8, 128), 1)
    out = edges[0:8]
    for g in range(1, 4):
        moved = pltpu.roll(edges[8 * g : 8 * g + 8], 16 * g, axis=1)
        out = jnp.where((lane >= 16 * g) & (lane < 16 * g + 16), moved, out)
    return jnp.where(iota((4, 128), 1) < 64, out[0:4], pltpu.roll(out, 64, axis=1)[4:8])


def unpack_edges(tile):
    whole = jnp.concatenate([tile, pltpu.roll(tile, 64, axis=1)], axis=0)
    return jnp.concatenate(
        [whole] + [pltpu.roll(whole, 128 - 16 * g, axis=1) for g in range(1, 4)], axis=0
    )


def depth_of(gap, live):
    return jnp.where(iota((SLOTS, 256), 0) < live, jnp.maximum(-gap, 0.0), 0.0)


def total2(x):
    return jnp.sum(jnp.sum(x, axis=0, keepdims=True), axis=1, keepdims=True)


def first_mask(pline):
    shape = (SLOTS, SLOTS)
    row = jnp.broadcast_to(pline.astype(F32), shape)
    col = column(pline.astype(F32), 0, SLOTS)
    again = jnp.where((row == col) & (iota(shape, 1) < iota(shape, 0)), 1.0, 0.0)
    first = jnp.sum(again, axis=1, keepdims=True) == 0.0
    return jnp.broadcast_to(jnp.where(first, 1.0, 0.0), (SLOTS, 256))


def residual_of(near, first):
    square = near[0] * near[0] + near[1] * near[1] + near[2] * near[2]
    return total2(first[...] * square)


def own_index(far):
    z = far[...] - 3
    return jnp.clip(z, 0, 255), (z >= 0) & (z < 256)


def respond(normal, energy, node, far, geom, first, sel, requests, outs):
    *replies, sums, change = outs
    bottom = pack_edges(edge_lanes(normal, 0, None))
    top = pack_edges(edge_lanes(normal, None, 0))
    lines = [pick(sel[...], normal[c]) for c in range(3)]
    residual = residual_of([v[0:SLOTS] for v in lines], first)
    tile = pair_tile(energy, residual)
    for j in range(128):
        sums[j] = tile
    lane = iota((4, 128), 1)
    keep = (lane & 15) < 9
    me, k = position()
    sums[jnp.where(k > 0, me - 1, me)] = jnp.where(keep, bottom, tile)
    sums[jnp.where(k < 7, me + 1, me)] = jnp.where(keep, top, tile)
    for d, (buf, reply) in enumerate(zip(requests, replies, strict=True)):
        at = 2 * SLOTS + OUTER * d
        values = take_lanes([v[at : at + OUTER] for v in lines], buf[192:208, :].astype(I32))
        answer = jnp.zeros((OUTER, 256), F32)
        for c in range(3):
            answer = answer + buf[144 + 16 * c : 160 + 16 * c, :] * values[c]
        reply[...] = answer
    index, inside = own_index(far)
    near = take_lanes([v[0:SLOTS] for v in lines], node[...])
    other = take_lanes([v[SLOTS : 2 * SLOTS] for v in lines], index)
    moved = jnp.zeros((SLOTS, 256), F32)
    for c in range(3):
        moved = moved + geom[c] * (near[c] - jnp.where(inside, other[c], 0.0))
    change[...] = moved


def base_kernel(
    pos, node, far, geom, pline, fline, live,
    gap_out, own_out, face_out, inverse_out, first, xs, ys,
):
    first[...] = first_mask(pline[...])
    own = pline[...].astype(F32)
    near_col = column(own, 0, SLOTS)
    far_col = column(fline[...].astype(F32), 0, SLOTS)
    x, y, line = decode(far_col.astype(I32))
    inside = (x >= 0) & (x < 16) & (y >= 0) & (y < 16)
    local = jnp.where(inside, line, -2).astype(F32)
    both = jnp.concatenate([near_col, local], axis=0)
    own_out[...] = jnp.broadcast_to(both, (2 * SLOTS, 128))
    xo, yo = x[OUTER:], y[OUTER:]
    even_x, even_y, _ = evens()
    at_x, at_y = jnp.where(even_x, 48, 0), jnp.where(even_y, 48, 0)
    face = jnp.where(xo < 0, at_x + (xo + 3) * 16 + yo, -1)
    face = jnp.where(xo > 15, 48 - at_x + (xo - 16) * 16 + yo, face)
    face = jnp.where(yo < 0, 96 + at_y + xo * 3 + yo + 3, face)
    face = jnp.where(yo > 15, 144 - at_y + xo * 3 + yo - 16, face)
    face_out[...] = hot(iota((OUTER, 192), 1), face)
    ones = jnp.where(iota((SLOTS, 256), 0) < live[...], 1.0, 0.0)
    (counts,) = scatter([ones], node, xs, ys)
    same = hot(jnp.broadcast_to(twice(own), (SLOTS, 2 * SLOTS)), near_col)
    inverse_out[...] = 1.0 / (1.0 + pick(same, counts))
    sel = hot(iota((2 * SLOTS, 256), 1).astype(F32), both)
    index, within = own_index(far)
    got = [pick(sel, pos[c]) for c in range(3)]
    near = take_lanes([v[0:SLOTS] for v in got], node[...])
    other = take_lanes([v[SLOTS:] for v in got], index)
    gap = jnp.zeros((SLOTS, 256), F32)
    for c in range(3):
        gap = gap + geom[c] * (near[c] - jnp.where(within, other[c], 0.0))
    gap_out[...] = gap - geom[3]


def first_kernel(
    gap_in, own, face, inverse, far, geom, pline, live, node, first,
    xa, xb, ya, yb, za, zb,
    gap_out, normal_out, moved_out, sel_out, selz_out, *rest,
):
    *outs, xs, ys = rest
    requests = (xa, xb, ya, yb)
    even_z = evens()[2]
    above = jnp.where(even_z, za[...], zb[...])
    below = jnp.where(even_z, zb[...], za[...])
    wanted = jnp.concatenate(
        [own[:, 0:1]] + [buf[208:224, 0:1] - 1.0 for buf in requests], axis=0
    )
    lines = twice(pline[...].astype(F32))
    sel_out[...] = hot(jnp.broadcast_to(lines, (128, 2 * SLOTS)), wanted)
    local = own[SLOTS + OUTER :, 0:1]
    selz = jnp.concatenate([above[32:33, 0:SLOTS], below[32:33, 0:SLOTS]], axis=1) - 1.0
    selz_out[...] = hot(jnp.broadcast_to(twice(selz), (OUTER, 4 * SLOTS)), local)
    edges = jnp.where(
        iota((256, 128), 1) < 9,
        unpack_rows(above[0:32]),
        pltpu.roll(unpack_rows(below[0:32]), 9, axis=1),
    )
    sel = hot(iota((OUTER, 256), 1).astype(F32), local)
    ends = z_values(pick(sel, edges), far[OUTER:, :])
    index, within = own_index(far)
    faces = [
        pick(face[...], jnp.concatenate([buf[48 * c : 48 * c + 48, :] for buf in requests], axis=0))
        for c in range(3)
    ]
    faces = take_lanes(faces, index[OUTER:])
    outer = jnp.zeros((OUTER, 256), F32)
    for c in range(3):
        outer = outer + geom[c, OUTER:, :] * (
            jnp.where(within[OUTER:], faces[c], 0.0) + ends[c]
        )
    gap = gap_in[...] - jnp.concatenate([jnp.zeros((OUTER, 256), F32), outer], axis=0)
    gap_out[...] = gap
    depth = depth_of(gap, live[...])
    got = scatter([depth * geom[c] for c in range(3)], node, xs, ys)
    normal = [got[c] * inverse[...] for c in range(3)]
    for c in range(3):
        normal_out[c] = normal[c]
        moved_out[c] = jnp.zeros((SLOTS, 256), F32)
    respond(normal, total2(depth * depth), node, far, geom, first, sel_out, requests, outs)


def update(gap, change, far, geom, selz, replies, got):
    sums = jnp.sum(got[...], axis=0)
    scale = RELAX * (1.0 / (1.0 + sums[0:1, 9:10] / N_PAIRS))
    me, k = position()
    lane = iota((SLOTS, 128), 1)
    above = unpack_edges(got[jnp.where(k < 7, me + 1, me)])
    below = pltpu.roll(unpack_edges(got[jnp.where(k > 0, me - 1, me)]), 9, axis=1)
    above = jnp.where(lane < 9, above, 0.0)
    below = jnp.where((lane > 8) & (lane < 18), below, 0.0)
    ends = z_values(
        pick(selz[...], jnp.concatenate([above, below], axis=0)), far[OUTER:, :]
    )
    outer = (replies[0][...] + replies[1][...]) + (replies[2][...] + replies[3][...])
    for c in range(3):
        outer = outer + geom[c, OUTER:, :] * ends[c]
    full = change[...] - jnp.concatenate([jnp.zeros((OUTER, 256), F32), outer], axis=0)
    return sums, scale, gap[...] + scale * full


def sweep_kernel(
    last, gap, change, normal, moved, inverse, node, far, geom, first, live, sel, selz,
    r0, r1, r2, r3, got, *rest,
):
    *rest, xs, ys = rest
    if last:
        sums_out, normal_out, moved_out, out = rest
    else:
        requests, (gap_out, sums_out, normal_out, moved_out, *outs) = rest[:4], rest[4:]
    sums, scale, fresh = update(gap, change, far, geom, selz, (r0, r1, r2, r3), got)
    sums_out[...] = sums
    for c in range(3):
        moved_out[c] = moved[c] + scale * normal[c]
    depth = depth_of(fresh, live[...])
    energy = total2(depth * depth)
    found = scatter([depth * geom[c] for c in range(3)], node, xs, ys)
    fresh_normal = [found[c] * inverse[...] for c in range(3)]
    for c in range(3):
        normal_out[c] = fresh_normal[c]
    if last:
        lines = [pick(sel[0:SLOTS, :], fresh_normal[c]) for c in range(3)]
        tile = pair_tile(energy, residual_of(lines, first))
        for j in range(128):
            out[j] = tile
    else:
        gap_out[...] = fresh
        respond(fresh_normal, energy, node, far, geom, first, sel, requests, outs)


def last_kernel(pos, normal, moved, pline, got, s0, s1, s2, s3, out, history):
    every = [s[0:1, :] for s in (s0, s1, s2, s3)] + [jnp.sum(got[...], axis=0)[0:1]]
    scales = [RELAX * (1.0 / (1.0 + s[:, 9:10] / N_PAIRS)) for s in every]
    sel = hot(iota((256, SLOTS), 0), jnp.broadcast_to(pline[...], (256, SLOTS)))
    for c in range(3):
        out[c] = pos[c] + pick(sel, moved[c] + scales[-1] * normal[c])
    for t in range(SWEEPS):
        residual = scales[t] * scales[t] * every[t][:, 10:11]
        history[0:1, t : t + 1] = jnp.sqrt(1.0 + every[t][:, 9:10] / PAIRS_SLOTS)
        history[1:2, t : t + 1] = jnp.sqrt(1.0 + residual / NODES_BLK)


within = pltpu.with_memory_space_constraint


def call(kernel, outs, args, scratch=(), inputs=False):
    vmem = pl.BlockSpec(memory_space=pltpu.VMEM)
    hbm = pl.BlockSpec(memory_space=pltpu.HBM)
    return pl.pallas_call(
        kernel,
        out_shape=outs,
        in_specs=[hbm if inputs else vmem] * len(args),
        out_specs=[vmem] * len(outs) if isinstance(outs, list) else vmem,
        scratch_shapes=list(scratch),
        compiler_params=pltpu.CompilerParams(vmem_limit_bytes=12 * 2**20),
    )(*(args if inputs else [within(x, pltpu.VMEM) for x in args]))


def shape(*dims, dtype=F32):
    return pltpu.VMEM(dims, dtype)


def swap(x, axis, second):
    count = lax.axis_size(axis)
    pairs = [(i, (i + 1) % count) for i in range(int(second), count, 2)]
    return lax.ppermute(x, axis, pairs + [(b, a) for a, b in pairs])


def swap_all(arrays):
    axes = ("gx", "gx", "gy", "gy", GZ, GZ)
    return [swap(x, axis, n % 2) for n, (x, axis) in enumerate(zip(arrays, axes))]


def local(positions, pair_node, pair_line, pair_far, far_line, pair_geom, live_blocks):
    pos = positions.reshape(3, 256, 256)
    node = pair_node.reshape(SLOTS, 256)
    far = pair_far.reshape(SLOTS, 256)
    geom = pair_geom.reshape(SLOTS, 4, 256)
    pline = pair_line.reshape(1, SLOTS)
    fline = far_line.reshape(1, SLOTS)
    live = live_blocks.reshape(1, 1)
    work = [pltpu.VMEM((2, 256, 128), F32)] * 2

    face, ends = shape(224, 256), shape(40, 128)
    flat = shape(SLOTS, 256)
    flat_i = shape(SLOTS, 256, dtype=I32)
    few = shape(1, SLOTS, dtype=I32)
    packed = call(
        pack_kernel,
        [face] * 4
        + [ends] * 2
        + [shape(4, SLOTS, 256), shape(3, 256, 256), flat_i, flat_i, few, few]
        + [shape(1, 1, dtype=I32)],
        [within(x, pltpu.HBM) for x in (pos, node, far, geom, pline, fline)] + [live],
        [pltpu.VMEM((SLOTS, 4, 256), F32), pltpu.SemaphoreType.DMA((7,))],
        inputs=True,
    )
    *six, geom, pos, node, far, pline, fline, live = packed
    *requests, za, zb = swap_all(six)
    triple = shape(3, SLOTS, 256)
    outs = [shape(OUTER, 256)] * 4 + [shape(128, 4, 128), flat]
    gap, own, face, inverse, first = call(
        base_kernel,
        [
            flat,
            shape(2 * SLOTS, 128),
            shape(OUTER, 192, dtype=BF16),
            flat,
            flat,
        ],
        [pos, node, far, geom, pline, fline, live],
        work,
    )
    gap, normal, moved, sel, selz, *sent, sums, change = call(
        first_kernel,
        [flat, triple, triple]
        + [shape(128, 2 * SLOTS, dtype=BF16), shape(OUTER, 4 * SLOTS, dtype=BF16)]
        + outs,
        [gap, own, face, inverse, far, geom, pline, live, node, first]
        + requests
        + [za, zb],
        work,
    )
    totals = []
    for t in range(1, SWEEPS):
        replies = swap_all(sent)
        got = lax.all_to_all(sums, ALL, 0, 0, tiled=True)
        args = [
            gap, change, normal, moved, inverse, node, far, geom, first, live, sel, selz,
        ]
        args = args + replies + [got]
        if t + 1 < SWEEPS:
            gap, total, normal, moved, *sent, sums, change = call(
                functools.partial(sweep_kernel, False),
                [flat, shape(4, 128), triple, triple] + outs,
                args + requests,
                work,
            )
        else:
            total, normal, moved, sums = call(
                functools.partial(sweep_kernel, True),
                [shape(4, 128), triple, triple, shape(128, 4, 128)],
                args,
                work,
            )
        totals.append(total)
    got = lax.all_to_all(sums, ALL, 0, 0, tiled=True)
    corrected, history = call(
        last_kernel,
        [jax.ShapeDtypeStruct((3, 256, 256), F32), jax.ShapeDtypeStruct((2, SWEEPS), F32)],
        [pos, normal, moved, pline, got, *totals],
    )
    return corrected.reshape(positions.shape), history


def solution(mesh):
    finer = Mesh(
        mesh.devices.reshape(mesh.shape["gx"], mesh.shape["gy"], 4, 2), ("gx", "gy", "gz_0", "gz_1")
    )
    placed = (
        P(None, "gx", "gy", GZ),
        P("gx", "gy", GZ, None, None),
        P("gx", "gy", GZ, None),
        P("gx", "gy", GZ, None, None),
        P("gx", "gy", GZ, None),
        P("gx", "gy", GZ, None, None, None),
        P("gx", "gy", GZ),
    )
    return jax.shard_map(
        local,
        mesh=finer,
        in_specs=placed,
        out_specs=(P(None, "gx", "gy", GZ), P()),
        check_vma=False,
    )
```

```python
import functools

import jax
import jax.numpy as jnp
from jax import lax
from jax.experimental import pallas as pl
from jax.experimental.pallas import tpu as pltpu
from jax.sharding import Mesh
from jax.sharding import PartitionSpec as P

SWEEPS = 5
RELAX = 0.9
XY = ("gx", "gy")
GZ = ("gz_0", "gz_1")
ALL = ("gx", "gy", "gz_0", "gz_1")
F32 = jnp.float32
BF16 = jnp.bfloat16
I32 = jnp.int32
SLOTS = 32
OUTER = 16
N_PAIRS = 1048576
NODES_BLK = 65536
PAIRS_SLOTS = 8192


def iota(shape, dim):
    return lax.broadcasted_iota(I32, shape, dim)


def pick(sel, x):
    hi = x.astype(BF16)
    mid = (x - hi.astype(F32)).astype(BF16)
    dot = functools.partial(jnp.dot, preferred_element_type=F32)
    if sel.shape[1] == 2 * x.shape[0]:
        return dot(sel, jnp.concatenate([hi, mid], axis=0))
    return dot(sel, mid) + dot(sel, hi)


def hot(a, b):
    return jnp.where(a == b, 1.0, 0.0).astype(BF16)


def twice(row):
    return jnp.concatenate([row, row], axis=1)


def column(row, first, count):
    shape = (count, row.shape[1])
    chosen = iota(shape, 0) + first == iota(shape, 1)
    return jnp.sum(jnp.where(chosen, jnp.broadcast_to(row, shape), 0.0), axis=1, keepdims=True)


def take128(x, index):
    return jnp.take_along_axis(x, index, axis=1, mode="promise_in_bounds")


def take_lanes(xs, index):
    columns = [[] for _ in xs]
    for t in (0, 1):
        cut = index[:, t * 128 : (t + 1) * 128]
        low = cut & 127
        high = cut > 127
        rows = [[] for _ in xs]
        for g in range(0, index.shape[0], 8):
            at = slice(g, g + 8)
            for x, row in zip(xs, rows, strict=True):
                a = take128(x[at, :128], low[at])
                b = take128(x[at, 128:], low[at])
                row.append(jnp.where(high[at], b, a))
        for column_parts, row in zip(columns, rows, strict=True):
            column_parts.append(jnp.concatenate(row, axis=0))
    return [jnp.concatenate(parts, axis=1) for parts in columns]


def decode(far_line):
    x = (far_line * 2979) >> 16
    y = far_line - 22 * x - 3
    x = x - 3
    return x, y, (x & 15) * 16 + (y & 15)


def edge_lanes(parts, low_first, high_first):
    lane = iota((parts[0].shape[0], 128), 1)
    out = jnp.zeros((parts[0].shape[0], 128), F32)
    for c in range(3):
        for first, half, at in ((low_first, 0, 0), (high_first, 1, 125)):
            if first is None:
                continue
            to = first + 3 * c
            moved = parts[c][:, half * 128 : half * 128 + 128]
            if (to - at) % 128:
                moved = pltpu.roll(moved, (to - at) % 128, axis=1)
            out = jnp.where((lane >= to) & (lane < to + 3), moved, out)
    return out


def pack_rows(tall):
    lane = iota((SLOTS, 128), 1)
    out = jnp.zeros((SLOTS, 128), F32)
    for g in range(8):
        part = tall[32 * g : 32 * g + 32]
        part = pltpu.roll(part, 16 * g, axis=1) if g else part
        out = jnp.where((lane >= 16 * g) & (lane < 16 * g + 16), part, out)
    return out


def unpack_rows(flat):
    return jnp.concatenate(
        [flat] + [pltpu.roll(flat, 128 - 16 * g, axis=1) for g in range(1, 8)], axis=0
    )


def position():
    k = lax.axis_index(GZ)
    return (lax.axis_index("gx") * 4 + lax.axis_index("gy")) * 8 + k, k


def evens():
    return [lax.axis_index(axis) % 2 == 0 for axis in ("gx", "gy", "gz_1")]


def pack_kernel(
    pos_in, node_in, far_in, geom_in, pline_in, fline_in, live_in,
    xa, xb, ya, yb, za, zb, geom, pos, node, far, pline, fline, live,
    geom_raw, sems,
):
    copies = [
        pltpu.make_async_copy(source, target, sems.at[n])
        for n, (source, target) in enumerate(
            (
                (fline_in, fline),
                (far_in, far),
                (geom_in, geom_raw),
                (pline_in, pline),
                (pos_in, pos),
                (node_in, node),
                (live_in, live),
            )
        )
    ]
    for copy in copies:
        copy.start()
    for copy in copies[:4]:
        copy.wait()
    for c in range(4):
        geom[c] = geom_raw[:, c, :]
    fcol = column(fline[...].astype(F32), OUTER, OUTER).astype(I32)
    x, y, line = decode(fcol)
    tag = (line + 1).astype(F32)
    far_z = jnp.clip(far[OUTER:, :] - 3, 0, 255).astype(F32)
    even_x, even_y, even_z = evens()
    low = (x < 0).astype(I32), (y < 0).astype(I32)
    high = (x > 15).astype(I32), (y > 15).astype(I32)
    for axis, even, first, second in ((0, even_x, xa, xb), (1, even_y, ya, yb)):
        for buf, mask in (
            (first, jnp.where(even, high[axis], low[axis])),
            (second, jnp.where(even, low[axis], high[axis])),
        ):
            for c in range(3):
                buf[144 + 16 * c : 160 + 16 * c, :] = geom[c, OUTER:, :]
            buf[192:208, :] = far_z
            buf[208:224, :] = jnp.broadcast_to(jnp.where(mask > 0, tag, 0.0), (OUTER, 256))
    lines = jnp.broadcast_to(pline[...].astype(F32) + 1.0, (8, SLOTS))
    for buf in (za, zb):
        buf[32:40, :] = jnp.zeros((8, 128), F32)
        buf[32:40, 0:SLOTS] = lines
    for copy in copies[4:]:
        copy.wait()
    for c in range(3):
        low, high = pos[c, 0:48, :], pos[c, 208:256, :]
        xa[48 * c : 48 * c + 48, :] = jnp.where(even_x, high, low)
        xb[48 * c : 48 * c + 48, :] = jnp.where(even_x, low, high)
        for i in range(16):
            to = 48 * c + 3 * i
            low, high = pos[c, 16 * i : 16 * i + 3, :], pos[c, 16 * i + 13 : 16 * i + 16, :]
            ya[to : to + 3, :] = jnp.where(even_y, high, low)
            yb[to : to + 3, :] = jnp.where(even_y, low, high)
    parts = [pos[c] for c in range(3)]
    low = pack_rows(edge_lanes(parts, 0, None))
    high = pack_rows(edge_lanes(parts, None, 0))
    za[0:32, :] = jnp.where(even_z, high, low)
    zb[0:32, :] = jnp.where(even_z, low, high)


def z_index(far_outer):
    z = far_outer - 3
    below = z < 0
    above = z > 255
    index = jnp.where(below, z + 12, jnp.where(above, z - 256, 0))
    return index, below | above


def z_values(edges, far_outer):
    index, outside = z_index(far_outer)
    out = []
    for c in range(3):
        parts = [
            take128(edges, index[:, t * 128 : (t + 1) * 128] + 3 * c) for t in (0, 1)
        ]
        out.append(jnp.where(outside, jnp.concatenate(parts, axis=1), 0.0))
    return out


def scatter(rows, node, xs, ys):
    for r, value in enumerate(rows):
        for t in (0, 1):
            xs[t, pl.ds(r, SLOTS, stride=8), :] = value[:, t * 128 : (t + 1) * 128]
    places = iota((256, 256), 0).astype(F32).astype(BF16)
    one, zero = jnp.ones((), BF16), jnp.zeros((), BF16)
    for s in range(SLOTS):
        at = slice(8 * s, 8 * s + 8)
        x = jnp.concatenate([xs[0, at, :], xs[1, at, :]], axis=1)
        hi = x.astype(BF16).astype(F32)
        index = node[s : s + 1, :].astype(F32).astype(BF16)
        got = lax.dot_general(
            jnp.concatenate([hi, x - hi], axis=0).astype(BF16),
            jnp.where(places == jnp.broadcast_to(index, (256, 256)), one, zero),
            (((1,), (1,)), ((), ())),
            preferred_element_type=F32,
        )
        total = got[8:16] + got[0:8]
        ys[0, at, :] = total[:, :128]
        ys[1, at, :] = total[:, 128:]
    return [
        jnp.concatenate([ys[t, pl.ds(r, SLOTS, stride=8), :] for t in (0, 1)], axis=1)
        for r in range(len(rows))
    ]


def pair_tile(rows, energy, *residuals):
    lane = iota((rows, 128), 1)
    out = jnp.where(lane == 9, energy, 0.0)
    for n, residual in enumerate(residuals):
        out = jnp.where(lane == 10 + n, residual, out)
    return out


def pack_edges(edges):
    lane = iota((8, 128), 1)
    out = edges[0:8]
    for g in range(1, 4):
        moved = pltpu.roll(edges[8 * g : 8 * g + 8], 16 * g, axis=1)
        out = jnp.where((lane >= 16 * g) & (lane < 16 * g + 16), moved, out)
    return jnp.where(iota((4, 128), 1) < 64, out[0:4], pltpu.roll(out, 64, axis=1)[4:8])


def unpack_edges(tile):
    whole = jnp.concatenate([tile, pltpu.roll(tile, 64, axis=1)], axis=0)
    return jnp.concatenate(
        [whole] + [pltpu.roll(whole, 128 - 16 * g, axis=1) for g in range(1, 4)], axis=0
    )


def depth_of(gap, live):
    return jnp.where(iota((SLOTS, 256), 0) < live, jnp.maximum(-gap, 0.0), 0.0)


def total2(x):
    return jnp.sum(jnp.sum(x, axis=0, keepdims=True), axis=1, keepdims=True)


def first_mask(pline):
    shape = (SLOTS, SLOTS)
    row = jnp.broadcast_to(pline.astype(F32), shape)
    col = column(pline.astype(F32), 0, SLOTS)
    again = jnp.where((row == col) & (iota(shape, 1) < iota(shape, 0)), 1.0, 0.0)
    first = jnp.sum(again, axis=1, keepdims=True) == 0.0
    return jnp.broadcast_to(jnp.where(first, 1.0, 0.0), (SLOTS, 256))


def residual_of(near, first):
    square = near[0] * near[0] + near[1] * near[1] + near[2] * near[2]
    return total2(first[...] * square)


def own_index(far):
    z = far[...] - 3
    return jnp.clip(z, 0, 255), (z >= 0) & (z < 256)


def respond(normal, tile, sel, requests, replies, sums):
    bottom = pack_edges(edge_lanes(normal, 0, None))
    top = pack_edges(edge_lanes(normal, None, 0))
    for j in range(128):
        sums[j] = tile
    keep = (iota((4, 128), 1) & 15) < 9
    me, k = position()
    sums[jnp.where(k > 0, me - 1, me)] = jnp.where(keep, bottom, tile)
    sums[jnp.where(k < 7, me + 1, me)] = jnp.where(keep, top, tile)
    for pair in (0, 2):
        at = slice(OUTER * pair, OUTER * pair + 2 * OUTER)
        lines = [pick(sel[at, :], normal[c]) for c in range(3)]
        for d, low in ((pair, 0), (pair + 1, OUTER)):
            buf = requests[d]
            index = buf[192:208, :].astype(I32)
            values = take_lanes([v[low : low + OUTER] for v in lines], index)
            answer = jnp.zeros((OUTER, 256), F32)
            for c in range(3):
                answer = answer + buf[144 + 16 * c : 160 + 16 * c, :] * values[c]
            replies[d][...] = answer


def own_kernel(normal, node, far, geom, first, sel, change, residual):
    index, inside = own_index(far)
    lines = [pick(sel[0:SLOTS, :], normal[c]) for c in range(3)]
    residual[...] = jnp.broadcast_to(residual_of(lines, first), (1, 128))
    near = take_lanes(lines, node[...])
    other = [pick(sel[SLOTS : 2 * SLOTS, :], normal[c]) for c in range(3)]
    other = take_lanes(other, index)
    moved = jnp.zeros((SLOTS, 256), F32)
    for c in range(3):
        moved = moved + geom[c] * (near[c] - jnp.where(inside, other[c], 0.0))
    change[...] = moved


def base_kernel(
    pos, node, far, geom, pline, fline, live,
    gap_out, own_out, face_out, inverse_out, first, xs, ys,
):
    first[...] = first_mask(pline[...])
    own = pline[...].astype(F32)
    near_col = column(own, 0, SLOTS)
    far_col = column(fline[...].astype(F32), 0, SLOTS)
    x, y, line = decode(far_col.astype(I32))
    inside = (x >= 0) & (x < 16) & (y >= 0) & (y < 16)
    local = jnp.where(inside, line, -2).astype(F32)
    both = jnp.concatenate([near_col, local], axis=0)
    own_out[...] = jnp.broadcast_to(both, (2 * SLOTS, 128))
    xo, yo = x[OUTER:], y[OUTER:]
    even_x, even_y, _ = evens()
    at_x, at_y = jnp.where(even_x, 48, 0), jnp.where(even_y, 48, 0)
    face = jnp.where(xo < 0, at_x + (xo + 3) * 16 + yo, -1)
    face = jnp.where(xo > 15, 48 - at_x + (xo - 16) * 16 + yo, face)
    face = jnp.where(yo < 0, 96 + at_y + xo * 3 + yo + 3, face)
    face = jnp.where(yo > 15, 144 - at_y + xo * 3 + yo - 16, face)
    face_out[...] = hot(iota((OUTER, 192), 1), face)
    ones = jnp.where(iota((SLOTS, 256), 0) < live[...], 1.0, 0.0)
    (counts,) = scatter([ones], node, xs, ys)
    same = hot(jnp.broadcast_to(twice(own), (SLOTS, 2 * SLOTS)), near_col)
    inverse_out[...] = 1.0 / (1.0 + pick(same, counts))
    sel = hot(iota((2 * SLOTS, 256), 1).astype(F32), both)
    index, within = own_index(far)
    got = [pick(sel, pos[c]) for c in range(3)]
    near = take_lanes([v[0:SLOTS] for v in got], node[...])
    other = take_lanes([v[SLOTS:] for v in got], index)
    gap = jnp.zeros((SLOTS, 256), F32)
    for c in range(3):
        gap = gap + geom[c] * (near[c] - jnp.where(within, other[c], 0.0))
    gap_out[...] = gap - geom[3]


def first_kernel(
    gap_in, own, face, inverse, far, geom, pline, live, node,
    xa, xb, ya, yb, za, zb,
    gap_out, normal_out, moved_out, own_sel, out_sel, selz_out, *rest,
):
    *replies, sums, xs, ys = rest
    requests = (xa, xb, ya, yb)
    even_z = evens()[2]
    above = jnp.where(even_z, za[...], zb[...])
    below = jnp.where(even_z, zb[...], za[...])
    wanted = jnp.concatenate(
        [own[:, 0:1]] + [buf[208:224, 0:1] - 1.0 for buf in requests], axis=0
    )
    lines = twice(pline[...].astype(F32))
    sel = hot(jnp.broadcast_to(lines, (128, 2 * SLOTS)), wanted)
    own_sel[...] = sel[0:64]
    out_sel[...] = sel[64:128]
    local = own[SLOTS + OUTER :, 0:1]
    selz = jnp.concatenate([above[32:33, 0:SLOTS], below[32:33, 0:SLOTS]], axis=1) - 1.0
    selz_out[...] = hot(jnp.broadcast_to(twice(selz), (OUTER, 4 * SLOTS)), local)
    edges = jnp.where(
        iota((256, 128), 1) < 9,
        unpack_rows(above[0:32]),
        pltpu.roll(unpack_rows(below[0:32]), 9, axis=1),
    )
    sel = hot(iota((OUTER, 256), 1).astype(F32), local)
    ends = z_values(pick(sel, edges), far[OUTER:, :])
    index, within = own_index(far)
    faces = [
        pick(face[...], jnp.concatenate([buf[48 * c : 48 * c + 48, :] for buf in requests], axis=0))
        for c in range(3)
    ]
    faces = take_lanes(faces, index[OUTER:])
    outer = jnp.zeros((OUTER, 256), F32)
    for c in range(3):
        outer = outer + geom[c, OUTER:, :] * (
            jnp.where(within[OUTER:], faces[c], 0.0) + ends[c]
        )
    gap = gap_in[...] - jnp.concatenate([jnp.zeros((OUTER, 256), F32), outer], axis=0)
    gap_out[...] = gap
    depth = depth_of(gap, live[...])
    got = scatter([depth * geom[c] for c in range(3)], node, xs, ys)
    normal = [got[c] * inverse[...] for c in range(3)]
    for c in range(3):
        normal_out[c] = normal[c]
        moved_out[c] = jnp.zeros((SLOTS, 256), F32)
    tile = pair_tile(4, total2(depth * depth))
    respond(normal, tile, out_sel, requests, replies, sums)


def update(gap, change, far, geom, selz, replies, got):
    sums = jnp.sum(got[:, 0, :], axis=0, keepdims=True)
    scale = RELAX * (1.0 / (1.0 + sums[0:1, 9:10] / N_PAIRS))
    me, k = position()
    lane = iota((SLOTS, 128), 1)
    above = unpack_edges(got[jnp.where(k < 7, me + 1, me)])
    below = pltpu.roll(unpack_edges(got[jnp.where(k > 0, me - 1, me)]), 9, axis=1)
    above = jnp.where(lane < 9, above, 0.0)
    below = jnp.where((lane > 8) & (lane < 18), below, 0.0)
    ends = z_values(
        pick(selz[...], jnp.concatenate([above, below], axis=0)), far[OUTER:, :]
    )
    outer = (replies[0][...] + replies[1][...]) + (replies[2][...] + replies[3][...])
    for c in range(3):
        outer = outer + geom[c, OUTER:, :] * ends[c]
    full = change[...] - jnp.concatenate([jnp.zeros((OUTER, 256), F32), outer], axis=0)
    return sums, scale, gap[...] + scale * full


def sweep_kernel(
    last, gap, change, residual, normal, moved, inverse, node, far, geom, live, selz,
    r0, r1, r2, r3, got, *rest,
):
    *rest, xs, ys = rest
    if last:
        first, own_sel, sums_out, normal_out, moved_out, out = rest
    else:
        *requests, out_sel, gap_out, sums_out, normal_out, moved_out = rest[:9]
        *replies, out = rest[9:]
    sums, scale, fresh = update(gap, change, far, geom, selz, (r0, r1, r2, r3), got)
    sums_out[...] = sums
    for c in range(3):
        moved_out[c] = moved[c] + scale * normal[c]
    depth = depth_of(fresh, live[...])
    energy = total2(depth * depth)
    found = scatter([depth * geom[c] for c in range(3)], node, xs, ys)
    fresh_normal = [found[c] * inverse[...] for c in range(3)]
    for c in range(3):
        normal_out[c] = fresh_normal[c]
    before = residual[:, 0:1]
    if last:
        lines = [pick(own_sel[0:SLOTS, :], fresh_normal[c]) for c in range(3)]
        tile = pair_tile(8, energy, before, residual_of(lines, first))
        out[...] = jnp.broadcast_to(tile[0:1, :], (128, 128))
    else:
        gap_out[...] = fresh
        tile = pair_tile(4, energy, before)
        respond(fresh_normal, tile, out_sel, requests, replies, out)


def last_kernel(pos, normal, moved, pline, got, s0, s1, s2, s3, out, history):
    every = [s[0:1, :] for s in (s0, s1, s2, s3)] + [jnp.sum(got[...], axis=0, keepdims=True)]
    scales = [RELAX * (1.0 / (1.0 + s[:, 9:10] / N_PAIRS)) for s in every]
    sel = hot(iota((256, SLOTS), 0), jnp.broadcast_to(pline[...], (256, SLOTS)))
    for c in range(3):
        out[c] = pos[c] + pick(sel, moved[c] + scales[-1] * normal[c])
    for t in range(SWEEPS):
        later = every[t + 1][:, 10:11] if t + 1 < SWEEPS else every[t][:, 11:12]
        residual = scales[t] * scales[t] * later
        history[0:1, t : t + 1] = jnp.sqrt(1.0 + every[t][:, 9:10] / PAIRS_SLOTS)
        history[1:2, t : t + 1] = jnp.sqrt(1.0 + residual / NODES_BLK)


within = pltpu.with_memory_space_constraint


def call(kernel, outs, args, scratch=(), inputs=False):
    vmem = pl.BlockSpec(memory_space=pltpu.VMEM)
    hbm = pl.BlockSpec(memory_space=pltpu.HBM)
    return pl.pallas_call(
        kernel,
        out_shape=outs,
        in_specs=[hbm if inputs else vmem] * len(args),
        out_specs=[vmem] * len(outs) if isinstance(outs, list) else vmem,
        scratch_shapes=list(scratch),
        compiler_params=pltpu.CompilerParams(vmem_limit_bytes=12 * 2**20),
    )(*(args if inputs else [within(x, pltpu.VMEM) for x in args]))


def shape(*dims, dtype=F32):
    return pltpu.VMEM(dims, dtype)


def swap(x, axis, second):
    count = lax.axis_size(axis)
    pairs = [(i, (i + 1) % count) for i in range(int(second), count, 2)]
    return lax.ppermute(x, axis, pairs + [(b, a) for a, b in pairs])


def swap_all(arrays):
    axes = ("gx", "gx", "gy", "gy", GZ, GZ)
    return [swap(x, axis, n % 2) for n, (x, axis) in enumerate(zip(arrays, axes))]


def local(positions, pair_node, pair_line, pair_far, far_line, pair_geom, live_blocks):
    pos = positions.reshape(3, 256, 256)
    node = pair_node.reshape(SLOTS, 256)
    far = pair_far.reshape(SLOTS, 256)
    geom = pair_geom.reshape(SLOTS, 4, 256)
    pline = pair_line.reshape(1, SLOTS)
    fline = far_line.reshape(1, SLOTS)
    live = live_blocks.reshape(1, 1)
    work = [pltpu.VMEM((2, 256, 128), F32)] * 2

    face, ends = shape(224, 256), shape(40, 128)
    flat = shape(SLOTS, 256)
    flat_i = shape(SLOTS, 256, dtype=I32)
    few = shape(1, SLOTS, dtype=I32)
    packed = call(
        pack_kernel,
        [face] * 4
        + [ends] * 2
        + [shape(4, SLOTS, 256), shape(3, 256, 256), flat_i, flat_i, few, few]
        + [shape(1, 1, dtype=I32)],
        [within(x, pltpu.HBM) for x in (pos, node, far, geom, pline, fline)] + [live],
        [pltpu.VMEM((SLOTS, 4, 256), F32), pltpu.SemaphoreType.DMA((7,))],
        inputs=True,
    )
    *six, geom, pos, node, far, pline, fline, live = packed
    *requests, za, zb = swap_all(six)
    triple = shape(3, SLOTS, 256)
    outs = [shape(OUTER, 256)] * 4 + [shape(128, 4, 128)]
    gap, own, face, inverse, first = call(
        base_kernel,
        [
            flat,
            shape(2 * SLOTS, 128),
            shape(OUTER, 192, dtype=BF16),
            flat,
            flat,
        ],
        [pos, node, far, geom, pline, fline, live],
        work,
    )
    choice = shape(2 * SLOTS, 2 * SLOTS, dtype=BF16)
    gap, normal, moved, own_sel, out_sel, selz, *sent, sums = call(
        first_kernel,
        [flat, triple, triple, choice, choice, shape(OUTER, 4 * SLOTS, dtype=BF16)] + outs,
        [gap, own, face, inverse, far, geom, pline, live, node] + requests + [za, zb],
        work,
    )
    totals = []
    row = shape(1, 128)
    for t in range(1, SWEEPS):
        replies = swap_all(sent)
        got = lax.all_to_all(sums, ALL, 0, 0, tiled=True)
        change, residual = call(
            own_kernel, [flat, row], [normal, node, far, geom, first, own_sel]
        )
        args = [
            gap, change, residual, normal, moved, inverse, node, far, geom, live, selz,
        ]
        args = args + replies + [got]
        if t + 1 < SWEEPS:
            gap, total, normal, moved, *sent, sums = call(
                functools.partial(sweep_kernel, False),
                [flat, row, triple, triple] + outs,
                args + requests + [out_sel],
                work,
            )
        else:
            total, normal, moved, sums = call(
                functools.partial(sweep_kernel, True),
                [row, triple, triple, shape(128, 128)],
                args + [first, own_sel],
                work,
            )
        totals.append(total)
    sums = sums.reshape(128, 1, 128)
    got = lax.all_to_all(sums, ALL, 0, 0, tiled=True).reshape(128, 128)
    corrected, history = call(
        last_kernel,
        [jax.ShapeDtypeStruct((3, 256, 256), F32), jax.ShapeDtypeStruct((2, SWEEPS), F32)],
        [pos, normal, moved, pline, got, *totals],
    )
    return corrected.reshape(positions.shape), history


def solution(mesh):
    finer = Mesh(
        mesh.devices.reshape(mesh.shape["gx"], mesh.shape["gy"], 4, 2), ("gx", "gy", "gz_0", "gz_1")
    )
    placed = (
        P(None, "gx", "gy", GZ),
        P("gx", "gy", GZ, None, None),
        P("gx", "gy", GZ, None),
        P("gx", "gy", GZ, None, None),
        P("gx", "gy", GZ, None),
        P("gx", "gy", GZ, None, None, None),
        P("gx", "gy", GZ),
    )
    return jax.shard_map(
        local,
        mesh=finer,
        in_specs=placed,
        out_specs=(P(None, "gx", "gy", GZ), P()),
        check_vma=False,
    )
```

```python
import functools

import jax
import jax.numpy as jnp
from jax import lax
from jax.experimental import pallas as pl
from jax.experimental.pallas import tpu as pltpu
from jax.sharding import Mesh
from jax.sharding import PartitionSpec as P

SWEEPS = 5
RELAX = 0.9
XY = ("gx", "gy")
GZ = ("gz_0", "gz_1")
ALL = ("gx", "gy", "gz_0", "gz_1")
F32 = jnp.float32
BF16 = jnp.bfloat16
I32 = jnp.int32
SLOTS = 32
OUTER = 16
N_PAIRS = 1048576
NODES_BLK = 65536
PAIRS_SLOTS = 8192


def iota(shape, dim):
    return lax.broadcasted_iota(I32, shape, dim)


def pick(sel, x):
    hi = x.astype(BF16)
    mid = (x - hi.astype(F32)).astype(BF16)
    dot = functools.partial(jnp.dot, preferred_element_type=F32)
    if sel.shape[1] == 2 * x.shape[0]:
        return dot(sel, jnp.concatenate([hi, mid], axis=0))
    return dot(sel, mid) + dot(sel, hi)


def hot(a, b):
    return jnp.where(a == b, 1.0, 0.0).astype(BF16)


def twice(row):
    return jnp.concatenate([row, row], axis=1)


def column(row, first, count):
    shape = (count, row.shape[1])
    chosen = iota(shape, 0) + first == iota(shape, 1)
    return jnp.sum(jnp.where(chosen, jnp.broadcast_to(row, shape), 0.0), axis=1, keepdims=True)


def take128(x, index):
    return jnp.take_along_axis(x, index, axis=1, mode="promise_in_bounds")


def take_lanes(xs, index):
    columns = [[] for _ in xs]
    for t in (0, 1):
        cut = index[:, t * 128 : (t + 1) * 128]
        low = cut & 127
        high = cut > 127
        rows = [[] for _ in xs]
        for g in range(0, index.shape[0], 8):
            at = slice(g, g + 8)
            for x, row in zip(xs, rows, strict=True):
                a = take128(x[at, :128], low[at])
                b = take128(x[at, 128:], low[at])
                row.append(jnp.where(high[at], b, a))
        for column_parts, row in zip(columns, rows, strict=True):
            column_parts.append(jnp.concatenate(row, axis=0))
    return [jnp.concatenate(parts, axis=1) for parts in columns]


def decode(far_line):
    x = (far_line * 2979) >> 16
    y = far_line - 22 * x - 3
    x = x - 3
    return x, y, (x & 15) * 16 + (y & 15)


def edge_lanes(parts, low_first, high_first):
    lane = iota((parts[0].shape[0], 128), 1)
    out = jnp.zeros((parts[0].shape[0], 128), F32)
    for c in range(3):
        for first, half, at in ((low_first, 0, 0), (high_first, 1, 125)):
            if first is None:
                continue
            to = first + 3 * c
            moved = parts[c][:, half * 128 : half * 128 + 128]
            if (to - at) % 128:
                moved = pltpu.roll(moved, (to - at) % 128, axis=1)
            out = jnp.where((lane >= to) & (lane < to + 3), moved, out)
    return out


def pack_rows(tall):
    lane = iota((SLOTS, 128), 1)
    out = jnp.zeros((SLOTS, 128), F32)
    for g in range(8):
        part = tall[32 * g : 32 * g + 32]
        part = pltpu.roll(part, 16 * g, axis=1) if g else part
        out = jnp.where((lane >= 16 * g) & (lane < 16 * g + 16), part, out)
    return out


def unpack_rows(flat):
    return jnp.concatenate(
        [flat] + [pltpu.roll(flat, 128 - 16 * g, axis=1) for g in range(1, 8)], axis=0
    )


def position():
    k = lax.axis_index(GZ)
    return (lax.axis_index("gx") * 4 + lax.axis_index("gy")) * 8 + k, k


def evens():
    return [lax.axis_index(axis) % 2 == 0 for axis in ("gx", "gy", "gz_1")]


def pack_kernel(
    pos_in, node_in, far_in, geom_in, pline_in, fline_in, live_in,
    xa, xb, ya, yb, za, zb, geom, pos, node, far, pline, fline, live,
    geom_raw, sems,
):
    copies = [
        pltpu.make_async_copy(source, target, sems.at[n])
        for n, (source, target) in enumerate(
            (
                (fline_in, fline),
                (far_in, far),
                (geom_in, geom_raw),
                (pline_in, pline),
                (pos_in, pos),
                (node_in, node),
                (live_in, live),
            )
        )
    ]
    for copy in copies:
        copy.start()
    for copy in copies[:4]:
        copy.wait()
    for c in range(4):
        geom[c] = geom_raw[:, c, :]
    fcol = column(fline[...].astype(F32), OUTER, OUTER).astype(I32)
    x, y, line = decode(fcol)
    tag = (line + 1).astype(F32)
    far_z = jnp.clip(far[OUTER:, :] - 3, 0, 255).astype(F32)
    even_x, even_y, even_z = evens()
    low = (x < 0).astype(I32), (y < 0).astype(I32)
    high = (x > 15).astype(I32), (y > 15).astype(I32)
    for axis, even, first, second in ((0, even_x, xa, xb), (1, even_y, ya, yb)):
        for buf, mask in (
            (first, jnp.where(even, high[axis], low[axis])),
            (second, jnp.where(even, low[axis], high[axis])),
        ):
            for c in range(3):
                buf[144 + 16 * c : 160 + 16 * c, :] = geom[c, OUTER:, :]
            buf[192:208, :] = far_z
            buf[208:224, :] = jnp.broadcast_to(jnp.where(mask > 0, tag, 0.0), (OUTER, 256))
    lines = jnp.broadcast_to(pline[...].astype(F32) + 1.0, (8, SLOTS))
    for buf in (za, zb):
        buf[32:40, :] = jnp.zeros((8, 128), F32)
        buf[32:40, 0:SLOTS] = lines
    for copy in copies[4:]:
        copy.wait()
    for c in range(3):
        low, high = pos[c, 0:48, :], pos[c, 208:256, :]
        xa[48 * c : 48 * c + 48, :] = jnp.where(even_x, high, low)
        xb[48 * c : 48 * c + 48, :] = jnp.where(even_x, low, high)
        for i in range(16):
            to = 48 * c + 3 * i
            low, high = pos[c, 16 * i : 16 * i + 3, :], pos[c, 16 * i + 13 : 16 * i + 16, :]
            ya[to : to + 3, :] = jnp.where(even_y, high, low)
            yb[to : to + 3, :] = jnp.where(even_y, low, high)
    parts = [pos[c] for c in range(3)]
    low = pack_rows(edge_lanes(parts, 0, None))
    high = pack_rows(edge_lanes(parts, None, 0))
    za[0:32, :] = jnp.where(even_z, high, low)
    zb[0:32, :] = jnp.where(even_z, low, high)


def z_index(far_outer):
    z = far_outer - 3
    below = z < 0
    above = z > 255
    index = jnp.where(below, z + 12, jnp.where(above, z - 256, 0))
    return index, below | above


def z_values(edges, far_outer):
    index, outside = z_index(far_outer)
    out = []
    for c in range(3):
        parts = [
            take128(edges, index[:, t * 128 : (t + 1) * 128] + 3 * c) for t in (0, 1)
        ]
        out.append(jnp.where(outside, jnp.concatenate(parts, axis=1), 0.0))
    return out


def scatter(rows, node, xs, ys):
    for r, value in enumerate(rows):
        for t in (0, 1):
            xs[t, pl.ds(r, SLOTS, stride=8), :] = value[:, t * 128 : (t + 1) * 128]
    places = iota((256, 256), 0).astype(F32).astype(BF16)
    one, zero = jnp.ones((), BF16), jnp.zeros((), BF16)
    for s in range(SLOTS):
        at = slice(8 * s, 8 * s + 8)
        x = jnp.concatenate([xs[0, at, :], xs[1, at, :]], axis=1)
        hi = x.astype(BF16).astype(F32)
        index = node[s : s + 1, :].astype(F32).astype(BF16)
        got = lax.dot_general(
            jnp.concatenate([hi, x - hi], axis=0).astype(BF16),
            jnp.where(places == jnp.broadcast_to(index, (256, 256)), one, zero),
            (((1,), (1,)), ((), ())),
            preferred_element_type=F32,
        )
        total = got[8:16] + got[0:8]
        ys[0, at, :] = total[:, :128]
        ys[1, at, :] = total[:, 128:]
    return [
        jnp.concatenate([ys[t, pl.ds(r, SLOTS, stride=8), :] for t in (0, 1)], axis=1)
        for r in range(len(rows))
    ]


def pair_tile(rows, energy, *residuals):
    lane = iota((rows, 128), 1)
    out = jnp.where(lane == 9, energy, 0.0)
    for n, residual in enumerate(residuals):
        out = jnp.where(lane == 10 + n, residual, out)
    return out


def roll(x, shift):
    return pltpu.roll(x, shift % 128, axis=1) if shift % 128 else x


def pack_edges(parts, first):
    lane = iota((8, 128), 1)
    half, at = first // 128, first % 128
    out = jnp.zeros((8, 128), F32)
    for g in range(4):
        for c in range(3):
            part = parts[c][8 * g : 8 * g + 8, half * 128 : half * 128 + 128]
            for h in (0, 1):
                to = 64 * h + 16 * g + 3 * c
                out = jnp.where((lane >= to) & (lane < to + 3), roll(part, to - at), out)
    return jnp.where(iota((4, 128), 1) < 64, out[0:4], out[4:8])


def unpack_edges(tile, to):
    rows = [roll(tile, to - 64 * h - 16 * g) for g in range(4) for h in (0, 1)]
    return jnp.concatenate(rows, axis=0)


def depth_of(gap, live):
    return jnp.where(iota((SLOTS, 256), 0) < live, jnp.maximum(-gap, 0.0), 0.0)


def total2(x):
    return jnp.sum(jnp.sum(x, axis=0, keepdims=True), axis=1, keepdims=True)


def first_mask(pline):
    shape = (SLOTS, SLOTS)
    row = jnp.broadcast_to(pline.astype(F32), shape)
    col = column(pline.astype(F32), 0, SLOTS)
    again = jnp.where((row == col) & (iota(shape, 1) < iota(shape, 0)), 1.0, 0.0)
    first = jnp.sum(again, axis=1, keepdims=True) == 0.0
    return jnp.broadcast_to(jnp.where(first, 1.0, 0.0), (SLOTS, 256))


def residual_of(near, first):
    square = near[0] * near[0] + near[1] * near[1] + near[2] * near[2]
    return total2(first[...] * square)


def own_index(far):
    z = far[...] - 3
    return jnp.clip(z, 0, 255), (z >= 0) & (z < 256)


def respond(normal, tile, sel, requests, replies, sums, stage, sem):
    for j in range(128):
        stage[j] = tile
    keep = (iota((4, 128), 1) & 15) < 9
    me, k = position()
    stage[jnp.where(k > 0, me - 1, me)] = jnp.where(keep, pack_edges(normal, 0), tile)
    stage[jnp.where(k < 7, me + 1, me)] = jnp.where(keep, pack_edges(normal, 253), tile)
    copy = pltpu.make_async_copy(stage, sums, sem)
    copy.start()
    for pair in (0, 2):
        at = slice(OUTER * pair, OUTER * pair + 2 * OUTER)
        lines = [pick(sel[at, :], normal[c]) for c in range(3)]
        for d, low in ((pair, 0), (pair + 1, OUTER)):
            buf = requests[d]
            index = buf[192:208, :].astype(I32)
            values = take_lanes([v[low : low + OUTER] for v in lines], index)
            answer = jnp.zeros((OUTER, 256), F32)
            for c in range(3):
                answer = answer + buf[144 + 16 * c : 160 + 16 * c, :] * values[c]
            replies[d][...] = answer
    copy.wait()


def own_kernel(normal, node, far, geom, first, sel, change, residual):
    index, inside = own_index(far)
    lines = [pick(sel[0:SLOTS, :], normal[c]) for c in range(3)]
    residual[...] = jnp.broadcast_to(residual_of(lines, first), (1, 128))
    near = take_lanes(lines, node[...])
    other = [pick(sel[SLOTS : 2 * SLOTS, :], normal[c]) for c in range(3)]
    other = take_lanes(other, index)
    moved = jnp.zeros((SLOTS, 256), F32)
    for c in range(3):
        moved = moved + geom[c] * (near[c] - jnp.where(inside, other[c], 0.0))
    change[...] = moved


def base_kernel(
    pos, node, far, geom, pline, fline, live,
    gap_out, own_out, face_out, inverse_out, first, xs, ys,
):
    first[...] = first_mask(pline[...])
    own = pline[...].astype(F32)
    near_col = column(own, 0, SLOTS)
    far_col = column(fline[...].astype(F32), 0, SLOTS)
    x, y, line = decode(far_col.astype(I32))
    inside = (x >= 0) & (x < 16) & (y >= 0) & (y < 16)
    local = jnp.where(inside, line, -2).astype(F32)
    both = jnp.concatenate([near_col, local], axis=0)
    own_out[...] = jnp.broadcast_to(both, (2 * SLOTS, 128))
    xo, yo = x[OUTER:], y[OUTER:]
    even_x, even_y, _ = evens()
    at_x, at_y = jnp.where(even_x, 48, 0), jnp.where(even_y, 48, 0)
    face = jnp.where(xo < 0, at_x + (xo + 3) * 16 + yo, -1)
    face = jnp.where(xo > 15, 48 - at_x + (xo - 16) * 16 + yo, face)
    face = jnp.where(yo < 0, 96 + at_y + xo * 3 + yo + 3, face)
    face = jnp.where(yo > 15, 144 - at_y + xo * 3 + yo - 16, face)
    face_out[...] = hot(iota((OUTER, 192), 1), face)
    ones = jnp.where(iota((SLOTS, 256), 0) < live[...], 1.0, 0.0)
    (counts,) = scatter([ones], node, xs, ys)
    same = hot(jnp.broadcast_to(twice(own), (SLOTS, 2 * SLOTS)), near_col)
    inverse_out[...] = 1.0 / (1.0 + pick(same, counts))
    sel = hot(iota((2 * SLOTS, 256), 1).astype(F32), both)
    index, within = own_index(far)
    got = [pick(sel, pos[c]) for c in range(3)]
    near = take_lanes([v[0:SLOTS] for v in got], node[...])
    other = take_lanes([v[SLOTS:] for v in got], index)
    gap = jnp.zeros((SLOTS, 256), F32)
    for c in range(3):
        gap = gap + geom[c] * (near[c] - jnp.where(within, other[c], 0.0))
    gap_out[...] = gap - geom[3]


def first_kernel(
    gap_in, own, face, inverse, far, geom, pline, live, node,
    xa, xb, ya, yb, za, zb,
    gap_out, normal_out, moved_out, own_sel, out_sel, selz_out, *rest,
):
    *replies, sums, xs, ys, stage, sem = rest
    requests = (xa, xb, ya, yb)
    even_z = evens()[2]
    above = jnp.where(even_z, za[...], zb[...])
    below = jnp.where(even_z, zb[...], za[...])
    wanted = jnp.concatenate(
        [own[:, 0:1]] + [buf[208:224, 0:1] - 1.0 for buf in requests], axis=0
    )
    lines = twice(pline[...].astype(F32))
    sel = hot(jnp.broadcast_to(lines, (128, 2 * SLOTS)), wanted)
    own_sel[...] = sel[0:64]
    out_sel[...] = sel[64:128]
    local = own[SLOTS + OUTER :, 0:1]
    selz = jnp.concatenate([above[32:33, 0:SLOTS], below[32:33, 0:SLOTS]], axis=1) - 1.0
    selz_out[...] = hot(jnp.broadcast_to(twice(selz), (OUTER, 4 * SLOTS)), local)
    edges = jnp.where(
        iota((256, 128), 1) < 9,
        unpack_rows(above[0:32]),
        pltpu.roll(unpack_rows(below[0:32]), 9, axis=1),
    )
    sel = hot(iota((OUTER, 256), 1).astype(F32), local)
    ends = z_values(pick(sel, edges), far[OUTER:, :])
    index, within = own_index(far)
    faces = [
        pick(face[...], jnp.concatenate([buf[48 * c : 48 * c + 48, :] for buf in requests], axis=0))
        for c in range(3)
    ]
    faces = take_lanes(faces, index[OUTER:])
    outer = jnp.zeros((OUTER, 256), F32)
    for c in range(3):
        outer = outer + geom[c, OUTER:, :] * (
            jnp.where(within[OUTER:], faces[c], 0.0) + ends[c]
        )
    gap = gap_in[...] - jnp.concatenate([jnp.zeros((OUTER, 256), F32), outer], axis=0)
    gap_out[...] = gap
    depth = depth_of(gap, live[...])
    tile = pair_tile(4, total2(depth * depth))
    got = scatter([depth * geom[c] for c in range(3)], node, xs, ys)
    normal = [got[c] * inverse[...] for c in range(3)]
    for c in range(3):
        normal_out[c] = normal[c]
        moved_out[c] = jnp.zeros((SLOTS, 256), F32)
    respond(normal, tile, out_sel, requests, replies, sums, stage, sem)


def chunk_sum(got):
    parts = [got[j] for j in range(128)]
    while len(parts) > 1:
        parts = [a + b for a, b in zip(parts[::2], parts[1::2], strict=True)]
    return parts[0][0:1]


def update(gap, change, far, geom, selz, replies, got):
    sums = chunk_sum(got)
    scale = RELAX * (1.0 / (1.0 + sums[0:1, 9:10] / N_PAIRS))
    me, k = position()
    lane = iota((SLOTS, 128), 1)
    above = unpack_edges(got[jnp.where(k < 7, me + 1, me)], 0)
    below = unpack_edges(got[jnp.where(k > 0, me - 1, me)], 9)
    above = jnp.where(lane < 9, above, 0.0)
    below = jnp.where((lane > 8) & (lane < 18), below, 0.0)
    ends = z_values(
        pick(selz[...], jnp.concatenate([above, below], axis=0)), far[OUTER:, :]
    )
    outer = (replies[0][...] + replies[1][...]) + (replies[2][...] + replies[3][...])
    for c in range(3):
        outer = outer + geom[c, OUTER:, :] * ends[c]
    full = change[...] - jnp.concatenate([jnp.zeros((OUTER, 256), F32), outer], axis=0)
    return sums, scale, gap[...] + scale * full


def sweep_kernel(
    last, gap, change, residual, normal, moved, inverse, node, far, geom, live, selz,
    r0, r1, r2, r3, got, *rest,
):
    if last:
        first, own_sel, sums_out, normal_out, moved_out, out, xs, ys = rest
    else:
        *rest, xs, ys, stage, sem = rest
        *requests, out_sel, gap_out, sums_out, normal_out, moved_out = rest[:9]
        *replies, out = rest[9:]
    sums, scale, fresh = update(gap, change, far, geom, selz, (r0, r1, r2, r3), got)
    sums_out[...] = sums
    for c in range(3):
        moved_out[c] = moved[c] + scale * normal[c]
    depth = depth_of(fresh, live[...])
    energy = total2(depth * depth)
    before = residual[:, 0:1]
    if not last:
        tile = pair_tile(4, energy, before)
    found = scatter([depth * geom[c] for c in range(3)], node, xs, ys)
    fresh_normal = [found[c] * inverse[...] for c in range(3)]
    for c in range(3):
        normal_out[c] = fresh_normal[c]
    if last:
        lines = [pick(own_sel[0:SLOTS, :], fresh_normal[c]) for c in range(3)]
        tile = pair_tile(8, energy, before, residual_of(lines, first))
        out[...] = jnp.broadcast_to(tile[0:1, :], (128, 128))
    else:
        gap_out[...] = fresh
        respond(fresh_normal, tile, out_sel, requests, replies, out, stage, sem)


def last_kernel(pos, normal, moved, pline, got, s0, s1, s2, s3, out, history):
    every = [s[0:1, :] for s in (s0, s1, s2, s3)] + [jnp.sum(got[...], axis=0, keepdims=True)]
    scales = [RELAX * (1.0 / (1.0 + s[:, 9:10] / N_PAIRS)) for s in every]
    sel = hot(iota((256, SLOTS), 0), jnp.broadcast_to(pline[...], (256, SLOTS)))
    for c in range(3):
        out[c] = pos[c] + pick(sel, moved[c] + scales[-1] * normal[c])
    for t in range(SWEEPS):
        later = every[t + 1][:, 10:11] if t + 1 < SWEEPS else every[t][:, 11:12]
        residual = scales[t] * scales[t] * later
        history[0:1, t : t + 1] = jnp.sqrt(1.0 + every[t][:, 9:10] / PAIRS_SLOTS)
        history[1:2, t : t + 1] = jnp.sqrt(1.0 + residual / NODES_BLK)


within = pltpu.with_memory_space_constraint


def call(kernel, outs, args, scratch=(), inputs=False):
    vmem = pl.BlockSpec(memory_space=pltpu.VMEM)
    hbm = pl.BlockSpec(memory_space=pltpu.HBM)
    return pl.pallas_call(
        kernel,
        out_shape=outs,
        in_specs=[hbm if inputs else vmem] * len(args),
        out_specs=[hbm if o is CHUNKS else vmem for o in outs],
        scratch_shapes=list(scratch),
        compiler_params=pltpu.CompilerParams(vmem_limit_bytes=12 * 2**20),
    )(*(args if inputs else [within(x, pltpu.VMEM) for x in args]))


CHUNKS = pltpu.HBM((128, 4, 128), F32)


def shape(*dims, dtype=F32):
    return pltpu.VMEM(dims, dtype)


def swap(x, axis, second):
    count = lax.axis_size(axis)
    pairs = [(i, (i + 1) % count) for i in range(int(second), count, 2)]
    return lax.ppermute(x, axis, pairs + [(b, a) for a, b in pairs])


def swap_all(arrays):
    axes = ("gx", "gx", "gy", "gy", GZ, GZ)
    return [swap(x, axis, n % 2) for n, (x, axis) in enumerate(zip(arrays, axes))]


def local(positions, pair_node, pair_line, pair_far, far_line, pair_geom, live_blocks):
    pos = positions.reshape(3, 256, 256)
    node = pair_node.reshape(SLOTS, 256)
    far = pair_far.reshape(SLOTS, 256)
    geom = pair_geom.reshape(SLOTS, 4, 256)
    pline = pair_line.reshape(1, SLOTS)
    fline = far_line.reshape(1, SLOTS)
    live = live_blocks.reshape(1, 1)
    work = [pltpu.VMEM((2, 256, 128), F32)] * 2
    send = [pltpu.VMEM((128, 4, 128), F32), pltpu.SemaphoreType.DMA]

    face, ends = shape(224, 256), shape(40, 128)
    flat = shape(SLOTS, 256)
    flat_i = shape(SLOTS, 256, dtype=I32)
    few = shape(1, SLOTS, dtype=I32)
    packed = call(
        pack_kernel,
        [face] * 4
        + [ends] * 2
        + [shape(4, SLOTS, 256), shape(3, 256, 256), flat_i, flat_i, few, few]
        + [shape(1, 1, dtype=I32)],
        [within(x, pltpu.HBM) for x in (pos, node, far, geom, pline, fline)] + [live],
        [pltpu.VMEM((SLOTS, 4, 256), F32), pltpu.SemaphoreType.DMA((7,))],
        inputs=True,
    )
    *six, geom, pos, node, far, pline, fline, live = packed
    *requests, za, zb = swap_all(six)
    triple = shape(3, SLOTS, 256)
    outs = [shape(OUTER, 256)] * 4 + [CHUNKS]
    gap, own, face, inverse, first = call(
        base_kernel,
        [
            flat,
            shape(2 * SLOTS, 128),
            shape(OUTER, 192, dtype=BF16),
            flat,
            flat,
        ],
        [pos, node, far, geom, pline, fline, live],
        work,
    )
    choice = shape(2 * SLOTS, 2 * SLOTS, dtype=BF16)
    gap, normal, moved, own_sel, out_sel, selz, *sent, sums = call(
        first_kernel,
        [flat, triple, triple, choice, choice, shape(OUTER, 4 * SLOTS, dtype=BF16)] + outs,
        [gap, own, face, inverse, far, geom, pline, live, node] + requests + [za, zb],
        work + send,
    )
    totals = []
    row = shape(1, 128)
    for t in range(1, SWEEPS):
        replies = swap_all(sent)
        got = lax.all_to_all(sums, ALL, 0, 0, tiled=True)
        change, residual = call(
            own_kernel, [flat, row], [normal, node, far, geom, first, own_sel]
        )
        args = [
            gap, change, residual, normal, moved, inverse, node, far, geom, live, selz,
        ]
        args = args + replies + [got]
        if t + 1 < SWEEPS:
            gap, total, normal, moved, *sent, sums = call(
                functools.partial(sweep_kernel, False),
                [flat, row, triple, triple] + outs,
                args + requests + [out_sel],
                work + send,
            )
        else:
            total, normal, moved, sums = call(
                functools.partial(sweep_kernel, True),
                [row, triple, triple, shape(128, 128)],
                args + [first, own_sel],
                work,
            )
        totals.append(total)
    sums = sums.reshape(128, 1, 128)
    got = lax.all_to_all(sums, ALL, 0, 0, tiled=True).reshape(128, 128)
    corrected, history = call(
        last_kernel,
        [jax.ShapeDtypeStruct((3, 256, 256), F32), jax.ShapeDtypeStruct((2, SWEEPS), F32)],
        [pos, normal, moved, pline, got, *totals],
    )
    return corrected.reshape(positions.shape), history


def solution(mesh):
    finer = Mesh(
        mesh.devices.reshape(mesh.shape["gx"], mesh.shape["gy"], 4, 2), ("gx", "gy", "gz_0", "gz_1")
    )
    placed = (
        P(None, "gx", "gy", GZ),
        P("gx", "gy", GZ, None, None),
        P("gx", "gy", GZ, None),
        P("gx", "gy", GZ, None, None),
        P("gx", "gy", GZ, None),
        P("gx", "gy", GZ, None, None, None),
        P("gx", "gy", GZ),
    )
    return jax.shard_map(
        local,
        mesh=finer,
        in_specs=placed,
        out_specs=(P(None, "gx", "gy", GZ), P()),
        check_vma=False,
    )
```

```python
import functools

import jax
import jax.numpy as jnp
from jax import lax
from jax.experimental import pallas as pl
from jax.experimental.pallas import tpu as pltpu
from jax.sharding import Mesh
from jax.sharding import PartitionSpec as P

SWEEPS = 5
RELAX = 0.9
XY = ("gx", "gy")
GZ = ("gz_0", "gz_1")
ALL = ("gx", "gy", "gz_0", "gz_1")
F32 = jnp.float32
BF16 = jnp.bfloat16
I32 = jnp.int32
SLOTS = 32
OUTER = 16
N_PAIRS = 1048576
NODES_BLK = 65536
PAIRS_SLOTS = 8192


def iota(shape, dim):
    return lax.broadcasted_iota(I32, shape, dim)


def pick(sel, x):
    hi = x.astype(BF16)
    mid = (x - hi.astype(F32)).astype(BF16)
    dot = functools.partial(jnp.dot, preferred_element_type=F32)
    if sel.shape[1] == 2 * x.shape[0]:
        return dot(sel, jnp.concatenate([hi, mid], axis=0))
    return dot(sel, mid) + dot(sel, hi)


def hot(a, b):
    return jnp.where(a == b, 1.0, 0.0).astype(BF16)


def twice(row):
    return jnp.concatenate([row, row], axis=1)


def column(row, first, count):
    shape = (count, row.shape[1])
    chosen = iota(shape, 0) + first == iota(shape, 1)
    return jnp.sum(jnp.where(chosen, jnp.broadcast_to(row, shape), 0.0), axis=1, keepdims=True)


def take128(x, index):
    return jnp.take_along_axis(x, index, axis=1, mode="promise_in_bounds")


def take_lanes(xs, index):
    columns = [[] for _ in xs]
    for t in (0, 1):
        cut = index[:, t * 128 : (t + 1) * 128]
        low = cut & 127
        high = cut > 127
        rows = [[] for _ in xs]
        for g in range(0, index.shape[0], 8):
            at = slice(g, g + 8)
            for x, row in zip(xs, rows, strict=True):
                a = take128(x[at, :128], low[at])
                b = take128(x[at, 128:], low[at])
                row.append(jnp.where(high[at], b, a))
        for column_parts, row in zip(columns, rows, strict=True):
            column_parts.append(jnp.concatenate(row, axis=0))
    return [jnp.concatenate(parts, axis=1) for parts in columns]


def decode(far_line):
    x = (far_line * 2979) >> 16
    y = far_line - 22 * x - 3
    x = x - 3
    return x, y, (x & 15) * 16 + (y & 15)


def edge_lanes(parts, low_first, high_first):
    lane = iota((parts[0].shape[0], 128), 1)
    out = jnp.zeros((parts[0].shape[0], 128), F32)
    for c in range(3):
        for first, half, at in ((low_first, 0, 0), (high_first, 1, 125)):
            if first is None:
                continue
            to = first + 3 * c
            moved = parts[c][:, half * 128 : half * 128 + 128]
            if (to - at) % 128:
                moved = pltpu.roll(moved, (to - at) % 128, axis=1)
            out = jnp.where((lane >= to) & (lane < to + 3), moved, out)
    return out


def pack_rows(tall):
    lane = iota((SLOTS, 128), 1)
    out = jnp.zeros((SLOTS, 128), F32)
    for g in range(8):
        part = tall[32 * g : 32 * g + 32]
        part = pltpu.roll(part, 16 * g, axis=1) if g else part
        out = jnp.where((lane >= 16 * g) & (lane < 16 * g + 16), part, out)
    return out


def unpack_rows(flat):
    return jnp.concatenate(
        [flat] + [pltpu.roll(flat, 128 - 16 * g, axis=1) for g in range(1, 8)], axis=0
    )


def position():
    k = lax.axis_index(GZ)
    return (lax.axis_index("gx") * 4 + lax.axis_index("gy")) * 8 + k, k


def evens():
    return [lax.axis_index(axis) % 2 == 0 for axis in ("gx", "gy", "gz_1")]


def pack_kernel(
    pos_in, node_in, far_in, geom_in, pline_in, fline_in, live_in,
    xa, xb, ya, yb, za, zb, geom, pos, node, far, pline, fline, live,
    geom_raw, sems,
):
    copies = [
        pltpu.make_async_copy(source, target, sems.at[n])
        for n, (source, target) in enumerate(
            (
                (fline_in, fline),
                (far_in, far),
                (geom_in, geom_raw),
                (pline_in, pline),
                (pos_in, pos),
                (node_in, node),
                (live_in, live),
            )
        )
    ]
    for copy in copies:
        copy.start()
    for copy in copies[:4]:
        copy.wait()
    for c in range(4):
        geom[c] = geom_raw[:, c, :]
    fcol = column(fline[...].astype(F32), OUTER, OUTER).astype(I32)
    x, y, line = decode(fcol)
    tag = (line + 1).astype(F32)
    far_z = jnp.clip(far[OUTER:, :] - 3, 0, 255).astype(F32)
    even_x, even_y, even_z = evens()
    low = (x < 0).astype(I32), (y < 0).astype(I32)
    high = (x > 15).astype(I32), (y > 15).astype(I32)
    for axis, even, first, second in ((0, even_x, xa, xb), (1, even_y, ya, yb)):
        for buf, mask in (
            (first, jnp.where(even, high[axis], low[axis])),
            (second, jnp.where(even, low[axis], high[axis])),
        ):
            for c in range(3):
                buf[144 + 16 * c : 160 + 16 * c, :] = geom[c, OUTER:, :]
            buf[192:208, :] = far_z
            buf[208:224, :] = jnp.broadcast_to(jnp.where(mask > 0, tag, 0.0), (OUTER, 256))
    lines = jnp.broadcast_to(pline[...].astype(F32) + 1.0, (8, SLOTS))
    for buf in (za, zb):
        buf[32:40, :] = jnp.zeros((8, 128), F32)
        buf[32:40, 0:SLOTS] = lines
    for copy in copies[4:]:
        copy.wait()
    for c in range(3):
        low, high = pos[c, 0:48, :], pos[c, 208:256, :]
        xa[48 * c : 48 * c + 48, :] = jnp.where(even_x, high, low)
        xb[48 * c : 48 * c + 48, :] = jnp.where(even_x, low, high)
        for i in range(16):
            to = 48 * c + 3 * i
            low, high = pos[c, 16 * i : 16 * i + 3, :], pos[c, 16 * i + 13 : 16 * i + 16, :]
            ya[to : to + 3, :] = jnp.where(even_y, high, low)
            yb[to : to + 3, :] = jnp.where(even_y, low, high)
    parts = [pos[c] for c in range(3)]
    low = pack_rows(edge_lanes(parts, 0, None))
    high = pack_rows(edge_lanes(parts, None, 0))
    za[0:32, :] = jnp.where(even_z, high, low)
    zb[0:32, :] = jnp.where(even_z, low, high)


def z_index(far_outer):
    z = far_outer - 3
    below = z < 0
    above = z > 255
    index = jnp.where(below, z + 12, jnp.where(above, z - 256, 0))
    return index, below | above


def z_values(edges, far_outer):
    index, outside = z_index(far_outer)
    out = []
    for c in range(3):
        parts = [
            take128(edges, index[:, t * 128 : (t + 1) * 128] + 3 * c) for t in (0, 1)
        ]
        out.append(jnp.where(outside, jnp.concatenate(parts, axis=1), 0.0))
    return out


def scatter(rows, node, xs, ys):
    for r, value in enumerate(rows):
        for t in (0, 1):
            xs[t, pl.ds(r, SLOTS, stride=8), :] = value[:, t * 128 : (t + 1) * 128]
    places = iota((256, 256), 0).astype(F32).astype(BF16)
    one, zero = jnp.ones((), BF16), jnp.zeros((), BF16)
    for s in range(SLOTS):
        at = slice(8 * s, 8 * s + 8)
        x = jnp.concatenate([xs[0, at, :], xs[1, at, :]], axis=1)
        hi = x.astype(BF16).astype(F32)
        index = node[s : s + 1, :].astype(F32).astype(BF16)
        got = lax.dot_general(
            jnp.concatenate([hi, x - hi], axis=0).astype(BF16),
            jnp.where(places == jnp.broadcast_to(index, (256, 256)), one, zero),
            (((1,), (1,)), ((), ())),
            preferred_element_type=F32,
        )
        total = got[8:16] + got[0:8]
        ys[0, at, :] = total[:, :128]
        ys[1, at, :] = total[:, 128:]
    return [
        jnp.concatenate([ys[t, pl.ds(r, SLOTS, stride=8), :] for t in (0, 1)], axis=1)
        for r in range(len(rows))
    ]


def pair_tile(rows, energy, *residuals):
    lane = iota((rows, 128), 1)
    out = jnp.where(lane == 9, energy, 0.0)
    for n, residual in enumerate(residuals):
        out = jnp.where(lane == 10 + n, residual, out)
    return out


def roll(x, shift):
    return pltpu.roll(x, shift % 128, axis=1) if shift % 128 else x


def pack_edges(parts, first):
    lane = iota((8, 128), 1)
    half, at = first // 128, first % 128
    out = jnp.zeros((8, 128), F32)
    for g in range(4):
        for c in range(3):
            part = parts[c][8 * g : 8 * g + 8, half * 128 : half * 128 + 128]
            for h in (0, 1):
                to = 64 * h + 16 * g + 3 * c
                out = jnp.where((lane >= to) & (lane < to + 3), roll(part, to - at), out)
    return jnp.where(iota((4, 128), 1) < 64, out[0:4], out[4:8])


def unpack_edges(tile, to):
    rows = [roll(tile, to - 64 * h - 16 * g) for g in range(4) for h in (0, 1)]
    return jnp.concatenate(rows, axis=0)


def depth_of(gap, live):
    return jnp.where(iota((SLOTS, 256), 0) < live, jnp.maximum(-gap, 0.0), 0.0)


def total2(x):
    return jnp.sum(jnp.sum(x, axis=0, keepdims=True), axis=1, keepdims=True)


def first_mask(pline):
    shape = (SLOTS, SLOTS)
    row = jnp.broadcast_to(pline.astype(F32), shape)
    col = column(pline.astype(F32), 0, SLOTS)
    again = jnp.where((row == col) & (iota(shape, 1) < iota(shape, 0)), 1.0, 0.0)
    first = jnp.sum(again, axis=1, keepdims=True) == 0.0
    return jnp.broadcast_to(jnp.where(first, 1.0, 0.0), (SLOTS, 256))


def residual_of(near, first):
    square = near[0] * near[0] + near[1] * near[1] + near[2] * near[2]
    return total2(first[...] * square)


def own_index(far):
    z = far[...] - 3
    return jnp.clip(z, 0, 255), (z >= 0) & (z < 256)


def respond(normal, tile, sel, requests, replies, sums):
    for j in range(128):
        sums[j] = tile
    keep = (iota((4, 128), 1) & 15) < 9
    me, k = position()
    sums[jnp.where(k > 0, me - 1, me)] = jnp.where(keep, pack_edges(normal, 0), tile)
    sums[jnp.where(k < 7, me + 1, me)] = jnp.where(keep, pack_edges(normal, 253), tile)
    for pair in (0, 2):
        at = slice(OUTER * pair, OUTER * pair + 2 * OUTER)
        lines = [pick(sel[at, :], normal[c]) for c in range(3)]
        for d, low in ((pair, 0), (pair + 1, OUTER)):
            buf = requests[d]
            index = buf[192:208, :].astype(I32)
            values = take_lanes([v[low : low + OUTER] for v in lines], index)
            answer = jnp.zeros((OUTER, 256), F32)
            for c in range(3):
                answer = answer + buf[144 + 16 * c : 160 + 16 * c, :] * values[c]
            replies[d][...] = answer


def own_kernel(normal, node, far, geom, first, sel, change, residual):
    index, inside = own_index(far)
    lines = [pick(sel[0:SLOTS, :], normal[c]) for c in range(3)]
    residual[...] = jnp.broadcast_to(residual_of(lines, first), (1, 128))
    near = take_lanes(lines, node[...])
    other = [pick(sel[SLOTS : 2 * SLOTS, :], normal[c]) for c in range(3)]
    other = take_lanes(other, index)
    moved = jnp.zeros((SLOTS, 256), F32)
    for c in range(3):
        moved = moved + geom[c] * (near[c] - jnp.where(inside, other[c], 0.0))
    change[...] = moved


def base_kernel(
    pos, node, far, geom, pline, fline, live,
    gap_out, own_out, face_out, inverse_out, first, xs, ys,
):
    first[...] = first_mask(pline[...])
    own = pline[...].astype(F32)
    near_col = column(own, 0, SLOTS)
    far_col = column(fline[...].astype(F32), 0, SLOTS)
    x, y, line = decode(far_col.astype(I32))
    inside = (x >= 0) & (x < 16) & (y >= 0) & (y < 16)
    local = jnp.where(inside, line, -2).astype(F32)
    both = jnp.concatenate([near_col, local], axis=0)
    own_out[...] = jnp.broadcast_to(both, (2 * SLOTS, 128))
    xo, yo = x[OUTER:], y[OUTER:]
    even_x, even_y, _ = evens()
    at_x, at_y = jnp.where(even_x, 48, 0), jnp.where(even_y, 48, 0)
    face = jnp.where(xo < 0, at_x + (xo + 3) * 16 + yo, -1)
    face = jnp.where(xo > 15, 48 - at_x + (xo - 16) * 16 + yo, face)
    face = jnp.where(yo < 0, 96 + at_y + xo * 3 + yo + 3, face)
    face = jnp.where(yo > 15, 144 - at_y + xo * 3 + yo - 16, face)
    face_out[...] = hot(iota((OUTER, 192), 1), face)
    ones = jnp.where(iota((SLOTS, 256), 0) < live[...], 1.0, 0.0)
    (counts,) = scatter([ones], node, xs, ys)
    same = hot(jnp.broadcast_to(twice(own), (SLOTS, 2 * SLOTS)), near_col)
    inverse_out[...] = 1.0 / (1.0 + pick(same, counts))
    sel = hot(iota((2 * SLOTS, 256), 1).astype(F32), both)
    index, within = own_index(far)
    got = [pick(sel, pos[c]) for c in range(3)]
    near = take_lanes([v[0:SLOTS] for v in got], node[...])
    other = take_lanes([v[SLOTS:] for v in got], index)
    gap = jnp.zeros((SLOTS, 256), F32)
    for c in range(3):
        gap = gap + geom[c] * (near[c] - jnp.where(within, other[c], 0.0))
    gap_out[...] = gap - geom[3]


def first_kernel(
    gap_in, own, face, inverse, far, geom, pline, live, node,
    xa, xb, ya, yb, za, zb,
    gap_out, normal_out, moved_out, own_sel, out_sel, selz_out, *rest,
):
    *replies, sums, xs, ys = rest
    requests = (xa, xb, ya, yb)
    even_z = evens()[2]
    above = jnp.where(even_z, za[...], zb[...])
    below = jnp.where(even_z, zb[...], za[...])
    wanted = jnp.concatenate(
        [own[:, 0:1]] + [buf[208:224, 0:1] - 1.0 for buf in requests], axis=0
    )
    lines = twice(pline[...].astype(F32))
    sel = hot(jnp.broadcast_to(lines, (128, 2 * SLOTS)), wanted)
    own_sel[...] = sel[0:64]
    out_sel[...] = sel[64:128]
    local = own[SLOTS + OUTER :, 0:1]
    selz = jnp.concatenate([above[32:33, 0:SLOTS], below[32:33, 0:SLOTS]], axis=1) - 1.0
    selz_out[...] = hot(jnp.broadcast_to(twice(selz), (OUTER, 4 * SLOTS)), local)
    edges = jnp.where(
        iota((256, 128), 1) < 9,
        unpack_rows(above[0:32]),
        pltpu.roll(unpack_rows(below[0:32]), 9, axis=1),
    )
    sel = hot(iota((OUTER, 256), 1).astype(F32), local)
    ends = z_values(pick(sel, edges), far[OUTER:, :])
    index, within = own_index(far)
    faces = [
        pick(face[...], jnp.concatenate([buf[48 * c : 48 * c + 48, :] for buf in requests], axis=0))
        for c in range(3)
    ]
    faces = take_lanes(faces, index[OUTER:])
    outer = jnp.zeros((OUTER, 256), F32)
    for c in range(3):
        outer = outer + geom[c, OUTER:, :] * (
            jnp.where(within[OUTER:], faces[c], 0.0) + ends[c]
        )
    gap = gap_in[...] - jnp.concatenate([jnp.zeros((OUTER, 256), F32), outer], axis=0)
    gap_out[...] = gap
    depth = depth_of(gap, live[...])
    tile = pair_tile(4, total2(depth * depth))
    got = scatter([depth * geom[c] for c in range(3)], node, xs, ys)
    normal = [got[c] * inverse[...] for c in range(3)]
    for c in range(3):
        normal_out[c] = normal[c]
        moved_out[c] = jnp.zeros((SLOTS, 256), F32)
    respond(normal, tile, out_sel, requests, replies, sums)


def chunk_sum(got):
    parts = [got[j] for j in range(128)]
    while len(parts) > 1:
        parts = [a + b for a, b in zip(parts[::2], parts[1::2], strict=True)]
    return parts[0][0:1]


def update(gap, change, far, geom, selz, replies, got):
    sums = chunk_sum(got)
    scale = RELAX * (1.0 / (1.0 + sums[0:1, 9:10] / N_PAIRS))
    me, k = position()
    lane = iota((SLOTS, 128), 1)
    above = unpack_edges(got[jnp.where(k < 7, me + 1, me)], 0)
    below = unpack_edges(got[jnp.where(k > 0, me - 1, me)], 9)
    above = jnp.where(lane < 9, above, 0.0)
    below = jnp.where((lane > 8) & (lane < 18), below, 0.0)
    ends = z_values(
        pick(selz[...], jnp.concatenate([above, below], axis=0)), far[OUTER:, :]
    )
    outer = (replies[0][...] + replies[1][...]) + (replies[2][...] + replies[3][...])
    for c in range(3):
        outer = outer + geom[c, OUTER:, :] * ends[c]
    full = change[...] - jnp.concatenate([jnp.zeros((OUTER, 256), F32), outer], axis=0)
    return sums, scale, gap[...] + scale * full


def sweep_kernel(
    last, gap, change, residual, normal, moved, inverse, node, far, geom, live, selz,
    r0, r1, r2, r3, got, *rest,
):
    if last:
        first, own_sel, sums_out, normal_out, moved_out, out, xs, ys = rest
    else:
        *rest, xs, ys = rest
        *requests, out_sel, gap_out, sums_out, normal_out, moved_out = rest[:9]
        *replies, out = rest[9:]
    sums, scale, fresh = update(gap, change, far, geom, selz, (r0, r1, r2, r3), got)
    sums_out[...] = sums
    for c in range(3):
        moved_out[c] = moved[c] + scale * normal[c]
    depth = depth_of(fresh, live[...])
    energy = total2(depth * depth)
    before = residual[:, 0:1]
    if not last:
        tile = pair_tile(4, energy, before)
    found = scatter([depth * geom[c] for c in range(3)], node, xs, ys)
    fresh_normal = [found[c] * inverse[...] for c in range(3)]
    for c in range(3):
        normal_out[c] = fresh_normal[c]
    if last:
        lines = [pick(own_sel[0:SLOTS, :], fresh_normal[c]) for c in range(3)]
        tile = pair_tile(8, energy, before, residual_of(lines, first))
        out[...] = jnp.broadcast_to(tile[0:1, :], (128, 128))
    else:
        gap_out[...] = fresh
        respond(fresh_normal, tile, out_sel, requests, replies, out)


def last_kernel(pos, normal, moved, pline, got, s0, s1, s2, s3, out, history):
    every = [s[0:1, :] for s in (s0, s1, s2, s3)] + [jnp.sum(got[...], axis=0, keepdims=True)]
    scales = [RELAX * (1.0 / (1.0 + s[:, 9:10] / N_PAIRS)) for s in every]
    sel = hot(iota((256, SLOTS), 0), jnp.broadcast_to(pline[...], (256, SLOTS)))
    for c in range(3):
        out[c] = pos[c] + pick(sel, moved[c] + scales[-1] * normal[c])
    for t in range(SWEEPS):
        later = every[t + 1][:, 10:11] if t + 1 < SWEEPS else every[t][:, 11:12]
        residual = scales[t] * scales[t] * later
        history[0:1, t : t + 1] = jnp.sqrt(1.0 + every[t][:, 9:10] / PAIRS_SLOTS)
        history[1:2, t : t + 1] = jnp.sqrt(1.0 + residual / NODES_BLK)


within = pltpu.with_memory_space_constraint


def call(kernel, outs, args, scratch=(), inputs=False):
    vmem = pl.BlockSpec(memory_space=pltpu.VMEM)
    hbm = pl.BlockSpec(memory_space=pltpu.HBM)
    return pl.pallas_call(
        kernel,
        out_shape=outs,
        in_specs=[hbm if inputs else vmem] * len(args),
        out_specs=[vmem] * len(outs),
        scratch_shapes=list(scratch),
        compiler_params=pltpu.CompilerParams(
            vmem_limit_bytes=12 * 2**20,
        ),
    )(*(args if inputs else [within(x, pltpu.VMEM) for x in args]))


def shape(*dims, dtype=F32):
    return pltpu.VMEM(dims, dtype)


def swap(x, axis, second):
    count = lax.axis_size(axis)
    pairs = [(i, (i + 1) % count) for i in range(int(second), count, 2)]
    return lax.ppermute(x, axis, pairs + [(b, a) for a, b in pairs])


def swap_all(arrays):
    axes = ("gx", "gx", "gy", "gy", GZ, GZ)
    return [swap(x, axis, n % 2) for n, (x, axis) in enumerate(zip(arrays, axes))]


def local(positions, pair_node, pair_line, pair_far, far_line, pair_geom, live_blocks):
    pos = positions.reshape(3, 256, 256)
    node = pair_node.reshape(SLOTS, 256)
    far = pair_far.reshape(SLOTS, 256)
    geom = pair_geom.reshape(SLOTS, 4, 256)
    pline = pair_line.reshape(1, SLOTS)
    fline = far_line.reshape(1, SLOTS)
    live = live_blocks.reshape(1, 1)
    work = [pltpu.VMEM((2, 256, 128), F32)] * 2

    face, ends = shape(224, 256), shape(40, 128)
    flat = shape(SLOTS, 256)
    flat_i = shape(SLOTS, 256, dtype=I32)
    few = shape(1, SLOTS, dtype=I32)
    packed = call(
        pack_kernel,
        [face] * 4
        + [ends] * 2
        + [shape(4, SLOTS, 256), shape(3, 256, 256), flat_i, flat_i, few, few]
        + [shape(1, 1, dtype=I32)],
        [within(x, pltpu.HBM) for x in (pos, node, far, geom, pline, fline)] + [live],
        [pltpu.VMEM((SLOTS, 4, 256), F32), pltpu.SemaphoreType.DMA((7,))],
        inputs=True,
    )
    *six, geom, pos, node, far, pline, fline, live = packed
    *requests, za, zb = swap_all(six)
    triple = shape(3, SLOTS, 256)
    outs = [shape(OUTER, 256)] * 4 + [shape(128, 4, 128)]
    gap, own, face, inverse, first = call(
        base_kernel,
        [
            flat,
            shape(2 * SLOTS, 128),
            shape(OUTER, 192, dtype=BF16),
            flat,
            flat,
        ],
        [pos, node, far, geom, pline, fline, live],
        work,
    )
    choice = shape(2 * SLOTS, 2 * SLOTS, dtype=BF16)
    gap, normal, moved, own_sel, out_sel, selz, *sent, sums = call(
        first_kernel,
        [flat, triple, triple, choice, choice, shape(OUTER, 4 * SLOTS, dtype=BF16)] + outs,
        [gap, own, face, inverse, far, geom, pline, live, node] + requests + [za, zb],
        work,
    )
    totals = []
    row = shape(1, 128)
    for t in range(1, SWEEPS):
        replies = swap_all(sent)
        got = lax.all_to_all(sums, ALL, 0, 0, tiled=True)
        change, residual = call(
            own_kernel, [flat, row], [normal, node, far, geom, first, own_sel]
        )
        args = [
            gap, change, residual, normal, moved, inverse, node, far, geom, live, selz,
        ]
        args = args + replies + [got]
        if t + 1 < SWEEPS:
            gap, total, normal, moved, *sent, sums = call(
                functools.partial(sweep_kernel, False),
                [flat, row, triple, triple] + outs,
                args + requests + [out_sel],
                work,
            )
        else:
            total, normal, moved, sums = call(
                functools.partial(sweep_kernel, True),
                [row, triple, triple, shape(128, 128)],
                args + [first, own_sel],
                work,
            )
        totals.append(total)
    sums = sums.reshape(128, 1, 128)
    got = lax.all_to_all(sums, ALL, 0, 0, tiled=True).reshape(128, 128)
    corrected, history = call(
        last_kernel,
        [jax.ShapeDtypeStruct((3, 256, 256), F32), jax.ShapeDtypeStruct((2, SWEEPS), F32)],
        [pos, normal, moved, pline, got, *totals],
    )
    return corrected.reshape(positions.shape), history


def solution(mesh):
    finer = Mesh(
        mesh.devices.reshape(mesh.shape["gx"], mesh.shape["gy"], 4, 2), ("gx", "gy", "gz_0", "gz_1")
    )
    placed = (
        P(None, "gx", "gy", GZ),
        P("gx", "gy", GZ, None, None),
        P("gx", "gy", GZ, None),
        P("gx", "gy", GZ, None, None),
        P("gx", "gy", GZ, None),
        P("gx", "gy", GZ, None, None, None),
        P("gx", "gy", GZ),
    )
    return jax.shard_map(
        local,
        mesh=finer,
        in_specs=placed,
        out_specs=(P(None, "gx", "gy", GZ), P()),
        check_vma=False,
    )
```

```python
import functools

import jax
import jax.numpy as jnp
from jax import lax
from jax.experimental import pallas as pl
from jax.experimental.pallas import tpu as pltpu
from jax.sharding import Mesh
from jax.sharding import PartitionSpec as P

SWEEPS = 5
RELAX = 0.9
XY = ("gx", "gy")
GZ = ("gz_0", "gz_1")
ALL = ("gx", "gy", "gz_0", "gz_1")
F32 = jnp.float32
BF16 = jnp.bfloat16
I32 = jnp.int32
SLOTS = 32
OUTER = 16
N_PAIRS = 1048576
NODES_BLK = 65536
PAIRS_SLOTS = 8192


def iota(shape, dim):
    return lax.broadcasted_iota(I32, shape, dim)


def pick(sel, x):
    hi = x.astype(BF16)
    mid = (x - hi.astype(F32)).astype(BF16)
    dot = functools.partial(jnp.dot, preferred_element_type=F32)
    if sel.shape[1] == 2 * x.shape[0]:
        return dot(sel, jnp.concatenate([hi, mid], axis=0))
    return dot(sel, mid) + dot(sel, hi)


def hot(a, b):
    return jnp.where(a == b, 1.0, 0.0).astype(BF16)


def twice(row):
    return jnp.concatenate([row, row], axis=1)


def column(row, first, count):
    shape = (count, row.shape[1])
    chosen = iota(shape, 0) + first == iota(shape, 1)
    return jnp.sum(jnp.where(chosen, jnp.broadcast_to(row, shape), 0.0), axis=1, keepdims=True)


def take128(x, index):
    return jnp.take_along_axis(x, index, axis=1, mode="promise_in_bounds")


def take_lanes(xs, index):
    columns = [[] for _ in xs]
    for t in (0, 1):
        cut = index[:, t * 128 : (t + 1) * 128]
        low = cut & 127
        high = cut > 127
        rows = [[] for _ in xs]
        for g in range(0, index.shape[0], 8):
            at = slice(g, g + 8)
            for x, row in zip(xs, rows, strict=True):
                a = take128(x[at, :128], low[at])
                b = take128(x[at, 128:], low[at])
                row.append(jnp.where(high[at], b, a))
        for column_parts, row in zip(columns, rows, strict=True):
            column_parts.append(jnp.concatenate(row, axis=0))
    return [jnp.concatenate(parts, axis=1) for parts in columns]


def decode(far_line):
    x = (far_line * 2979) >> 16
    y = far_line - 22 * x - 3
    x = x - 3
    return x, y, (x & 15) * 16 + (y & 15)


def edge_lanes(parts, low_first, high_first):
    lane = iota((parts[0].shape[0], 128), 1)
    out = jnp.zeros((parts[0].shape[0], 128), F32)
    for c in range(3):
        for first, half, at in ((low_first, 0, 0), (high_first, 1, 125)):
            if first is None:
                continue
            to = first + 3 * c
            moved = parts[c][:, half * 128 : half * 128 + 128]
            if (to - at) % 128:
                moved = pltpu.roll(moved, (to - at) % 128, axis=1)
            out = jnp.where((lane >= to) & (lane < to + 3), moved, out)
    return out


def pack_rows(tall):
    lane = iota((SLOTS, 128), 1)
    out = jnp.zeros((SLOTS, 128), F32)
    for g in range(8):
        part = tall[32 * g : 32 * g + 32]
        part = pltpu.roll(part, 16 * g, axis=1) if g else part
        out = jnp.where((lane >= 16 * g) & (lane < 16 * g + 16), part, out)
    return out


def unpack_rows(flat):
    return jnp.concatenate(
        [flat] + [pltpu.roll(flat, 128 - 16 * g, axis=1) for g in range(1, 8)], axis=0
    )


def position():
    k = lax.axis_index(GZ)
    return (lax.axis_index("gx") * 4 + lax.axis_index("gy")) * 8 + k, k


def evens():
    return [lax.axis_index(axis) % 2 == 0 for axis in ("gx", "gy", "gz_1")]


def pack_kernel(
    pos_in, node_in, far_in, geom_in, pline_in, fline_in, live_in,
    xa, xb, ya, yb, za, zb, geom, pos, node, far, pline, fline, live,
    geom_raw, sems,
):
    copies = [
        pltpu.make_async_copy(source, target, sems.at[n])
        for n, (source, target) in enumerate(
            (
                (fline_in, fline),
                (far_in, far),
                (geom_in, geom_raw),
                (pline_in, pline),
                (pos_in, pos),
                (node_in, node),
                (live_in, live),
            )
        )
    ]
    for copy in copies:
        copy.start()
    for copy in copies[:4]:
        copy.wait()
    for c in range(4):
        geom[c] = geom_raw[:, c, :]
    x, y, line = decode(fline[...])
    tag = (line + 1).astype(F32)
    far_z = jnp.clip(far[OUTER:, :] - 3, 0, 255).astype(F32)
    even_x, even_y, even_z = evens()
    low = (x < 0).astype(I32), (y < 0).astype(I32)
    high = (x > 15).astype(I32), (y > 15).astype(I32)
    for axis, even, first, second in ((0, even_x, xa, xb), (1, even_y, ya, yb)):
        for buf, mask in (
            (first, jnp.where(even, high[axis], low[axis])),
            (second, jnp.where(even, low[axis], high[axis])),
        ):
            for c in range(3):
                buf[144 + 16 * c : 160 + 16 * c, :] = geom[c, OUTER:, :]
            buf[192:208, :] = far_z
            buf[208:216, :] = jnp.zeros((8, 256), F32)
            buf[208:216, 0:SLOTS] = jnp.broadcast_to(jnp.where(mask > 0, tag, 0.0), (8, SLOTS))
    lines = jnp.broadcast_to(pline[...].astype(F32) + 1.0, (8, SLOTS))
    for buf in (za, zb):
        buf[32:40, :] = jnp.zeros((8, 128), F32)
        buf[32:40, 0:SLOTS] = lines
    for copy in copies[4:]:
        copy.wait()
    for c in range(3):
        low, high = pos[c, 0:48, :], pos[c, 208:256, :]
        xa[48 * c : 48 * c + 48, :] = jnp.where(even_x, high, low)
        xb[48 * c : 48 * c + 48, :] = jnp.where(even_x, low, high)
        for i in range(16):
            to = 48 * c + 3 * i
            low, high = pos[c, 16 * i : 16 * i + 3, :], pos[c, 16 * i + 13 : 16 * i + 16, :]
            ya[to : to + 3, :] = jnp.where(even_y, high, low)
            yb[to : to + 3, :] = jnp.where(even_y, low, high)
    parts = [pos[c] for c in range(3)]
    low = pack_rows(edge_lanes(parts, 0, None))
    high = pack_rows(edge_lanes(parts, None, 0))
    za[0:32, :] = jnp.where(even_z, high, low)
    zb[0:32, :] = jnp.where(even_z, low, high)


def z_index(far_outer):
    z = far_outer - 3
    below = z < 0
    above = z > 255
    index = jnp.where(below, z + 12, jnp.where(above, z - 256, 0))
    return index, below | above


def z_values(edges, far_outer):
    index, outside = z_index(far_outer)
    out = []
    for c in range(3):
        parts = [
            take128(edges, index[:, t * 128 : (t + 1) * 128] + 3 * c) for t in (0, 1)
        ]
        out.append(jnp.where(outside, jnp.concatenate(parts, axis=1), 0.0))
    return out


def scatter(rows, node, xs, ys):
    for r, value in enumerate(rows):
        for t in (0, 1):
            xs[t, pl.ds(r, SLOTS, stride=8), :] = value[:, t * 128 : (t + 1) * 128]
    places = iota((256, 256), 0).astype(F32).astype(BF16)
    one, zero = jnp.ones((), BF16), jnp.zeros((), BF16)
    for s in range(SLOTS):
        at = slice(8 * s, 8 * s + 8)
        x = jnp.concatenate([xs[0, at, :], xs[1, at, :]], axis=1)
        hi = x.astype(BF16).astype(F32)
        index = node[s : s + 1, :].astype(F32).astype(BF16)
        got = lax.dot_general(
            jnp.concatenate([hi, x - hi], axis=0).astype(BF16),
            jnp.where(places == jnp.broadcast_to(index, (256, 256)), one, zero),
            (((1,), (1,)), ((), ())),
            preferred_element_type=F32,
        )
        total = got[8:16] + got[0:8]
        ys[0, at, :] = total[:, :128]
        ys[1, at, :] = total[:, 128:]
    return [
        jnp.concatenate([ys[t, pl.ds(r, SLOTS, stride=8), :] for t in (0, 1)], axis=1)
        for r in range(len(rows))
    ]


def pair_tile(rows, energy, *residuals):
    lane = iota((rows, 128), 1)
    out = jnp.where(lane == 9, energy, 0.0)
    for n, residual in enumerate(residuals):
        out = jnp.where(lane == 10 + n, residual, out)
    return out


def roll(x, shift):
    return pltpu.roll(x, shift % 128, axis=1) if shift % 128 else x


def pack_edges(parts, first):
    lane = iota((8, 128), 1)
    half, at = first // 128, first % 128
    out = jnp.zeros((8, 128), F32)
    for g in range(4):
        for c in range(3):
            part = parts[c][8 * g : 8 * g + 8, half * 128 : half * 128 + 128]
            for h in (0, 1):
                to = 64 * h + 16 * g + 3 * c
                out = jnp.where((lane >= to) & (lane < to + 3), roll(part, to - at), out)
    return jnp.where(iota((4, 128), 1) < 64, out[0:4], out[4:8])


def unpack_edges(tile, to):
    rows = [roll(tile, to - 64 * h - 16 * g) for g in range(4) for h in (0, 1)]
    return jnp.concatenate(rows, axis=0)


def depth_of(gap, live):
    return jnp.where(iota((SLOTS, 256), 0) < live, jnp.maximum(-gap, 0.0), 0.0)


def total2(x):
    return jnp.sum(jnp.sum(x, axis=0, keepdims=True), axis=1, keepdims=True)


def first_mask(pline):
    shape = (SLOTS, SLOTS)
    row = jnp.broadcast_to(pline.astype(F32), shape)
    col = column(pline.astype(F32), 0, SLOTS)
    again = jnp.where((row == col) & (iota(shape, 1) < iota(shape, 0)), 1.0, 0.0)
    first = jnp.sum(again, axis=1, keepdims=True) == 0.0
    return jnp.broadcast_to(jnp.where(first, 1.0, 0.0), (SLOTS, 256))


def residual_of(near, first):
    square = near[0] * near[0] + near[1] * near[1] + near[2] * near[2]
    return total2(first[...] * square)


def own_index(far):
    z = far[...] - 3
    return jnp.clip(z, 0, 255), (z >= 0) & (z < 256)


def respond(normal, tile, sel, requests, replies, sums):
    for j in range(128):
        sums[j] = tile
    keep = (iota((4, 128), 1) & 15) < 9
    me, k = position()
    sums[jnp.where(k > 0, me - 1, me)] = jnp.where(keep, pack_edges(normal, 0), tile)
    sums[jnp.where(k < 7, me + 1, me)] = jnp.where(keep, pack_edges(normal, 253), tile)
    for pair in (0, 2):
        at = slice(OUTER * pair, OUTER * pair + 2 * OUTER)
        lines = [pick(sel[at, :], normal[c]) for c in range(3)]
        for d, low in ((pair, 0), (pair + 1, OUTER)):
            buf = requests[d]
            index = buf[192:208, :].astype(I32)
            values = take_lanes([v[low : low + OUTER] for v in lines], index)
            answer = jnp.zeros((OUTER, 256), F32)
            for c in range(3):
                answer = answer + buf[144 + 16 * c : 160 + 16 * c, :] * values[c]
            replies[d][...] = answer


def own_kernel(normal, node, far, geom, first, sel, change, residual):
    index, inside = own_index(far)
    lines = [pick(sel[0:SLOTS, :], normal[c]) for c in range(3)]
    residual[...] = jnp.broadcast_to(residual_of(lines, first), (1, 128))
    near = take_lanes(lines, node[...])
    other = [pick(sel[SLOTS : 2 * SLOTS, :], normal[c]) for c in range(3)]
    other = take_lanes(other, index)
    moved = jnp.zeros((SLOTS, 256), F32)
    for c in range(3):
        moved = moved + geom[c] * (near[c] - jnp.where(inside, other[c], 0.0))
    change[...] = moved


def base_kernel(
    pos, node, far, geom, pline, fline, live,
    gap_out, own_out, face_out, inverse_out, first, xs, ys,
):
    first[...] = first_mask(pline[...])
    own = pline[...].astype(F32)
    near_col = column(own, 0, SLOTS)
    far_col = column(fline[...].astype(F32), 0, SLOTS)
    x, y, line = decode(far_col.astype(I32))
    inside = (x >= 0) & (x < 16) & (y >= 0) & (y < 16)
    local = jnp.where(inside, line, -2).astype(F32)
    both = jnp.concatenate([near_col, local], axis=0)
    own_out[...] = jnp.broadcast_to(both, (2 * SLOTS, 128))
    xo, yo = x[OUTER:], y[OUTER:]
    even_x, even_y, _ = evens()
    at_x, at_y = jnp.where(even_x, 48, 0), jnp.where(even_y, 48, 0)
    face = jnp.where(xo < 0, at_x + (xo + 3) * 16 + yo, -1)
    face = jnp.where(xo > 15, 48 - at_x + (xo - 16) * 16 + yo, face)
    face = jnp.where(yo < 0, 96 + at_y + xo * 3 + yo + 3, face)
    face = jnp.where(yo > 15, 144 - at_y + xo * 3 + yo - 16, face)
    face_out[...] = hot(iota((OUTER, 192), 1), face)
    ones = jnp.where(iota((SLOTS, 256), 0) < live[...], 1.0, 0.0)
    (counts,) = scatter([ones], node, xs, ys)
    same = hot(jnp.broadcast_to(twice(own), (SLOTS, 2 * SLOTS)), near_col)
    inverse_out[...] = 1.0 / (1.0 + pick(same, counts))
    sel = hot(iota((2 * SLOTS, 256), 1).astype(F32), both)
    index, within = own_index(far)
    got = [pick(sel, pos[c]) for c in range(3)]
    near = take_lanes([v[0:SLOTS] for v in got], node[...])
    other = take_lanes([v[SLOTS:] for v in got], index)
    gap = jnp.zeros((SLOTS, 256), F32)
    for c in range(3):
        gap = gap + geom[c] * (near[c] - jnp.where(within, other[c], 0.0))
    gap_out[...] = gap - geom[3]


def first_kernel(
    gap_in, own, face, inverse, far, geom, pline, live, node,
    xa, xb, ya, yb, za, zb,
    gap_out, normal_out, moved_out, own_sel, out_sel, selz_out, *rest,
):
    *replies, sums, xs, ys = rest
    requests = (xa, xb, ya, yb)
    even_z = evens()[2]
    above = jnp.where(even_z, za[...], zb[...])
    below = jnp.where(even_z, zb[...], za[...])
    wanted = jnp.concatenate(
        [own[:, 0:1]] + [column(buf[208:209, 0:SLOTS], OUTER, OUTER) - 1.0 for buf in requests], axis=0
    )
    lines = twice(pline[...].astype(F32))
    sel = hot(jnp.broadcast_to(lines, (128, 2 * SLOTS)), wanted)
    own_sel[...] = sel[0:64]
    out_sel[...] = sel[64:128]
    local = own[SLOTS + OUTER :, 0:1]
    selz = jnp.concatenate([above[32:33, 0:SLOTS], below[32:33, 0:SLOTS]], axis=1) - 1.0
    selz_out[...] = hot(jnp.broadcast_to(twice(selz), (OUTER, 4 * SLOTS)), local)
    edges = jnp.where(
        iota((256, 128), 1) < 9,
        unpack_rows(above[0:32]),
        pltpu.roll(unpack_rows(below[0:32]), 9, axis=1),
    )
    sel = hot(iota((OUTER, 256), 1).astype(F32), local)
    ends = z_values(pick(sel, edges), far[OUTER:, :])
    index, within = own_index(far)
    faces = [
        pick(face[...], jnp.concatenate([buf[48 * c : 48 * c + 48, :] for buf in requests], axis=0))
        for c in range(3)
    ]
    faces = take_lanes(faces, index[OUTER:])
    outer = jnp.zeros((OUTER, 256), F32)
    for c in range(3):
        outer = outer + geom[c, OUTER:, :] * (
            jnp.where(within[OUTER:], faces[c], 0.0) + ends[c]
        )
    gap = gap_in[...] - jnp.concatenate([jnp.zeros((OUTER, 256), F32), outer], axis=0)
    gap_out[...] = gap
    depth = depth_of(gap, live[...])
    tile = pair_tile(4, total2(depth * depth))
    got = scatter([depth * geom[c] for c in range(3)], node, xs, ys)
    normal = [got[c] * inverse[...] for c in range(3)]
    for c in range(3):
        normal_out[c] = normal[c]
        moved_out[c] = jnp.zeros((SLOTS, 256), F32)
    respond(normal, tile, out_sel, requests, replies, sums)


def chunk_sum(got):
    parts = [got[j] for j in range(128)]
    while len(parts) > 1:
        parts = [a + b for a, b in zip(parts[::2], parts[1::2], strict=True)]
    return parts[0][0:1]


def update(gap, change, far, geom, selz, replies, got):
    sums = chunk_sum(got)
    scale = RELAX * (1.0 / (1.0 + sums[0:1, 9:10] / N_PAIRS))
    me, k = position()
    lane = iota((SLOTS, 128), 1)
    above = unpack_edges(got[jnp.where(k < 7, me + 1, me)], 0)
    below = unpack_edges(got[jnp.where(k > 0, me - 1, me)], 9)
    above = jnp.where(lane < 9, above, 0.0)
    below = jnp.where((lane > 8) & (lane < 18), below, 0.0)
    ends = z_values(
        pick(selz[...], jnp.concatenate([above, below], axis=0)), far[OUTER:, :]
    )
    outer = (replies[0][...] + replies[1][...]) + (replies[2][...] + replies[3][...])
    for c in range(3):
        outer = outer + geom[c, OUTER:, :] * ends[c]
    full = change[...] - jnp.concatenate([jnp.zeros((OUTER, 256), F32), outer], axis=0)
    return sums, scale, gap[...] + scale * full


def sweep_kernel(
    last, gap, change, residual, normal, moved, inverse, node, far, geom, live, selz,
    r0, r1, r2, r3, got, *rest,
):
    if last:
        first, own_sel, sums_out, normal_out, moved_out, out, xs, ys = rest
    else:
        *rest, xs, ys = rest
        *requests, out_sel, gap_out, sums_out, normal_out, moved_out = rest[:9]
        *replies, out = rest[9:]
    sums, scale, fresh = update(gap, change, far, geom, selz, (r0, r1, r2, r3), got)
    sums_out[...] = sums
    for c in range(3):
        moved_out[c] = moved[c] + scale * normal[c]
    depth = depth_of(fresh, live[...])
    energy = total2(depth * depth)
    before = residual[:, 0:1]
    if not last:
        tile = pair_tile(4, energy, before)
    found = scatter([depth * geom[c] for c in range(3)], node, xs, ys)
    fresh_normal = [found[c] * inverse[...] for c in range(3)]
    for c in range(3):
        normal_out[c] = fresh_normal[c]
    if last:
        lines = [pick(own_sel[0:SLOTS, :], fresh_normal[c]) for c in range(3)]
        tile = pair_tile(8, energy, before, residual_of(lines, first))
        out[...] = jnp.broadcast_to(tile[0:1, :], (128, 128))
    else:
        gap_out[...] = fresh
        respond(fresh_normal, tile, out_sel, requests, replies, out)


def last_kernel(pos, normal, moved, pline, got, s0, s1, s2, s3, out, history):
    every = [s[0:1, :] for s in (s0, s1, s2, s3)] + [jnp.sum(got[...], axis=0, keepdims=True)]
    scales = [RELAX * (1.0 / (1.0 + s[:, 9:10] / N_PAIRS)) for s in every]
    sel = hot(iota((256, SLOTS), 0), jnp.broadcast_to(pline[...], (256, SLOTS)))
    for c in range(3):
        out[c] = pos[c] + pick(sel, moved[c] + scales[-1] * normal[c])
    for t in range(SWEEPS):
        later = every[t + 1][:, 10:11] if t + 1 < SWEEPS else every[t][:, 11:12]
        residual = scales[t] * scales[t] * later
        history[0:1, t : t + 1] = jnp.sqrt(1.0 + every[t][:, 9:10] / PAIRS_SLOTS)
        history[1:2, t : t + 1] = jnp.sqrt(1.0 + residual / NODES_BLK)


within = pltpu.with_memory_space_constraint


def call(kernel, outs, args, scratch=(), inputs=False):
    vmem = pl.BlockSpec(memory_space=pltpu.VMEM)
    hbm = pl.BlockSpec(memory_space=pltpu.HBM)
    return pl.pallas_call(
        kernel,
        out_shape=outs,
        in_specs=[hbm if inputs else vmem] * len(args),
        out_specs=[vmem] * len(outs),
        scratch_shapes=list(scratch),
        compiler_params=pltpu.CompilerParams(
            vmem_limit_bytes=12 * 2**20,
        ),
    )(*(args if inputs else [within(x, pltpu.VMEM) for x in args]))


def shape(*dims, dtype=F32):
    return pltpu.VMEM(dims, dtype)


def swap(x, axis, second):
    count = lax.axis_size(axis)
    pairs = [(i, (i + 1) % count) for i in range(int(second), count, 2)]
    return lax.ppermute(x, axis, pairs + [(b, a) for a, b in pairs])


def swap_all(arrays):
    axes = ("gx", "gx", "gy", "gy", GZ, GZ)
    return [swap(x, axis, n % 2) for n, (x, axis) in enumerate(zip(arrays, axes))]


def local(positions, pair_node, pair_line, pair_far, far_line, pair_geom, live_blocks):
    pos = positions.reshape(3, 256, 256)
    node = pair_node.reshape(SLOTS, 256)
    far = pair_far.reshape(SLOTS, 256)
    geom = pair_geom.reshape(SLOTS, 4, 256)
    pline = pair_line.reshape(1, SLOTS)
    fline = far_line.reshape(1, SLOTS)
    live = live_blocks.reshape(1, 1)
    work = [pltpu.VMEM((2, 256, 128), F32)] * 2

    face, ends = shape(216, 256), shape(40, 128)
    flat = shape(SLOTS, 256)
    flat_i = shape(SLOTS, 256, dtype=I32)
    few = shape(1, SLOTS, dtype=I32)
    packed = call(
        pack_kernel,
        [face] * 4
        + [ends] * 2
        + [shape(4, SLOTS, 256), shape(3, 256, 256), flat_i, flat_i, few, few]
        + [shape(1, 1, dtype=I32)],
        [within(x, pltpu.HBM) for x in (pos, node, far, geom, pline, fline)] + [live],
        [pltpu.VMEM((SLOTS, 4, 256), F32), pltpu.SemaphoreType.DMA((7,))],
        inputs=True,
    )
    *six, geom, pos, node, far, pline, fline, live = packed
    *requests, za, zb = swap_all(six)
    triple = shape(3, SLOTS, 256)
    outs = [shape(OUTER, 256)] * 4 + [shape(128, 4, 128)]
    gap, own, face, inverse, first = call(
        base_kernel,
        [
            flat,
            shape(2 * SLOTS, 128),
            shape(OUTER, 192, dtype=BF16),
            flat,
            flat,
        ],
        [pos, node, far, geom, pline, fline, live],
        work,
    )
    choice = shape(2 * SLOTS, 2 * SLOTS, dtype=BF16)
    gap, normal, moved, own_sel, out_sel, selz, *sent, sums = call(
        first_kernel,
        [flat, triple, triple, choice, choice, shape(OUTER, 4 * SLOTS, dtype=BF16)] + outs,
        [gap, own, face, inverse, far, geom, pline, live, node] + requests + [za, zb],
        work,
    )
    totals = []
    row = shape(1, 128)
    for t in range(1, SWEEPS):
        replies = swap_all(sent)
        got = lax.all_to_all(sums, ALL, 0, 0, tiled=True)
        change, residual = call(
            own_kernel, [flat, row], [normal, node, far, geom, first, own_sel]
        )
        args = [
            gap, change, residual, normal, moved, inverse, node, far, geom, live, selz,
        ]
        args = args + replies + [got]
        if t + 1 < SWEEPS:
            gap, total, normal, moved, *sent, sums = call(
                functools.partial(sweep_kernel, False),
                [flat, row, triple, triple] + outs,
                args + requests + [out_sel],
                work,
            )
        else:
            total, normal, moved, sums = call(
                functools.partial(sweep_kernel, True),
                [row, triple, triple, shape(128, 128)],
                args + [first, own_sel],
                work,
            )
        totals.append(total)
    sums = sums.reshape(128, 1, 128)
    got = lax.all_to_all(sums, ALL, 0, 0, tiled=True).reshape(128, 128)
    corrected, history = call(
        last_kernel,
        [jax.ShapeDtypeStruct((3, 256, 256), F32), jax.ShapeDtypeStruct((2, SWEEPS), F32)],
        [pos, normal, moved, pline, got, *totals],
    )
    return corrected.reshape(positions.shape), history


def solution(mesh):
    finer = Mesh(
        mesh.devices.reshape(mesh.shape["gx"], mesh.shape["gy"], 4, 2), ("gx", "gy", "gz_0", "gz_1")
    )
    placed = (
        P(None, "gx", "gy", GZ),
        P("gx", "gy", GZ, None, None),
        P("gx", "gy", GZ, None),
        P("gx", "gy", GZ, None, None),
        P("gx", "gy", GZ, None),
        P("gx", "gy", GZ, None, None, None),
        P("gx", "gy", GZ),
    )
    return jax.shard_map(
        local,
        mesh=finer,
        in_specs=placed,
        out_specs=(P(None, "gx", "gy", GZ), P()),
        check_vma=False,
    )
```
